256 devices in a mesh: grp: 8 (over x_lo, y), smp: 32 (over x_hi, z, core).
Axes of the slice: x: 4 (x_hi: 2, x_lo: 2; x = x_hi * 2 + x_lo), y: 4, z: 8, core: 2. Of those that a mesh axis runs over, the one named last changes fastest.
Arguments:
- spins_packed: int32 [32, 32768], P(None, 'smp'), may hold values from -2147483648 to 2147483646
- weight: bfloat16 [1024, 8192], P(None, 'grp'), may hold values from -0.1875 to 0.1875
- hidden_bias: float32 [8192], P('grp'), may hold values from -1.5 to 1.5
- force_w: float32 [1024, 8192], P('smp', 'grp'), may hold values from -6 to 6
- force_b: float32 [8192], P('grp'), may hold values from -6 to 6
Outputs:
- update_w: float32 [1024, 8192], P('smp', 'grp')
- update_b: float32 [8192], P('grp')
The draws below stay inside these ranges and needn't reach their ends.
All inputs are finite; a program needn't handle non-finite values.
Results may differ from the reference program's by a relative error of at most 0.0003.
Values sent between devices are 32-bit elements; how exact they have to be, the bound alone decides.
No kernel may reach another device: no remote copies, remote signals or barrier semaphores. Data moves between devices by JAX's collectives and lax.ppermute only.
A program may use at most 64 MiB of HBM per device.

```python
import jax
import jax.numpy as jnp
from jax import lax

NV = 1024
NH = 8192
TOK_DEV = 1024
ITERS = 2
WORDS = 32
TOKENS = 32768


def with_ends(entries, stream_key, low, high):
    dims = entries.shape
    spot = [jax.random.randint(jax.random.fold_in(stream_key, axis), (), 0, dims[axis]) for axis in range(len(dims))]
    entries = entries.at[tuple(spot)].set(low)
    longest = dims.index(max(dims))
    spot[longest] = (spot[longest] + 1) % dims[longest]
    return entries.at[tuple(spot)].set(high)


def block_levels(stream_key, dims, split, smallest, top_value):
    level = 1.0
    for axis_at, shards_of in split:
        heights = jax.random.uniform(jax.random.fold_in(jax.random.fold_in(stream_key, 6), axis_at), (shards_of,), jnp.float32, smallest / len(split), top_value / len(split))
        level = level * jnp.repeat(jnp.exp(heights), dims[axis_at] // shards_of).reshape((-1,) + (1,) * (len(dims) - 1 - axis_at))
    return level


def bell_draw(rng, shape, width, reach, shards=(), kind=jnp.bfloat16):
    array = width * jax.random.normal(rng, shape, jnp.float32)
    if shards:
        array = array * block_levels(rng, shape, shards, -0.22, 0.18)
    return jnp.clip(array, -reach, reach).astype(kind)


def setup_inputs(seed: int = 0) -> dict:
    key_of = jax.random.split(jax.random.key(seed), 6)
    spins_packed = with_ends(jax.random.randint(key_of[0], (WORDS, TOKENS), -2147483648, 2147483647), jax.random.fold_in(key_of[0], 1), -2147483648, 2147483646).astype(jnp.int32)
    weight = bell_draw(key_of[1], (NV, NH), NV ** -0.5, 0.1875, ((1, 8),))
    hidden_bias = jnp.clip(jax.random.uniform(key_of[2], (NH,), jnp.float32, -1.5, 1.5) * block_levels(key_of[2], (NH,), ((0, 8),), -0.4, 0.0), -1.5, 1.5)
    force_w = bell_draw(key_of[3], (NV, NH), 1.0, 6.0, ((0, 32), (1, 8)), jnp.float32)
    force_b = bell_draw(key_of[4], (NH,), 1.0, 6.0, ((0, 8),), jnp.float32)
    return dict(spins_packed=spins_packed, weight=weight, hidden_bias=hidden_bias, force_w=force_w, force_b=force_b)


diag_shift = 0.01


def unpack(packed):
    shifts = jnp.arange(32, dtype=jnp.int32)
    bit_values = jnp.bitwise_and(jnp.right_shift(packed[:, None, :], shifts[None, :, None]), 1)
    signs = 2 * bit_values - 1
    return signs.reshape(packed.shape[0] * 32, packed.shape[1]).astype(jnp.bfloat16)


def reference(spins_packed, weight, hidden_bias, force_w, force_b):
    spins = unpack(spins_packed)
    tile_count = TOKENS // TOK_DEV
    tiles = spins.reshape(NV, tile_count, TOK_DEV).transpose(1, 0, 2)

    def activations(sample_tile):
        pre_activation = jnp.einsum("it,ih->th", sample_tile, weight, preferred_element_type=jnp.float32)
        return jnp.tanh(pre_activation + hidden_bias)

    def forward(direction_w, direction_b):
        def scan_step(running, sample_tile):
            hidden = activations(sample_tile)
            projected = jnp.einsum("it,ih->th", sample_tile, direction_w, precision=lax.Precision.HIGHEST, preferred_element_type=jnp.float32)
            return running, jnp.sum(hidden * (projected + direction_b), axis=1)

        _, sample_values = lax.scan(scan_step, jnp.zeros((), jnp.float32), tiles)
        sample_values = sample_values.reshape(TOKENS)
        return sample_values - jnp.sum(sample_values) / TOKENS

    def metric(centred, direction_w, direction_b):
        scaled = (centred / TOKENS).reshape(tile_count, TOK_DEV)

        def scan_step(running, inputs):
            sample_tile, weights_now = inputs
            hidden = activations(sample_tile)
            weighted = weights_now[:, None] * hidden
            grad_w = running[0] + jnp.einsum("it,th->ih", sample_tile, weighted, precision=lax.Precision.HIGHEST, preferred_element_type=jnp.float32)
            grad_b = running[1] + jnp.dot(weights_now, hidden, precision=lax.Precision.HIGHEST, preferred_element_type=jnp.float32)
            return (grad_w, grad_b), None

        zeros_pair = (jnp.zeros((NV, NH), jnp.float32), jnp.zeros((NH,), jnp.float32))
        (grad_w, grad_b), _ = lax.scan(scan_step, zeros_pair, (tiles, scaled))
        return grad_w + diag_shift * direction_w, grad_b + diag_shift * direction_b

    solution_w = jnp.zeros_like(force_w)
    solution_b = jnp.zeros_like(force_b)
    residual_w, residual_b = force_w, force_b
    direction_w, direction_b = force_w, force_b
    norm_now = jnp.sum(residual_w * residual_w) + jnp.sum(residual_b * residual_b)
    for iteration in range(ITERS):
        centred = forward(direction_w, direction_b)
        curvature = jnp.sum(centred * centred) / TOKENS + diag_shift * (jnp.sum(direction_w * direction_w) + jnp.sum(direction_b * direction_b))
        step_size = norm_now / curvature
        solution_w = solution_w + step_size * direction_w
        solution_b = solution_b + step_size * direction_b
        if iteration + 1 < ITERS:
            image_w, image_b = metric(centred, direction_w, direction_b)
            residual_w = residual_w - step_size * image_w
            residual_b = residual_b - step_size * image_b
            norm_next = jnp.sum(residual_w * residual_w) + jnp.sum(residual_b * residual_b)
            direction_w = residual_w + (norm_next / norm_now) * direction_w
            direction_b = residual_b + (norm_next / norm_now) * direction_b
            norm_now = norm_next
    return solution_w, solution_b
```

```python
import functools

import jax
import jax.numpy as jnp
from jax import lax
from jax.experimental import pallas as pl
from jax.experimental.pallas import tpu as pltpu
from jax.sharding import Mesh
from jax.sharding import PartitionSpec as P

GRP = ("xl", "y")
SMP = ("xh", "zh", "zl", "c")
SUM = ("xl", "y", "zh")
SWAP = [(0, 1), (1, 0)]
LAM = 0.01
ROWS = 32
NB = 8
F32, BF16 = jnp.float32, jnp.bfloat16


def swap(x, axis):
    return lax.ppermute(x, axis, SWAP)


def split_terms(x):
    hi = x.astype(BF16)
    return hi, (x - hi.astype(F32)).astype(BF16)


def to_all(x, axes, size):
    return lax.all_to_all(jnp.broadcast_to(x[None], (size, *x.shape)), axes, 0, 0, tiled=True)


def params(limit=56 << 20):
    return pltpu.CompilerParams(dimension_semantics=("arbitrary",), vmem_limit_bytes=limit)


def unpack_tile(words_ref, packed_ref, out_ref):
    bits = lax.broadcasted_iota(jnp.int32, (ROWS, packed_ref.shape[1]), 0)
    for q in range(32):
        word = packed_ref[pl.ds(words_ref[q], 1), :]
        up = jnp.left_shift(jnp.broadcast_to(word, bits.shape), 31 - bits) < 0
        out_ref[q * ROWS : (q + 1) * ROWS, :] = jnp.where(up, 1.0, -1.0).astype(BF16)


def first_kernel(words_ref, packed_ref, wt_ref, f_ref, hb_ref, fb_ref, s_ref, h_ref, p_ref, n_ref, lhs):
    units = wt_ref.shape[0]

    @pl.when(pl.program_id(0) == 0)
    def _():
        lhs[:units, :] = wt_ref[...]
        total = jnp.zeros((units, 128), F32)
        for b in range(NB):
            block = f_ref[b]
            hi, lo = split_terms(block)
            lhs[units : 2 * units, b * 128 : (b + 1) * 128] = hi
            lhs[2 * units :, b * 128 : (b + 1) * 128] = lo
            total = total + block * block
        fb = fb_ref[...]
        n_ref[...] = jnp.full(n_ref.shape, jnp.sum(total) + jnp.sum(fb * fb), F32)

    unpack_tile(words_ref, packed_ref, s_ref)
    out = jnp.dot(lhs[...], s_ref[...], preferred_element_type=F32)
    hidden = jnp.tanh(out[:units] + hb_ref[...])
    h_ref[...] = hidden
    proj = out[units : 2 * units] + out[2 * units :] + fb_ref[...]
    p_ref[...] = jnp.sum(hidden * proj, axis=0, keepdims=True)


def first_pass(words, packed, wt, f, hb, fb):
    parts, _, tile = packed.shape
    units = wt.shape[0]
    n = parts * tile
    full = lambda shape: pl.BlockSpec(shape, lambda t: (0,) * len(shape))
    return pl.pallas_call(
        first_kernel,
        grid=(parts,),
        in_specs=[
            pl.BlockSpec(memory_space=pltpu.SMEM),
            pl.BlockSpec((None, ROWS, tile), lambda t: (t, 0, 0)),
            full(wt.shape),
            full(f.shape),
            full(hb.shape),
            full(fb.shape),
        ],
        out_specs=[
            pl.BlockSpec((NB * 128, tile), lambda t: (0, t)),
            pl.BlockSpec((units, tile), lambda t: (0, t)),
            pl.BlockSpec((1, tile), lambda t: (0, t)),
            full((1, 128)),
        ],
        out_shape=[
            jax.ShapeDtypeStruct((NB * 128, n), BF16),
            jax.ShapeDtypeStruct((units, n), F32),
            jax.ShapeDtypeStruct((1, n), F32),
            jax.ShapeDtypeStruct((1, 128), F32),
        ],
        scratch_shapes=[pltpu.VMEM((3 * units, NB * 128), BF16)],
        compiler_params=params(),
        name="first_pass",
    )(words, packed, wt, f, hb, fb)


def image_kernel(s_ref, h_ref, c_ref, keep_ref, send_ref, acc, bsum):
    units = h_ref.shape[0]
    step = pl.program_id(0)
    r = h_ref[...] * c_ref[...]
    hi, lo = split_terms(r)
    both = jnp.concatenate([hi, lo], axis=0)
    out = lax.dot_general(both, s_ref[...], (((1,), (1,)), ((), ())), preferred_element_type=F32)
    part = out[:units] + out[units:]
    lanes = r[:, :128]
    for k in range(1, r.shape[1] // 128):
        lanes = lanes + r[:, k * 128 : (k + 1) * 128]

    @pl.when(step == 0)
    def _():
        acc[...] = part
        bsum[...] = lanes

    @pl.when(step > 0)
    def _():
        acc[...] += part
        bsum[...] += lanes

    @pl.when(step == pl.num_programs(0) - 1)
    def _():
        half = NB // 2
        for b in range(half):
            keep_ref[b * units : (b + 1) * units, :] = acc[:, b * 128 : (b + 1) * 128]
            send_ref[b * units : (b + 1) * units, :] = acc[:, (b + half) * 128 : (b + half + 1) * 128]
        tail = pl.ds(half * units, 8)
        keep_ref[tail, :] = jnp.zeros((8, 128), F32)
        send_ref[tail, :] = jnp.zeros((8, 128), F32)
        for k in range(units // 128):
            row = jnp.sum(bsum[k * 128 : (k + 1) * 128, :].T, axis=0, keepdims=True)
            keep_ref[half * units + k : half * units + k + 1, :] = row
            send_ref[half * units + k : half * units + k + 1, :] = row


def image_pass(spins, hidden, c, tile=1024):
    units, n = hidden.shape
    rows = NB // 2 * units + 8
    full = lambda shape: pl.BlockSpec(shape, lambda t: (0,) * len(shape))
    return pl.pallas_call(
        image_kernel,
        grid=(n // tile,),
        in_specs=[
            pl.BlockSpec((NB * 128, tile), lambda t: (0, t)),
            pl.BlockSpec((units, tile), lambda t: (0, t)),
            pl.BlockSpec((1, tile), lambda t: (0, t)),
        ],
        out_specs=[full((rows, 128))] * 2,
        out_shape=[jax.ShapeDtypeStruct((rows, 128), F32)] * 2,
        scratch_shapes=[pltpu.VMEM((units, NB * 128), F32), pltpu.VMEM((units, 128), F32)],
        compiler_params=params(),
        name="image_pass",
    )(spins, hidden, c)


def second_kernel(step_ref, s_ref, h_ref, f_ref, g0_ref, g1_ref, fb_ref, gb_ref, p_ref, n_ref, lhs, rb):
    units = h_ref.shape[0]

    @pl.when(pl.program_id(0) == 0)
    def _():
        a = step_ref[0]
        rr = jnp.zeros((units, 128), F32)
        rf = jnp.zeros((units, 128), F32)
        for b in range(NB):
            f = f_ref[b]
            g_ref = g0_ref if b < NB // 2 else g1_ref
            row = (b % (NB // 2)) * units
            r = f - a * (g_ref[row : row + units, :] + LAM * f)
            hi, lo = split_terms(r)
            lhs[:units, b * 128 : (b + 1) * 128] = hi
            lhs[units:, b * 128 : (b + 1) * 128] = lo
            rr = rr + r * r
            rf = rf + r * f
        fb = fb_ref[...]
        r = fb - a * (gb_ref[...] + LAM * fb)
        rb[...] = r
        n_ref[...] = jnp.concatenate(
            [
                jnp.full((1, 128), jnp.sum(rr) + jnp.sum(r * r), F32),
                jnp.full((1, 128), jnp.sum(rf) + jnp.sum(r * fb), F32),
            ],
            axis=1,
        )

    out = jnp.dot(lhs[...], s_ref[...], preferred_element_type=F32)
    proj = out[:units] + out[units:] + rb[...]
    p_ref[...] = jnp.sum(h_ref[...] * proj, axis=0, keepdims=True)


def second_pass(step_size, spins, hidden, f, g0, g1, fb, gb, tile=1024):
    units, n = hidden.shape
    full = lambda shape: pl.BlockSpec(shape, lambda t: (0,) * len(shape))
    return pl.pallas_call(
        second_kernel,
        grid=(n // tile,),
        in_specs=[
            pl.BlockSpec(memory_space=pltpu.SMEM),
            pl.BlockSpec((NB * 128, tile), lambda t: (0, t)),
            pl.BlockSpec((units, tile), lambda t: (0, t)),
            full(f.shape),
            full(g0.shape),
            full(g1.shape),
            full(fb.shape),
            full(gb.shape),
        ],
        out_specs=[pl.BlockSpec((1, tile), lambda t: (0, t)), full((1, 256))],
        out_shape=[jax.ShapeDtypeStruct((1, n), F32), jax.ShapeDtypeStruct((1, 256), F32)],
        scratch_shapes=[pltpu.VMEM((2 * units, NB * 128), BF16), pltpu.VMEM((units, 1), F32)],
        compiler_params=params(),
        name="second_pass",
    )(step_size, spins, hidden, f, g0, g1, fb, gb)


def merged(mean, spread, count, axis):
    got = swap(jnp.stack([mean, spread]).reshape(1, 2), axis)
    delta = got[0, 0] - mean
    return 0.5 * (mean + got[0, 0]), spread + got[0, 1] + (0.5 * count) * delta * delta


def stats(values):
    count = values.size
    mean = jnp.sum(values) / count
    spread = jnp.sum((values - mean) ** 2)
    for axis in ("c", "zl", "xh"):
        mean, spread = merged(mean, spread, count, axis)
        count *= 2
    return mean, spread


def body(spins_packed, weight, hidden_bias, force_w, force_b):
    xh, zh, zl, c = (lax.axis_index(a) for a in SMP)
    parts = lax.axis_size("zh")
    summed = lax.axis_size(SUM)
    units = weight.shape[1] // parts
    samples = spins_packed.shape[1] * lax.axis_size(SMP)

    q = jnp.arange(32, dtype=jnp.int32)
    words = (((q >> 2) & 1) ^ xh) * 16 + (q & 3) * 4 + (((q >> 3) & 1) ^ zl) * 2 + ((q >> 4) ^ c)

    f_cols = force_w.reshape(ROWS, parts, units).transpose(1, 0, 2)
    f_rows = lax.all_to_all(f_cols, "zh", 0, 0, tiled=True).reshape(parts * ROWS, units)
    f = f_rows.T[None]
    for axis in ("xh", "zl", "c"):
        f = jnp.concatenate([f, swap(f, axis)], axis=0)

    packed = to_all(spins_packed, "zh", parts)

    w = lax.dynamic_slice_in_dim(weight, zh * units, units, 1).reshape(2, parts, 2, 2, ROWS, units)
    for dim, bit in ((0, xh), (2, zl), (3, c)):
        w = jnp.where(bit == 1, jnp.flip(w, dim), w)
    wt = w.transpose(3, 2, 0, 1, 4, 5).reshape(NB * 128, units).T
    hb = lax.dynamic_slice_in_dim(hidden_bias, zh * units, units, 0).reshape(units, 1)
    fb = lax.dynamic_slice_in_dim(force_b, zh * units, units, 0).reshape(units, 1)

    spins, hidden, partial, norm = first_pass(words, packed, wt, f, hb, fb)
    gathered = to_all(jnp.concatenate([partial, norm], axis=1), SUM, summed).sum(axis=0)
    n = partial.shape[1]
    values = gathered[:, :n]
    norm_now = gathered[0, n]
    mean, spread = stats(values)
    curvature = spread / samples + LAM * norm_now
    step0 = norm_now / curvature

    keep, send = image_pass(spins, hidden, (values - mean) / samples)
    g = keep + swap(send, "c")
    rows = 2 * units
    g = jnp.concatenate([g[:rows], g[2 * rows :]], axis=0) + swap(g[rows:], "zl")
    got = swap(g, "xh")
    g = g + jnp.concatenate([got[units:rows], got[:units], got[rows:]], axis=0)
    gb = g[rows : rows + units // 128].reshape(units)
    g_mine = g[:units].T.reshape(parts, ROWS, units)
    g_mine = jnp.concatenate([g_mine, jnp.broadcast_to(gb, (parts, 8, units))], axis=1)
    g = g[:rows]
    g = jnp.concatenate([g, swap(g, "zl")], axis=0)
    g1 = swap(g, "c")
    g_mine = lax.all_to_all(g_mine, "zh", 0, 0, tiled=True)
    gw = g_mine[:, :ROWS].transpose(1, 0, 2).reshape(ROWS, parts * units)
    gb_all = g_mine[:, ROWS].reshape(parts * units)

    partial, norms = second_pass(step0.reshape(1), spins, hidden, f, g, g1, fb, gb.reshape(units, 1))
    gathered = to_all(jnp.concatenate([partial, norms], axis=1), SUM, summed).sum(axis=0)
    norm_next = gathered[0, n]
    cross = gathered[0, n + 128]
    beta = norm_next / norm_now
    _, spread = stats(gathered[:, :n] + beta * values)
    length = norm_next + 2.0 * beta * cross + beta * beta * norm_now
    step1 = norm_next / (spread / samples + LAM * length)

    def update(f0, g0):
        r = f0 - step0 * (g0 + LAM * f0)
        return step0 * f0 + step1 * (r + beta * f0)

    return update(force_w, gw), update(force_b, gb_all)


def solution(mesh):
    torus = Mesh(mesh.devices.reshape(2, 4, 2, 4, 2, 2), ("xl", "y", "xh", "zh", "zl", "c"))
    in_specs = (P(None, SMP), P(None, GRP), P(GRP), P(SMP, GRP), P(GRP))
    out_specs = (P(SMP, GRP), P(GRP))
    return jax.shard_map(body, mesh=torus, in_specs=in_specs, out_specs=out_specs, check_vma=False)
```

```python
import functools

import jax
import jax.numpy as jnp
from jax import lax
from jax.experimental import pallas as pl
from jax.experimental.pallas import tpu as pltpu
from jax.sharding import Mesh
from jax.sharding import PartitionSpec as P

GRP = ("xl", "y")
SMP = ("xh", "zh", "zl", "c")
SUM = ("zh", "xl", "y")
QUAD = ("xh", "zl")
SWAP = [(0, 1), (1, 0)]
LAM = 0.01
ROWS = 32
NB = 8
TILE = 1024
EXTRA = 128
F32, BF16 = jnp.float32, jnp.bfloat16
VMEM = pl.BlockSpec(memory_space=pltpu.VMEM)
SMEM = pl.BlockSpec(memory_space=pltpu.SMEM)


def swap(x, axis):
    return lax.ppermute(x, axis, SWAP)


def to_all(x, axes, size):
    return lax.all_to_all(jnp.broadcast_to(x[None], (size, *x.shape)), axes, 0, 0, tiled=True)


def split_terms(x):
    hi = x.astype(BF16)
    return hi, (x - hi.astype(F32)).astype(BF16)


def resident(x):
    return pltpu.with_memory_space_constraint(x, pltpu.VMEM)


def call(kernel, ins, outs, scratch=(), flops=0, name=None):
    return pl.pallas_call(
        kernel,
        in_specs=ins,
        out_specs=[VMEM] * len(outs),
        out_shape=outs,
        scratch_shapes=scratch,
        compiler_params=pltpu.CompilerParams(vmem_limit_bytes=40 << 20),
        cost_estimate=pl.CostEstimate(flops=flops, bytes_accessed=1 << 20, transcendentals=0),
        name=name,
    )


def cols(t):
    return pl.ds(pl.multiple_of(t * TILE, TILE), TILE)


def rows_to_column(rows):
    return jnp.concatenate(
        [jnp.broadcast_to(rows[k : k + 1, :], (128, 128)).T[:, :1] for k in range(rows.shape[0])], axis=0
    )


def total(x):
    return jnp.full((1, EXTRA), jnp.sum(x), F32)


def hidden_kernel(pos_ref, packed_ref, wt_ref, hb_ref, s_ref, h_ref):
    units = wt_ref.shape[0]
    shifts = 31 - lax.broadcasted_iota(jnp.int32, (ROWS, TILE), 0)
    hb = rows_to_column(hb_ref[pl.ds(pos_ref[32] * (units // 128), units // 128), :])

    def step(t, carry):
        for q in range(32):
            word = packed_ref[t, pl.ds(pos_ref[q], 1), :]
            up = jnp.left_shift(jnp.broadcast_to(word, (ROWS, TILE)), shifts) < 0
            s_ref[q * ROWS : (q + 1) * ROWS, cols(t)] = jnp.where(up, 1.0, -1.0).astype(BF16)
        pre = jnp.dot(wt_ref[...], s_ref[:, cols(t)], preferred_element_type=F32)
        h_ref[:, cols(t)] = jnp.tanh(pre + hb)
        return carry

    lax.fori_loop(0, packed_ref.shape[0], step, 0)


def hidden_pass(pos, packed, wt, hb):
    units, n = wt.shape[0], packed.shape[0] * TILE
    return call(
        hidden_kernel,
        [SMEM, VMEM, VMEM, VMEM],
        [pltpu.VMEM((NB * 128, n), BF16), pltpu.VMEM((units, n), F32)],
        flops=4 * 10**9,
        name="hidden_pass",
    )(pos, packed, wt, hb)


def project(s_ref, h_ref, lhs, bias, p_ref):
    units = h_ref.shape[0]

    def step(t, carry):
        out = jnp.dot(lhs[...], s_ref[:, cols(t)], preferred_element_type=F32)
        proj = out[:units] + out[units:] + bias
        p_ref[pl.ds(t, 1), :TILE] = jnp.sum(h_ref[:, cols(t)] * proj, axis=0, keepdims=True)
        return carry

    lax.fori_loop(0, s_ref.shape[1] // TILE, step, 0)


def set_block(lhs, b, x):
    units = x.shape[0]
    hi, lo = split_terms(x)
    lhs[:units, b * 128 : (b + 1) * 128] = hi
    lhs[units:, b * 128 : (b + 1) * 128] = lo


def my_rows(pos_ref, ref, units):
    return ref[pl.ds(pos_ref[32] * (units // 128), units // 128), :]


def first_kernel(pos_ref, s_ref, h_ref, f0, f1, f2, f3, fb_ref, p_ref, lhs):
    units = h_ref.shape[0]
    norm = jnp.zeros((units, 128), F32)
    for b in range(NB):
        x = (f0, f1, f2, f3)[b // 2][b % 2]
        set_block(lhs, b, x)
        norm = norm + x * x
    fb = my_rows(pos_ref, fb_ref, units)
    p_ref[:, TILE:] = jnp.zeros((p_ref.shape[0], EXTRA), F32)
    p_ref[0:1, TILE:] = total(norm) + total(fb * fb)
    project(s_ref, h_ref, lhs, rows_to_column(fb), p_ref)


def first_pass(pos, spins, hidden, f, fb):
    units, n = hidden.shape
    return call(
        first_kernel,
        [SMEM] + [VMEM] * 7,
        [jax.ShapeDtypeStruct((n // TILE, TILE + EXTRA), F32)],
        [pltpu.VMEM((2 * units, NB * 128), BF16)],
        flops=4 * 10**9,
        name="first_pass",
    )(pos, resident(spins), resident(hidden), *f, fb)[0]


def step_of(norm, spread, samples, length):
    return norm / (spread / samples + LAM * length)


def second_kernel(samples, pos_ref, s_ref, h_ref, f0, f1, f2, f3, fb_ref, g0, g1, st_ref, norm_ref, p_ref, lhs):
    units = h_ref.shape[0]
    norm0 = norm_ref[0:1, :]
    a = step_of(norm0, st_ref[1:2, :], samples, norm0)
    rr = jnp.zeros((units, 128), F32)
    rf = jnp.zeros((units, 128), F32)
    for b in range(NB):
        f = (f0, f1, f2, f3)[b // 2][b % 2]
        g = (g0, g1)[b // 4][pos_ref[33 + b % 4], :units, :]
        r = f - a * (g + LAM * f)
        set_block(lhs, b, r)
        rr = rr + r * r
        rf = rf + r * f
    fb = my_rows(pos_ref, fb_ref, units)
    rb = fb - a * (g0[0, units : units + units // 128, :] + LAM * fb)
    p_ref[:, TILE:] = jnp.zeros((p_ref.shape[0], EXTRA), F32)
    p_ref[0:1, TILE:] = total(rr) + total(rb * rb)
    p_ref[1:2, TILE:] = total(rf) + total(rb * fb)
    project(s_ref, h_ref, lhs, rows_to_column(rb), p_ref)


def second_pass(samples, pos, spins, hidden, f, fb, g0, g1, st, norm):
    units, n = hidden.shape
    return call(
        functools.partial(second_kernel, samples),
        [SMEM] + [VMEM] * 11,
        [jax.ShapeDtypeStruct((n // TILE, TILE + EXTRA), F32)],
        [pltpu.VMEM((2 * units, NB * 128), BF16)],
        flops=4 * 10**9,
        name="second_pass",
    )(pos, resident(spins), resident(hidden), *f, fb, g0, g1, st, norm)[0]


def put_stats(v, st_ref):
    mean = jnp.sum(v) / v.size
    st_ref[0:1, :] = jnp.full((1, 128), mean, F32)
    st_ref[1:2, :] = total((v - mean) ** 2)


def first_sum_kernel(got_ref, v_ref, st_ref, norm_ref):
    x = got_ref[0]
    for k in range(1, got_ref.shape[0]):
        x = x + got_ref[k]
    v = x[:, :TILE]
    v_ref[...] = v
    norm_ref[...] = x[:, TILE:]
    put_stats(v, st_ref)


def first_sum(got):
    parts = got.shape[1]
    shape = lambda *s: jax.ShapeDtypeStruct(s, F32)
    return call(first_sum_kernel, [VMEM], [shape(parts, TILE), shape(2, 128), shape(parts, EXTRA)], name="first_sum")(
        got
    )


def second_sum_kernel(got_ref, v_ref, norm_ref, st_ref, next_ref):
    x = got_ref[0]
    for k in range(1, got_ref.shape[0]):
        x = x + got_ref[k]
    next_ref[...] = x[:, TILE:]
    beta = x[0:1, TILE : TILE + 1] / norm_ref[0:1, 0:1]
    put_stats(x[:, :TILE] + beta * v_ref[...], st_ref)


def second_sum(got, values, norm):
    shape = lambda *s: jax.ShapeDtypeStruct(s, F32)
    return call(second_sum_kernel, [VMEM] * 3, [shape(2, 128), shape(got.shape[1], EXTRA)], name="second_sum")(
        got, values, norm
    )


def merged(st, count, axis):
    got = swap(st, axis)
    delta = got[0:1] - st[0:1]
    first = lax.broadcasted_iota(jnp.int32, st.shape, 0) == 0
    return jnp.where(first, 0.5 * (st + got), st + got + (0.5 * count) * delta * delta)


def over_sets(st, count):
    for axis in ("c", "zl", "xh"):
        st = merged(st, count, axis)
        count *= 2
    return st


def image_kernel(samples, pos_ref, s_ref, h_ref, v_ref, st_ref, keep_ref, send_ref, acc, lanes):
    units = h_ref.shape[0]
    mean = st_ref[0:1, 0:1]
    acc[...] = jnp.zeros(acc.shape, F32)
    lanes[...] = jnp.zeros(lanes.shape, F32)

    def step(t, carry):
        r = h_ref[:, cols(t)] * ((v_ref[pl.ds(t, 1), :] - mean) * (1.0 / samples))
        both = jnp.concatenate(split_terms(r), axis=0)
        out = lax.dot_general(both, s_ref[:, cols(t)], (((1,), (1,)), ((), ())), preferred_element_type=F32)
        acc[...] += out[:units] + out[units:]
        part = r[:, :128]
        for k in range(1, TILE // 128):
            part = part + r[:, k * 128 : (k + 1) * 128]
        lanes[...] += part
        return carry

    lax.fori_loop(0, s_ref.shape[1] // TILE, step, 0)
    bias = [
        jnp.sum(lanes[k * 128 : (k + 1) * 128, :].T, axis=0, keepdims=True) for k in range(units // 128)
    ] + [jnp.zeros((8 - units // 128, 128), F32)]
    bias = jnp.concatenate(bias, axis=0)
    for b in range(NB):
        ref = (keep_ref, send_ref)[b // 4]
        at = pos_ref[33 + b % 4]
        ref[at, :units, :] = acc[:, b * 128 : (b + 1) * 128]
        ref[at, units:, :] = bias


def image_pass(samples, pos, spins, hidden, values, st):
    units = hidden.shape[0]
    return call(
        functools.partial(image_kernel, samples),
        [SMEM] + [VMEM] * 4,
        [jax.ShapeDtypeStruct((4, units + 8, 128), F32)] * 2,
        [pltpu.VMEM((units, NB * 128), F32), pltpu.VMEM((units, 128), F32)],
        flops=4 * 10**9,
        name="image_pass",
    )(pos, resident(spins), resident(hidden), values, st)


def update_kernel(samples, f_ref, fb_ref, g_ref, st0_ref, norm_ref, st1_ref, next_ref, w_ref, b_ref):
    norm0, norm1 = norm_ref[0:1, 0:1], next_ref[0:1, 0:1]
    cross = next_ref[1:2, 0:1]
    beta = norm1 / norm0
    step0 = step_of(norm0, st0_ref[1:2, 0:1], samples, norm0)
    step1 = step_of(norm1, st1_ref[1:2, 0:1], samples, norm1 + 2.0 * beta * cross + beta * beta * norm0)

    def update(f, g):
        r = f - step0 * (g + LAM * f)
        return step0 * f + step1 * (r + beta * f)

    units = g_ref.shape[2]
    for k in range(g_ref.shape[0]):
        at = slice(k * units, (k + 1) * units)
        w_ref[:, at] = update(f_ref[:, at], g_ref[k, :ROWS, :])
        for h in range(units // 128):
            row = slice(k * (units // 128) + h, k * (units // 128) + h + 1)
            b_ref[row, :] = update(fb_ref[row, :], g_ref[k, ROWS : ROWS + 1, h * 128 : (h + 1) * 128])


def update_pass(samples, f, fb, g, st0, norm, st1, norms):
    shape = lambda s: jax.ShapeDtypeStruct(s, F32)
    return call(
        functools.partial(update_kernel, samples), [VMEM] * 7, [shape(f.shape), shape(fb.shape)], name="update_pass"
    )(f, fb, g, st0, norm, st1, norms)


def body(spins_packed, weight, hidden_bias, force_w, force_b):
    xh, zh, zl, c = (lax.axis_index(a) for a in SMP)
    parts = lax.axis_size("zh")
    summed = lax.axis_size(SUM)
    units = weight.shape[1] // parts
    samples = spins_packed.shape[1] * lax.axis_size(SMP)
    hb = hidden_bias.reshape(-1, 128)
    fb = force_b.reshape(-1, 128)

    q = jnp.arange(32, dtype=jnp.int32)
    words = (((q >> 2) & 1) ^ xh) * 16 + (q & 3) * 4 + (((q >> 3) & 1) ^ zl) * 2 + ((q >> 4) ^ c)
    k = jnp.arange(4, dtype=jnp.int32)
    blocks = ((k & 1) ^ xh) * 2 + ((k >> 1) ^ zl)
    pos = jnp.concatenate([words, zh.reshape(1), blocks])

    f_cols = force_w.reshape(ROWS, parts, units).transpose(1, 0, 2)
    f = lax.all_to_all(f_cols, "zh", 0, 0, tiled=True).reshape(parts * ROWS, units).T[None]
    f = jnp.concatenate([f, swap(f, "xh")], axis=0)
    f_zl = swap(f, "zl")
    f = (f, f_zl, swap(f, "c"), swap(f_zl, "c"))

    packed = to_all(spins_packed, "zh", parts)
    w = lax.dynamic_slice_in_dim(weight, zh * units, units, 1).reshape(2, parts, 2, 2, ROWS, units)
    for dim, bit in ((0, xh), (2, zl), (3, c)):
        w = jnp.where(bit == 1, jnp.flip(w, dim), w)
    wt = w.transpose(3, 2, 0, 1, 4, 5).reshape(NB * 128, units).T

    spins, hidden = hidden_pass(pos, packed, wt, hb)
    partial = first_pass(pos, spins, hidden, f, fb)
    values, st, norm = first_sum(to_all(partial, SUM, summed))
    n = values.size
    st0 = over_sets(st, n)

    keep, send = image_pass(samples, pos, spins, hidden, values, st0)
    g = keep + swap(send, "c")
    g = lax.all_to_all(g, QUAD, 0, 0, tiled=True).sum(axis=0)
    g_mine = g[:units].T.reshape(parts, ROWS, units)
    gb = jnp.broadcast_to(g[units : units + units // 128].reshape(1, 1, units), (parts, 8, units))
    g_mine = lax.all_to_all(jnp.concatenate([g_mine, gb], axis=1), "zh", 0, 0, tiled=True)
    g = to_all(g, QUAD, 4)

    partial = second_pass(samples, pos, spins, hidden, f, fb, g, swap(g, "c"), st0, norm)
    st, norms = second_sum(to_all(partial, SUM, summed), values, norm)
    st1 = over_sets(st, n)
    out_w, out_b = update_pass(samples, force_w, fb, g_mine, st0, norm, st1, norms)
    return out_w, out_b.reshape(-1)


def solution(mesh):
    torus = Mesh(mesh.devices.reshape(2, 4, 2, 4, 2, 2), ("xl", "y", "xh", "zh", "zl", "c"))
    in_specs = (P(None, SMP), P(None, GRP), P(GRP), P(SMP, GRP), P(GRP))
    out_specs = (P(SMP, GRP), P(GRP))
    return jax.shard_map(body, mesh=torus, in_specs=in_specs, out_specs=out_specs, check_vma=False)
```

```python
import functools

import jax
import jax.numpy as jnp
from jax import lax
from jax.experimental import pallas as pl
from jax.experimental.pallas import tpu as pltpu
from jax.sharding import Mesh
from jax.sharding import PartitionSpec as P


GRP = ("xl", "y")
SMP = ("xh", "zh", "zl", "c")
SUM = ("zh", "xl", "y")
QUAD = ("xh", "zl")
SWAP = [(0, 1), (1, 0)]
LAM = 0.01
ROWS = 32
NB = 8
TILE = 1024
LIMIT = 14
EXTRA = 128
F32, BF16 = jnp.float32, jnp.bfloat16
VMEM = pl.BlockSpec(memory_space=pltpu.VMEM)
SMEM = pl.BlockSpec(memory_space=pltpu.SMEM)


def swap(x, axis):
    return lax.ppermute(x, axis, SWAP)


def to_all(x, axes, size):
    return lax.all_to_all(jnp.broadcast_to(x[None], (size, *x.shape)), axes, 0, 0, tiled=True)


def split_terms(x):
    hi = x.astype(BF16)
    return hi, (x - hi.astype(F32)).astype(BF16)


def resident(x):
    return pltpu.with_memory_space_constraint(x, pltpu.VMEM)


def call(kernel, ins, outs, scratch=(), flops=0):
    return pl.pallas_call(
        kernel,
        in_specs=ins,
        out_specs=[VMEM] * len(outs),
        out_shape=outs,
        scratch_shapes=scratch,
        compiler_params=pltpu.CompilerParams(vmem_limit_bytes=LIMIT << 20),
        cost_estimate=pl.CostEstimate(flops=flops, bytes_accessed=1 << 20, transcendentals=0),
    )


def cols(t):
    return pl.ds(pl.multiple_of(t * TILE, TILE), TILE)


def rows_to_column(rows):
    return jnp.concatenate(
        [jnp.broadcast_to(rows[k : k + 1, :], (128, 128)).T[:, :1] for k in range(rows.shape[0])], axis=0
    )


def total(x):
    return jnp.full((1, EXTRA), jnp.sum(x), F32)


def hidden_kernel(pos_ref, packed_ref, w_ref, hb_ref, s_ref, h_ref, wt):
    units = wt.shape[0]
    mine = pl.ds(pl.multiple_of(pos_ref[32] * units, units), units)
    for b in range(NB):
        rows = [w_ref[pl.ds(pl.multiple_of(pos_ref[4 * b + k] * ROWS, ROWS), ROWS), mine] for k in range(4)]
        block = jnp.concatenate(rows, axis=0).astype(F32)
        wt[:, b * 128 : (b + 1) * 128] = block.T.astype(BF16)
    shifts = 31 - lax.broadcasted_iota(jnp.int32, (ROWS, TILE), 0)
    hb = rows_to_column(my_rows(pos_ref, hb_ref, units))

    def step(t, carry):
        for q in range(32):
            word = packed_ref[t, pl.ds(pos_ref[q], 1), :]
            up = jnp.left_shift(jnp.broadcast_to(word, (ROWS, TILE)), shifts) < 0
            s_ref[q * ROWS : (q + 1) * ROWS, cols(t)] = jnp.where(up, 1.0, -1.0).astype(BF16)
        pre = jnp.dot(wt[...], s_ref[:, cols(t)], preferred_element_type=F32)
        h_ref[:, cols(t)] = jnp.tanh(pre + hb)
        return carry

    lax.fori_loop(0, packed_ref.shape[0], step, 0)


def hidden_pass(pos, packed, w, hb, units):
    n = packed.shape[0] * TILE
    return call(
        hidden_kernel,
        [SMEM, VMEM, VMEM, VMEM],
        [pltpu.VMEM((NB * 128, n), BF16), pltpu.VMEM((units, n), F32)],
        [pltpu.VMEM((units, NB * 128), BF16)],
        flops=4 * 10**9,
    )(pos, packed, w, hb)


def project(s_ref, h_ref, lhs, bias, p_ref):
    units = h_ref.shape[0]

    def step(t, carry):
        out = jnp.dot(lhs[...], s_ref[:, cols(t)], preferred_element_type=F32)
        proj = out[:units] + out[units:] + bias
        p_ref[pl.ds(t, 1), :TILE] = jnp.sum(h_ref[:, cols(t)] * proj, axis=0, keepdims=True)
        return carry

    lax.fori_loop(0, s_ref.shape[1] // TILE, step, 0)


def set_block(lhs, b, x):
    units = x.shape[0]
    hi, lo = split_terms(x)
    lhs[:units, b * 128 : (b + 1) * 128] = hi
    lhs[units:, b * 128 : (b + 1) * 128] = lo


def my_rows(pos_ref, ref, units):
    return ref[pl.ds(pos_ref[32] * (units // 128), units // 128), :]


def first_kernel(pos_ref, s_ref, h_ref, f0, f1, f2, f3, fb_ref, p_ref, lhs):
    units = h_ref.shape[0]
    norm = jnp.zeros((units, 128), F32)
    for b in range(NB):
        x = (f0, f1, f2, f3)[b // 2][b % 2]
        set_block(lhs, b, x)
        norm = norm + x * x
    fb = my_rows(pos_ref, fb_ref, units)
    p_ref[:, TILE:] = jnp.zeros((p_ref.shape[0], EXTRA), F32)
    p_ref[0:1, TILE:] = total(norm) + total(fb * fb)
    project(s_ref, h_ref, lhs, rows_to_column(fb), p_ref)


def first_pass(pos, spins, hidden, f, fb):
    units, n = hidden.shape
    return call(
        first_kernel,
        [SMEM] + [VMEM] * 7,
        [jax.ShapeDtypeStruct((n // TILE, TILE + EXTRA), F32)],
        [pltpu.VMEM((2 * units, NB * 128), BF16)],
        flops=4 * 10**9,
    )(pos, resident(spins), resident(hidden), *f, fb)[0]


def step_of(norm, spread, samples, length):
    return norm / (spread / samples + LAM * length)


def second_kernel(samples, pos_ref, s_ref, h_ref, f0, f1, f2, f3, fb_ref, g0, g1, st_ref, norm_ref, p_ref, lhs):
    units = h_ref.shape[0]
    norm0 = norm_ref[0:1, :]
    a = step_of(norm0, st_ref[1:2, :], samples, norm0)
    rr = jnp.zeros((units, 128), F32)
    rf = jnp.zeros((units, 128), F32)
    for b in range(NB):
        f = (f0, f1, f2, f3)[b // 2][b % 2]
        g = (g0, g1)[b // 4][pos_ref[33 + b % 4], :units, :]
        r = f - a * (g + LAM * f)
        set_block(lhs, b, r)
        rr = rr + r * r
        rf = rf + r * f
    fb = my_rows(pos_ref, fb_ref, units)
    rb = fb - a * (g0[0, units : units + units // 128, :] + LAM * fb)
    p_ref[:, TILE:] = jnp.zeros((p_ref.shape[0], EXTRA), F32)
    p_ref[0:1, TILE:] = total(rr) + total(rb * rb)
    p_ref[1:2, TILE:] = total(rf) + total(rb * fb)
    project(s_ref, h_ref, lhs, rows_to_column(rb), p_ref)


def second_pass(samples, pos, spins, hidden, f, fb, g0, g1, st, norm):
    units, n = hidden.shape
    return call(
        functools.partial(second_kernel, samples),
        [SMEM] + [VMEM] * 11,
        [jax.ShapeDtypeStruct((n // TILE, TILE + EXTRA), F32)],
        [pltpu.VMEM((2 * units, NB * 128), BF16)],
        flops=4 * 10**9,
    )(pos, resident(spins), resident(hidden), *f, fb, g0, g1, st, norm)[0]


def put_stats(v, st_ref):
    mean = jnp.sum(v) / v.size
    st_ref[0:1, :] = jnp.full((1, 128), mean, F32)
    st_ref[1:2, :] = total((v - mean) ** 2)


def first_sum_kernel(got_ref, v_ref, st_ref, norm_ref):
    x = got_ref[0]
    for k in range(1, got_ref.shape[0]):
        x = x + got_ref[k]
    v = x[:, :TILE]
    v_ref[...] = v
    norm_ref[...] = x[:, TILE:]
    put_stats(v, st_ref)


def first_sum(got):
    parts = got.shape[1]
    shape = lambda *s: jax.ShapeDtypeStruct(s, F32)
    return call(first_sum_kernel, [VMEM], [shape(parts, TILE), shape(2, 128), shape(parts, EXTRA)])(got)


def second_sum_kernel(got_ref, v_ref, norm_ref, st_ref, next_ref):
    x = got_ref[0]
    for k in range(1, got_ref.shape[0]):
        x = x + got_ref[k]
    next_ref[...] = x[:, TILE:]
    beta = x[0:1, TILE : TILE + 1] / norm_ref[0:1, 0:1]
    put_stats(x[:, :TILE] + beta * v_ref[...], st_ref)


def second_sum(got, values, norm):
    shape = lambda *s: jax.ShapeDtypeStruct(s, F32)
    return call(second_sum_kernel, [VMEM] * 3, [shape(2, 128), shape(got.shape[1], EXTRA)])(got, values, norm)


def merged(st, count, axis):
    got = swap(st, axis)
    delta = got[0:1] - st[0:1]
    first = lax.broadcasted_iota(jnp.int32, st.shape, 0) == 0
    return jnp.where(first, 0.5 * (st + got), st + got + (0.5 * count) * delta * delta)


def over_sets(st, count):
    for axis in ("c", "zl", "xh"):
        st = merged(st, count, axis)
        count *= 2
    return st


def image_kernel(samples, pos_ref, s_ref, h_ref, v_ref, st_ref, keep_ref, send_ref, acc, lanes):
    units = h_ref.shape[0]
    mean = st_ref[0:1, 0:1]
    acc[...] = jnp.zeros(acc.shape, F32)
    lanes[...] = jnp.zeros(lanes.shape, F32)

    def step(t, carry):
        r = h_ref[:, cols(t)] * ((v_ref[pl.ds(t, 1), :] - mean) * (1.0 / samples))
        both = jnp.concatenate(split_terms(r), axis=0)
        out = lax.dot_general(both, s_ref[:, cols(t)], (((1,), (1,)), ((), ())), preferred_element_type=F32)
        acc[...] += out[:units] + out[units:]
        part = r[:, :128]
        for k in range(1, TILE // 128):
            part = part + r[:, k * 128 : (k + 1) * 128]
        lanes[...] += part
        return carry

    lax.fori_loop(0, s_ref.shape[1] // TILE, step, 0)
    bias = [
        jnp.sum(lanes[k * 128 : (k + 1) * 128, :].T, axis=0, keepdims=True) for k in range(units // 128)
    ] + [jnp.zeros((8 - units // 128, 128), F32)]
    bias = jnp.concatenate(bias, axis=0)
    for b in range(NB):
        ref = (keep_ref, send_ref)[b // 4]
        at = pos_ref[33 + b % 4]
        ref[at, :units, :] = acc[:, b * 128 : (b + 1) * 128]
        ref[at, units:, :] = bias


def image_pass(samples, pos, spins, hidden, values, st):
    units = hidden.shape[0]
    return call(
        functools.partial(image_kernel, samples),
        [SMEM] + [VMEM] * 4,
        [jax.ShapeDtypeStruct((4, units + 8, 128), F32)] * 2,
        [pltpu.VMEM((units, NB * 128), F32), pltpu.VMEM((units, 128), F32)],
        flops=4 * 10**9,
    )(pos, resident(spins), resident(hidden), values, st)


def image_sum_kernel(pos_ref, got_ref, all_ref, r0, r1, r2, r3, turned):
    units = r0.shape[1]
    x = got_ref[0] + got_ref[1] + (got_ref[2] + got_ref[3])
    for k in range(4):
        all_ref[k] = x
    turned[...] = x[:units].T
    bias = jnp.concatenate([x[units + k : units + k + 1, :] for k in range(units // 128)], axis=1)
    for d, ref in enumerate((r0, r1, r2, r3)):
        to = (pos_ref[32] + d) % 4
        ref[:ROWS, :] = turned[pl.ds(pl.multiple_of(to * ROWS, ROWS), ROWS), :]
        ref[ROWS:, :] = jnp.broadcast_to(bias, (ref.shape[0] - ROWS, units))


def image_sum(pos, got, units):
    shape = lambda *s: jax.ShapeDtypeStruct(s, F32)
    return call(
        image_sum_kernel,
        [SMEM, VMEM],
        [shape(*got.shape)] + [shape(ROWS + 8, units)] * 4,
        [pltpu.VMEM((128, units), F32)],
    )(pos, got)


def update_kernel(samples, pos_ref, f_ref, fb_ref, g0, g1, g2, g3, st0_ref, norm_ref, st1_ref, next_ref, w_ref, b_ref):
    norm0, norm1 = norm_ref[0:1, 0:1], next_ref[0:1, 0:1]
    cross = next_ref[1:2, 0:1]
    beta = norm1 / norm0
    step0 = step_of(norm0, st0_ref[1:2, 0:1], samples, norm0)
    step1 = step_of(norm1, st1_ref[1:2, 0:1], samples, norm1 + 2.0 * beta * cross + beta * beta * norm0)

    def update(f, g):
        r = f - step0 * (g + LAM * f)
        return step0 * f + step1 * (r + beta * f)

    units = g0.shape[1]
    for d, g_ref in enumerate((g0, g1, g2, g3)):
        source = (pos_ref[32] + 4 - d) % 4
        at = pl.ds(pl.multiple_of(source * units, units), units)
        w_ref[:, at] = update(f_ref[:, at], g_ref[:ROWS, :])
        for h in range(units // 128):
            row = pl.ds(source * (units // 128) + h, 1)
            b_ref[row, :] = update(fb_ref[row, :], g_ref[ROWS : ROWS + 1, h * 128 : (h + 1) * 128])


def update_pass(samples, pos, f, fb, g, st0, norm, st1, norms):
    shape = lambda s: jax.ShapeDtypeStruct(s, F32)
    return call(
        functools.partial(update_kernel, samples), [SMEM] + [VMEM] * 10, [shape(f.shape), shape(fb.shape)]
    )(pos, f, fb, *g, st0, norm, st1, norms)


def body(spins_packed, weight, hidden_bias, force_w, force_b):
    xh, zh, zl, c = (lax.axis_index(a) for a in SMP)
    parts = lax.axis_size("zh")
    summed = lax.axis_size(SUM)
    units = weight.shape[1] // parts
    samples = spins_packed.shape[1] * lax.axis_size(SMP)
    hb = hidden_bias.reshape(-1, 128)
    fb = force_b.reshape(-1, 128)

    q = jnp.arange(32, dtype=jnp.int32)
    words = (((q >> 2) & 1) ^ xh) * 16 + (q & 3) * 4 + (((q >> 3) & 1) ^ zl) * 2 + ((q >> 4) ^ c)
    k = jnp.arange(4, dtype=jnp.int32)
    blocks = ((k & 1) ^ xh) * 2 + ((k >> 1) ^ zl)
    pos = jnp.concatenate([words, zh.reshape(1), blocks])

    f_cols = jnp.stack([force_w[:, k * units : (k + 1) * units] for k in range(parts)])
    f = lax.all_to_all(f_cols, "zh", 0, 0, tiled=True).reshape(parts * ROWS, units).T[None]
    f = jnp.concatenate([f, swap(f, "xh")], axis=0)
    f_zl = swap(f, "zl")
    f = (f, f_zl, swap(f, "c"), swap(f_zl, "c"))

    packed = to_all(spins_packed, "zh", parts)
    spins, hidden = hidden_pass(pos, packed, weight, hb, units)
    partial = first_pass(pos, spins, hidden, f, fb)
    values, st, norm = first_sum(to_all(partial, SUM, summed))
    n = values.size
    st0 = over_sets(st, n)

    keep, send = image_pass(samples, pos, spins, hidden, values, st0)
    g = keep + swap(send, "c")
    g, *rows = image_sum(pos, lax.all_to_all(g, QUAD, 0, 0, tiled=True), units)
    rows = [rows[0]] + [lax.ppermute(rows[d], "zh", [(i, (i + d) % 4) for i in range(4)]) for d in (1, 2, 3)]
    g = lax.all_to_all(g, QUAD, 0, 0, tiled=True)

    partial = second_pass(samples, pos, spins, hidden, f, fb, g, swap(g, "c"), st0, norm)
    st, norms = second_sum(to_all(partial, SUM, summed), values, norm)
    st1 = over_sets(st, n)
    out_w, out_b = update_pass(samples, pos, force_w, fb, rows, st0, norm, st1, norms)
    return out_w, out_b.reshape(-1)


def solution(mesh):
    torus = Mesh(mesh.devices.reshape(2, 4, 2, 4, 2, 2), ("xl", "y", "xh", "zh", "zl", "c"))
    in_specs = (P(None, SMP), P(None, GRP), P(GRP), P(SMP, GRP), P(GRP))
    out_specs = (P(SMP, GRP), P(GRP))
    return jax.shard_map(body, mesh=torus, in_specs=in_specs, out_specs=out_specs, check_vma=False)
```

```python
import functools

import jax
import jax.numpy as jnp
from jax import lax
from jax.experimental import pallas as pl
from jax.experimental.pallas import tpu as pltpu
from jax.sharding import Mesh
from jax.sharding import PartitionSpec as P


GRP = ("xl", "y")
SMP = ("xh", "zh", "zl", "c")
QUAD = ("xh", "zl")
SWAP = [(0, 1), (1, 0)]
LAM = 0.01
ROWS = 32
NB = 8
TILE = 1024
LIMIT = 14
EXTRA = 128
F32, BF16 = jnp.float32, jnp.bfloat16
VMEM = pl.BlockSpec(memory_space=pltpu.VMEM)
SMEM = pl.BlockSpec(memory_space=pltpu.SMEM)


def swap(x, axis):
    return lax.ppermute(x, axis, SWAP)


def to_all(x, axes, size):
    return lax.all_to_all(jnp.broadcast_to(x[None], (size, *x.shape)), axes, 0, 0, tiled=True)


def split_terms(x):
    hi = x.astype(BF16)
    return hi, (x - hi.astype(F32)).astype(BF16)


def resident(x):
    return pltpu.with_memory_space_constraint(x, pltpu.VMEM)


def call(kernel, ins, outs, scratch=(), flops=0):
    return pl.pallas_call(
        kernel,
        in_specs=ins,
        out_specs=[VMEM] * len(outs),
        out_shape=outs,
        scratch_shapes=scratch,
        compiler_params=pltpu.CompilerParams(vmem_limit_bytes=LIMIT << 20),
        cost_estimate=pl.CostEstimate(flops=flops, bytes_accessed=1 << 20, transcendentals=0),
    )


def cols(t):
    return pl.ds(pl.multiple_of(t * TILE, TILE), TILE)


def rows_to_column(rows):
    return jnp.concatenate(
        [jnp.broadcast_to(rows[k : k + 1, :], (128, 128)).T[:, :1] for k in range(rows.shape[0])], axis=0
    )


def total(x):
    return jnp.full((1, EXTRA), jnp.sum(x), F32)


def hidden_kernel(pos_ref, packed_ref, w_ref, hb_ref, s_ref, h_ref, wt):
    units = wt.shape[0]
    mine = pl.ds(pl.multiple_of(pos_ref[32] * units, units), units)
    for b in range(NB):
        rows = [w_ref[pl.ds(pl.multiple_of(pos_ref[4 * b + k] * ROWS, ROWS), ROWS), mine] for k in range(4)]
        block = jnp.concatenate(rows, axis=0).astype(F32)
        wt[:, b * 128 : (b + 1) * 128] = block.T.astype(BF16)
    shifts = 31 - lax.broadcasted_iota(jnp.int32, (ROWS, TILE), 0)
    hb = rows_to_column(my_rows(pos_ref, hb_ref, units))

    def step(t, carry):
        for q in range(32):
            word = packed_ref[t, pl.ds(pos_ref[q], 1), :]
            up = jnp.left_shift(jnp.broadcast_to(word, (ROWS, TILE)), shifts) < 0
            s_ref[q * ROWS : (q + 1) * ROWS, cols(t)] = jnp.where(up, 1.0, -1.0).astype(BF16)
        pre = jnp.dot(wt[...], s_ref[:, cols(t)], preferred_element_type=F32)
        h_ref[:, cols(t)] = jnp.tanh(pre + hb)
        return carry

    lax.fori_loop(0, packed_ref.shape[0], step, 0)


def hidden_pass(pos, packed, w, hb, units):
    n = packed.shape[0] * TILE
    return call(
        hidden_kernel,
        [SMEM, VMEM, VMEM, VMEM],
        [pltpu.VMEM((NB * 128, n), BF16), pltpu.VMEM((units, n), F32)],
        [pltpu.VMEM((units, NB * 128), BF16)],
        flops=4 * 10**9,
    )(pos, packed, w, hb)


def project(s_ref, h_ref, lhs, bias, p_ref):
    units = h_ref.shape[0]

    def step(t, carry):
        out = jnp.dot(lhs[...], s_ref[:, cols(t)], preferred_element_type=F32)
        proj = out[:units] + out[units:] + bias
        p_ref[pl.ds(t, 1), :TILE] = jnp.sum(h_ref[:, cols(t)] * proj, axis=0, keepdims=True)
        return carry

    lax.fori_loop(0, s_ref.shape[1] // TILE, step, 0)


def set_block(lhs, b, x):
    units = x.shape[0]
    hi, lo = split_terms(x)
    lhs[:units, b * 128 : (b + 1) * 128] = hi
    lhs[units:, b * 128 : (b + 1) * 128] = lo


def my_rows(pos_ref, ref, units):
    return ref[pl.ds(pos_ref[32] * (units // 128), units // 128), :]


def first_kernel(pos_ref, s_ref, h_ref, f0, f1, f2, f3, fb_ref, p_ref, lhs):
    units = h_ref.shape[0]
    norm = jnp.zeros((units, 128), F32)
    for b in range(NB):
        x = (f0, f1, f2, f3)[b // 2][b % 2]
        set_block(lhs, b, x)
        norm = norm + x * x
    fb = my_rows(pos_ref, fb_ref, units)
    p_ref[:, TILE:] = jnp.zeros((p_ref.shape[0], EXTRA), F32)
    p_ref[0:1, TILE:] = total(norm) + total(fb * fb)
    project(s_ref, h_ref, lhs, rows_to_column(fb), p_ref)


def first_pass(pos, spins, hidden, f, fb):
    units, n = hidden.shape
    return call(
        first_kernel,
        [SMEM] + [VMEM] * 7,
        [jax.ShapeDtypeStruct((n // TILE, TILE + EXTRA), F32)],
        [pltpu.VMEM((2 * units, NB * 128), BF16)],
        flops=4 * 10**9,
    )(pos, resident(spins), resident(hidden), *f, fb)[0]


def step_of(norm, spread, samples, length):
    return norm / (spread / samples + LAM * length)


def second_kernel(samples, pos_ref, s_ref, h_ref, f0, f1, f2, f3, fb_ref, g0, g1, st_ref, norm_ref, p_ref, lhs):
    units = h_ref.shape[0]
    norm0 = norm_ref[0:1, :]
    a = step_of(norm0, st_ref[1:2, :], samples, norm0)
    rr = jnp.zeros((units, 128), F32)
    rf = jnp.zeros((units, 128), F32)
    for b in range(NB):
        f = (f0, f1, f2, f3)[b // 2][b % 2]
        g = (g0, g1)[b // 4][pos_ref[33 + b % 4], :units, :]
        r = f - a * (g + LAM * f)
        set_block(lhs, b, r)
        rr = rr + r * r
        rf = rf + r * f
    fb = my_rows(pos_ref, fb_ref, units)
    rb = fb - a * (g0[0, units : units + units // 128, :] + LAM * fb)
    p_ref[:, TILE:] = jnp.zeros((p_ref.shape[0], EXTRA), F32)
    p_ref[0:1, TILE:] = total(rr) + total(rb * rb)
    p_ref[1:2, TILE:] = total(rf) + total(rb * fb)
    project(s_ref, h_ref, lhs, rows_to_column(rb), p_ref)


def second_pass(samples, pos, spins, hidden, f, fb, g0, g1, st, norm):
    units, n = hidden.shape
    return call(
        functools.partial(second_kernel, samples),
        [SMEM] + [VMEM] * 11,
        [jax.ShapeDtypeStruct((n // TILE, TILE + EXTRA), F32)],
        [pltpu.VMEM((2 * units, NB * 128), BF16)],
        flops=4 * 10**9,
    )(pos, resident(spins), resident(hidden), *f, fb, g0, g1, st, norm)[0]


def put_stats(v, st_ref):
    mean = jnp.sum(v) / v.size
    st_ref[0:1, :] = jnp.full((1, 128), mean, F32)
    st_ref[1:2, :] = total((v - mean) ** 2)


def over_chain_kernel(got_ref, all_ref):
    x = got_ref[0]
    for k in range(1, got_ref.shape[0]):
        x = x + got_ref[k]
    for k in range(all_ref.shape[0]):
        all_ref[k] = x


def over_groups(partial):
    got = to_all(partial, "zh", lax.axis_size("zh"))
    size = lax.axis_size(GRP)
    (x,) = call(over_chain_kernel, [VMEM], [jax.ShapeDtypeStruct((size, *partial.shape), F32)])(got)
    return lax.all_to_all(x, GRP, 0, 0, tiled=True)


def first_sum_kernel(got_ref, v_ref, st_ref, norm_ref):
    x = got_ref[0]
    for k in range(1, got_ref.shape[0]):
        x = x + got_ref[k]
    v = x[:, :TILE]
    v_ref[...] = v
    norm_ref[...] = x[:, TILE:]
    put_stats(v, st_ref)


def first_sum(got):
    parts = got.shape[1]
    shape = lambda *s: jax.ShapeDtypeStruct(s, F32)
    return call(first_sum_kernel, [VMEM], [shape(parts, TILE), shape(2, 128), shape(parts, EXTRA)])(got)


def second_sum_kernel(got_ref, v_ref, norm_ref, st_ref, next_ref):
    x = got_ref[0]
    for k in range(1, got_ref.shape[0]):
        x = x + got_ref[k]
    next_ref[...] = x[:, TILE:]
    beta = x[0:1, TILE : TILE + 1] / norm_ref[0:1, 0:1]
    put_stats(x[:, :TILE] + beta * v_ref[...], st_ref)


def second_sum(got, values, norm):
    shape = lambda *s: jax.ShapeDtypeStruct(s, F32)
    return call(second_sum_kernel, [VMEM] * 3, [shape(2, 128), shape(got.shape[1], EXTRA)])(got, values, norm)


def merged(st, count, axis):
    got = swap(st, axis)
    delta = got[0:1] - st[0:1]
    first = lax.broadcasted_iota(jnp.int32, st.shape, 0) == 0
    return jnp.where(first, 0.5 * (st + got), st + got + (0.5 * count) * delta * delta)


def over_sets(st, count):
    for axis in ("c", "zl", "xh"):
        st = merged(st, count, axis)
        count *= 2
    return st


def image_kernel(samples, pos_ref, s_ref, h_ref, v_ref, st_ref, keep_ref, send_ref, acc, lanes):
    units = h_ref.shape[0]
    mean = st_ref[0:1, 0:1]
    acc[...] = jnp.zeros(acc.shape, F32)
    lanes[...] = jnp.zeros(lanes.shape, F32)

    def step(t, carry):
        r = h_ref[:, cols(t)] * ((v_ref[pl.ds(t, 1), :] - mean) * (1.0 / samples))
        both = jnp.concatenate(split_terms(r), axis=0)
        out = lax.dot_general(both, s_ref[:, cols(t)], (((1,), (1,)), ((), ())), preferred_element_type=F32)
        acc[...] += out[:units] + out[units:]
        part = r[:, :128]
        for k in range(1, TILE // 128):
            part = part + r[:, k * 128 : (k + 1) * 128]
        lanes[...] += part
        return carry

    lax.fori_loop(0, s_ref.shape[1] // TILE, step, 0)
    bias = [
        jnp.sum(lanes[k * 128 : (k + 1) * 128, :].T, axis=0, keepdims=True) for k in range(units // 128)
    ] + [jnp.zeros((8 - units // 128, 128), F32)]
    bias = jnp.concatenate(bias, axis=0)
    for b in range(NB):
        ref = (keep_ref, send_ref)[b // 4]
        at = pos_ref[33 + b % 4]
        ref[at, :units, :] = acc[:, b * 128 : (b + 1) * 128]
        ref[at, units:, :] = bias


def image_pass(samples, pos, spins, hidden, values, st):
    units = hidden.shape[0]
    return call(
        functools.partial(image_kernel, samples),
        [SMEM] + [VMEM] * 4,
        [jax.ShapeDtypeStruct((4, units + 8, 128), F32)] * 2,
        [pltpu.VMEM((units, NB * 128), F32), pltpu.VMEM((units, 128), F32)],
        flops=4 * 10**9,
    )(pos, resident(spins), resident(hidden), values, st)


def image_sum_kernel(pos_ref, got_ref, all_ref, r0, r1, r2, r3, turned):
    units = r0.shape[1]
    x = got_ref[0] + got_ref[1] + (got_ref[2] + got_ref[3])
    for k in range(4):
        all_ref[k] = x
    turned[...] = x[:units].T
    bias = jnp.concatenate([x[units + k : units + k + 1, :] for k in range(units // 128)], axis=1)
    for d, ref in enumerate((r0, r1, r2, r3)):
        to = (pos_ref[32] + d) % 4
        ref[:ROWS, :] = turned[pl.ds(pl.multiple_of(to * ROWS, ROWS), ROWS), :]
        ref[ROWS:, :] = jnp.broadcast_to(bias, (ref.shape[0] - ROWS, units))


def image_sum(pos, got, units):
    shape = lambda *s: jax.ShapeDtypeStruct(s, F32)
    return call(
        image_sum_kernel,
        [SMEM, VMEM],
        [shape(*got.shape)] + [shape(ROWS + 8, units)] * 4,
        [pltpu.VMEM((128, units), F32)],
    )(pos, got)


def update_kernel(samples, pos_ref, f_ref, fb_ref, g0, g1, g2, g3, st0_ref, norm_ref, st1_ref, next_ref, w_ref, b_ref):
    norm0, norm1 = norm_ref[0:1, 0:1], next_ref[0:1, 0:1]
    cross = next_ref[1:2, 0:1]
    beta = norm1 / norm0
    step0 = step_of(norm0, st0_ref[1:2, 0:1], samples, norm0)
    step1 = step_of(norm1, st1_ref[1:2, 0:1], samples, norm1 + 2.0 * beta * cross + beta * beta * norm0)

    def update(f, g):
        r = f - step0 * (g + LAM * f)
        return step0 * f + step1 * (r + beta * f)

    units = g0.shape[1]
    for d, g_ref in enumerate((g0, g1, g2, g3)):
        source = (pos_ref[32] + 4 - d) % 4
        at = pl.ds(pl.multiple_of(source * units, units), units)
        w_ref[:, at] = update(f_ref[:, at], g_ref[:ROWS, :])
        for h in range(units // 128):
            row = pl.ds(source * (units // 128) + h, 1)
            b_ref[row, :] = update(fb_ref[row, :], g_ref[ROWS : ROWS + 1, h * 128 : (h + 1) * 128])


def update_pass(samples, pos, f, fb, g, st0, norm, st1, norms):
    shape = lambda s: jax.ShapeDtypeStruct(s, F32)
    return call(
        functools.partial(update_kernel, samples), [SMEM] + [VMEM] * 10, [shape(f.shape), shape(fb.shape)]
    )(pos, f, fb, *g, st0, norm, st1, norms)


def body(spins_packed, weight, hidden_bias, force_w, force_b):
    xh, zh, zl, c = (lax.axis_index(a) for a in SMP)
    parts = lax.axis_size("zh")
    units = weight.shape[1] // parts
    samples = spins_packed.shape[1] * lax.axis_size(SMP)
    hb = hidden_bias.reshape(-1, 128)
    fb = force_b.reshape(-1, 128)

    q = jnp.arange(32, dtype=jnp.int32)
    words = (((q >> 2) & 1) ^ xh) * 16 + (q & 3) * 4 + (((q >> 3) & 1) ^ zl) * 2 + ((q >> 4) ^ c)
    k = jnp.arange(4, dtype=jnp.int32)
    blocks = ((k & 1) ^ xh) * 2 + ((k >> 1) ^ zl)
    pos = jnp.concatenate([words, zh.reshape(1), blocks])

    f_cols = jnp.stack([force_w[:, k * units : (k + 1) * units] for k in range(parts)])
    f = lax.all_to_all(f_cols, "zh", 0, 0, tiled=True).reshape(parts * ROWS, units).T[None]
    f = jnp.concatenate([f, swap(f, "xh")], axis=0)
    f_zl = swap(f, "zl")
    f = (f, f_zl, swap(f, "c"), swap(f_zl, "c"))

    packed = to_all(spins_packed, "zh", parts)
    spins, hidden = hidden_pass(pos, packed, weight, hb, units)
    partial = first_pass(pos, spins, hidden, f, fb)
    values, st, norm = first_sum(over_groups(partial))
    n = values.size
    st0 = over_sets(st, n)

    keep, send = image_pass(samples, pos, spins, hidden, values, st0)
    g = keep + swap(send, "c")
    g, *rows = image_sum(pos, lax.all_to_all(g, QUAD, 0, 0, tiled=True), units)
    for d in (1, 2, 3):
        rows[d] = lax.ppermute(rows[d], "zh", [(i, (i + d) % 4) for i in range(4)])
    g = lax.all_to_all(g, QUAD, 0, 0, tiled=True)

    g_far = swap(g, "c")
    partial = second_pass(samples, pos, spins, hidden, f, fb, g, g_far, st0, norm)
    st, norms = second_sum(over_groups(partial), values, norm)
    st1 = over_sets(st, n)
    out_w, out_b = update_pass(samples, pos, force_w, fb, rows, st0, norm, st1, norms)
    return out_w, out_b.reshape(-1)


def solution(mesh):
    torus = Mesh(mesh.devices.reshape(2, 4, 2, 4, 2, 2), ("xl", "y", "xh", "zh", "zl", "c"))
    in_specs = (P(None, SMP), P(None, GRP), P(GRP), P(SMP, GRP), P(GRP))
    out_specs = (P(SMP, GRP), P(GRP))
    return jax.shard_map(body, mesh=torus, in_specs=in_specs, out_specs=out_specs, check_vma=False)
```

```python
import functools

import jax
import jax.numpy as jnp
from jax import lax
from jax.experimental import pallas as pl
from jax.experimental.pallas import tpu as pltpu
from jax.sharding import Mesh
from jax.sharding import PartitionSpec as P


GRP = ("xl", "y")
SMP = ("xh", "zh", "zl", "c")
QUAD = ("xh", "zl")
SWAP = [(0, 1), (1, 0)]
LAM = 0.01
ROWS = 32
NB = 8
TILE = 1024
LIMIT = 14
SUB = TILE // 128
EXTRA = 8
F32, BF16 = jnp.float32, jnp.bfloat16
VMEM = pl.BlockSpec(memory_space=pltpu.VMEM)
SMEM = pl.BlockSpec(memory_space=pltpu.SMEM)


def swap(x, axis):
    return lax.ppermute(x, axis, SWAP)


def to_all(x, axes, size):
    return lax.all_to_all(jnp.broadcast_to(x[None], (size, *x.shape)), axes, 0, 0, tiled=True)


def split_terms(x):
    hi = x.astype(BF16)
    return hi, (x - hi.astype(F32)).astype(BF16)


def resident(x):
    return pltpu.with_memory_space_constraint(x, pltpu.VMEM)


def call(kernel, ins, outs, scratch=(), flops=0):
    return pl.pallas_call(
        kernel,
        in_specs=ins,
        out_specs=[VMEM] * len(outs),
        out_shape=outs,
        scratch_shapes=scratch,
        compiler_params=pltpu.CompilerParams(vmem_limit_bytes=LIMIT << 20),
        cost_estimate=pl.CostEstimate(flops=flops, bytes_accessed=1 << 20, transcendentals=0),
    )


def cols(t):
    return pl.ds(pl.multiple_of(t * TILE, TILE), TILE)


def rows_to_column(rows):
    return jnp.concatenate(
        [jnp.broadcast_to(rows[k : k + 1, :], (128, 128)).T[:, :1] for k in range(rows.shape[0])], axis=0
    )


def total(x):
    return jnp.full((1, 128), jnp.sum(x), F32)


def to_rows(line):
    return jnp.concatenate([line[:, k * 128 : (k + 1) * 128] for k in range(line.shape[1] // 128)], axis=0)


def to_line(rows):
    return jnp.concatenate([rows[k : k + 1, :] for k in range(rows.shape[0])], axis=1)


def sub(t):
    return pl.ds(pl.multiple_of(t * SUB, SUB), SUB)


def hidden_kernel(pos_ref, packed_ref, w_ref, hb_ref, s_ref, h_ref, wt):
    units = wt.shape[0]
    for b in range(NB):
        rows = [w_ref[pl.ds(pl.multiple_of(pos_ref[4 * b + k] * ROWS, ROWS), ROWS), :] for k in range(4)]
        block = jnp.concatenate(rows, axis=0).astype(F32)
        wt[:, b * 128 : (b + 1) * 128] = block.T.astype(BF16)
    shifts = 31 - lax.broadcasted_iota(jnp.int32, (ROWS, TILE), 0)
    hb = rows_to_column(my_rows(pos_ref, hb_ref, units))

    def step(t, carry):
        for q in range(32):
            word = packed_ref[t, pl.ds(pos_ref[q], 1), :]
            up = jnp.left_shift(jnp.broadcast_to(word, (ROWS, TILE)), shifts) < 0
            s_ref[q * ROWS : (q + 1) * ROWS, cols(t)] = jnp.where(up, 1.0, -1.0).astype(BF16)
        pre = jnp.dot(wt[...], s_ref[:, cols(t)], preferred_element_type=F32)
        h_ref[:, cols(t)] = jnp.tanh(pre + hb)
        return carry

    lax.fori_loop(0, packed_ref.shape[0], step, 0)


def hidden_pass(pos, packed, w, hb, units):
    n = packed.shape[0] * TILE
    return call(
        hidden_kernel,
        [SMEM, VMEM, VMEM, VMEM],
        [pltpu.VMEM((NB * 128, n), BF16), pltpu.VMEM((units, n), F32)],
        [pltpu.VMEM((units, NB * 128), BF16)],
        flops=4 * 10**9,
    )(pos, packed, w, hb)


def project(s_ref, h_ref, lhs, bias, p_ref):
    units = h_ref.shape[0]

    def step(t, carry):
        out = jnp.dot(lhs[...], s_ref[:, cols(t)], preferred_element_type=F32)
        proj = out[:units] + out[units:] + bias
        p_ref[sub(t), :] = to_rows(jnp.sum(h_ref[:, cols(t)] * proj, axis=0, keepdims=True))
        return carry

    lax.fori_loop(0, s_ref.shape[1] // TILE, step, 0)


def set_block(lhs, b, x):
    units = x.shape[0]
    hi, lo = split_terms(x)
    lhs[:units, b * 128 : (b + 1) * 128] = hi
    lhs[units:, b * 128 : (b + 1) * 128] = lo


def my_rows(pos_ref, ref, units):
    return ref[pl.ds(pos_ref[32] * (units // 128), units // 128), :]


def first_kernel(pos_ref, s_ref, h_ref, f0, f1, f2, f3, fb_ref, p_ref, lhs):
    units = h_ref.shape[0]
    norm = jnp.zeros((units, 128), F32)
    for b in range(NB):
        x = (f0, f1, f2, f3)[b // 2][b % 2]
        set_block(lhs, b, x)
        norm = norm + x * x
    fb = my_rows(pos_ref, fb_ref, units)
    n = p_ref.shape[0] - EXTRA
    p_ref[n:, :] = jnp.zeros((EXTRA, 128), F32)
    p_ref[n : n + 1, :] = total(norm) + total(fb * fb)
    project(s_ref, h_ref, lhs, rows_to_column(fb), p_ref)


def first_pass(pos, spins, hidden, f, fb):
    units, n = hidden.shape
    return call(
        first_kernel,
        [SMEM] + [VMEM] * 7,
        [jax.ShapeDtypeStruct((n // 128 + EXTRA, 128), F32)],
        [pltpu.VMEM((2 * units, NB * 128), BF16)],
        flops=4 * 10**9,
    )(pos, resident(spins), resident(hidden), *f, fb)[0]


def step_of(norm, spread, samples, length):
    return norm / (spread / samples + LAM * length)


def second_kernel(samples, pos_ref, s_ref, h_ref, f0, f1, f2, f3, fb_ref, g0, g1, mine_ref, st_ref, norm_ref, out_ref, lhs):
    units = h_ref.shape[0]
    norm0 = norm_ref[0:1, :]
    a = step_of(norm0, st_ref[1:2, :], samples, norm0)
    rr = jnp.zeros((units, 128), F32)
    rf = jnp.zeros((units, 128), F32)
    for b in range(NB):
        f = (f0, f1, f2, f3)[b // 2][b % 2]
        g = (g0, g1)[b // 4][pos_ref[33 + b % 4], :units, :]
        r = f - a * (g + LAM * f)
        set_block(lhs, b, r)
        rr = rr + r * r
        rf = rf + r * f
    fb = my_rows(pos_ref, fb_ref, units)
    rb = fb - a * (g0[0, units : units + units // 128, :] + LAM * fb)
    n = h_ref.shape[1] // 128
    p_ref = out_ref.at[0]
    p_ref[n : n + EXTRA, :] = jnp.zeros((EXTRA, 128), F32)
    p_ref[n : n + 1, :] = total(rr) + total(rb * rb)
    p_ref[n + 1 : n + 2, :] = total(rf) + total(rb * fb)
    p_ref[n + 2 : n + 2 + units // 128, :] = g0[0, units : units + units // 128, :]
    project(s_ref, h_ref, lhs, rows_to_column(rb), p_ref)
    for k in range(1, out_ref.shape[0]):
        out_ref[k, : n + EXTRA, :] = out_ref[0, : n + EXTRA, :]
    for k in range(out_ref.shape[0]):
        for h in range(units // 128):
            at = n + EXTRA + h * ROWS
            out_ref[k, at : at + ROWS, :] = mine_ref[k * ROWS : (k + 1) * ROWS, h * 128 : (h + 1) * 128]


def second_pass(samples, pos, spins, hidden, f, fb, g0, g1, mine, st, norm):
    units, n = hidden.shape
    parts = mine.shape[0] // ROWS
    return call(
        functools.partial(second_kernel, samples),
        [SMEM] + [VMEM] * 12,
        [jax.ShapeDtypeStruct((parts, n // 128 + EXTRA + units // 128 * ROWS, 128), F32)],
        [pltpu.VMEM((2 * units, NB * 128), BF16)],
        flops=4 * 10**9,
    )(pos, resident(spins), resident(hidden), *f, fb, g0, g1, mine, st, norm)[0]


def put_stats(v, st_ref):
    mean = jnp.sum(v) / v.size
    st_ref[0:1, :] = jnp.full((1, 128), mean, F32)
    st_ref[1:2, :] = total((v - mean) ** 2)


def over_chain_kernel(got_ref, all_ref):
    rows = all_ref.shape[1]
    x = got_ref[0, :rows, :]
    for k in range(1, got_ref.shape[0]):
        x = x + got_ref[k, :rows, :]
    for k in range(all_ref.shape[0]):
        all_ref[k] = x


def over_groups(got, rows):
    (x,) = call(over_chain_kernel, [VMEM], [jax.ShapeDtypeStruct((lax.axis_size(GRP), rows, 128), F32)])(got)
    return lax.all_to_all(x, GRP, 0, 0, tiled=True)


def summed(got_ref):
    x = got_ref[0]
    for k in range(1, got_ref.shape[0]):
        x = x + got_ref[k]
    n = x.shape[0] - EXTRA
    return x[:n], x[n:]


def first_sum_kernel(got_ref, v_ref, st_ref, norm_ref):
    v, extra = summed(got_ref)
    v_ref[...] = v
    norm_ref[...] = extra
    put_stats(v, st_ref)


def first_sum(got):
    shape = lambda *s: jax.ShapeDtypeStruct(s, F32)
    return call(first_sum_kernel, [VMEM], [shape(got.shape[1] - EXTRA, 128), shape(2, 128), shape(EXTRA, 128)])(got)


def second_sum_kernel(got_ref, v_ref, norm_ref, st_ref, next_ref):
    u, extra = summed(got_ref)
    next_ref[...] = extra
    beta = extra[0:1, 0:1] / norm_ref[0:1, 0:1]
    put_stats(u + beta * v_ref[...], st_ref)


def second_sum(got, values, norm):
    shape = lambda *s: jax.ShapeDtypeStruct(s, F32)
    return call(second_sum_kernel, [VMEM] * 3, [shape(2, 128), shape(EXTRA, 128)])(
        got, values, norm
    )


def merged(st, count, axis):
    got = swap(st, axis)
    delta = got[0:1] - st[0:1]
    first = lax.broadcasted_iota(jnp.int32, st.shape, 0) == 0
    return jnp.where(first, 0.5 * (st + got), st + got + (0.5 * count) * delta * delta)


def over_sets(st, count):
    for axis in ("c", "zl", "xh"):
        st = merged(st, count, axis)
        count *= 2
    return st


def image_kernel(samples, pos_ref, s_ref, h_ref, v_ref, st_ref, keep_ref, send_ref, acc, lanes):
    units = h_ref.shape[0]
    mean = st_ref[0:1, 0:1]
    acc[...] = jnp.zeros(acc.shape, F32)
    lanes[...] = jnp.zeros(lanes.shape, F32)

    def step(t, carry):
        r = h_ref[:, cols(t)] * to_line((v_ref[sub(t), :] - mean) * (1.0 / samples))
        both = jnp.concatenate(split_terms(r), axis=0)
        out = lax.dot_general(both, s_ref[:, cols(t)], (((1,), (1,)), ((), ())), preferred_element_type=F32)
        acc[...] += out[:units] + out[units:]
        part = r[:, :128]
        for k in range(1, TILE // 128):
            part = part + r[:, k * 128 : (k + 1) * 128]
        lanes[...] += part
        return carry

    lax.fori_loop(0, s_ref.shape[1] // TILE, step, 0)
    bias = [
        jnp.sum(lanes[k * 128 : (k + 1) * 128, :].T, axis=0, keepdims=True) for k in range(units // 128)
    ] + [jnp.zeros((8 - units // 128, 128), F32)]
    bias = jnp.concatenate(bias, axis=0)
    for b in range(NB):
        ref = (keep_ref, send_ref)[b // 4]
        at = pos_ref[33 + b % 4]
        ref[at, :units, :] = acc[:, b * 128 : (b + 1) * 128]
        ref[at, units:, :] = bias


def image_pass(samples, pos, spins, hidden, values, st):
    units = hidden.shape[0]
    return call(
        functools.partial(image_kernel, samples),
        [SMEM] + [VMEM] * 4,
        [jax.ShapeDtypeStruct((4, units + 8, 128), F32)] * 2,
        [pltpu.VMEM((units, NB * 128), F32), pltpu.VMEM((units, 128), F32)],
        flops=4 * 10**9,
    )(pos, resident(spins), resident(hidden), values, st)


def image_sum_kernel(got_ref, all_ref, mine_ref):
    units = mine_ref.shape[1]
    x = got_ref[0] + got_ref[1] + (got_ref[2] + got_ref[3])
    for k in range(4):
        all_ref[k] = x
    mine_ref[...] = x[:units].T


def image_sum(got, units):
    shape = lambda *s: jax.ShapeDtypeStruct(s, F32)
    return call(image_sum_kernel, [VMEM], [shape(*got.shape), shape(128, units)])(got)


def update_kernel(samples, f_ref, fb_ref, got_ref, st0_ref, norm_ref, st1_ref, next_ref, w_ref, b_ref):
    norm0, norm1 = norm_ref[0:1, 0:1], next_ref[0:1, 0:1]
    cross = next_ref[1:2, 0:1]
    beta = norm1 / norm0
    step0 = step_of(norm0, st0_ref[1:2, 0:1], samples, norm0)
    step1 = step_of(norm1, st1_ref[1:2, 0:1], samples, norm1 + 2.0 * beta * cross + beta * beta * norm0)

    def update(f, g):
        r = f - step0 * (g + LAM * f)
        return step0 * f + step1 * (r + beta * f)

    parts = got_ref.shape[0]
    per = f_ref.shape[1] // 128 // parts
    n = got_ref.shape[1] - EXTRA - per * ROWS
    for k in range(parts):
        for h in range(per):
            b = k * per + h
            at = n + EXTRA + h * ROWS
            w_ref[:, b * 128 : (b + 1) * 128] = update(f_ref[:, b * 128 : (b + 1) * 128], got_ref[k, at : at + ROWS, :])
            b_ref[b : b + 1, :] = update(fb_ref[b : b + 1, :], got_ref[k, n + 2 + h : n + 3 + h, :])


def update_pass(samples, f, fb, got, st0, norm, st1, norms):
    shape = lambda s: jax.ShapeDtypeStruct(s, F32)
    return call(
        functools.partial(update_kernel, samples), [VMEM] * 7, [shape(f.shape), shape(fb.shape)]
    )(f, fb, got, st0, norm, st1, norms)


def body(spins_packed, weight, hidden_bias, force_w, force_b):
    xh, zh, zl, c = (lax.axis_index(a) for a in SMP)
    parts = lax.axis_size("zh")
    units = weight.shape[1] // parts
    samples = spins_packed.shape[1] * lax.axis_size(SMP)
    hb = hidden_bias.reshape(-1, 128)
    fb = force_b.reshape(-1, 128)

    q = jnp.arange(32, dtype=jnp.int32)
    words = (((q >> 2) & 1) ^ xh) * 16 + (q & 3) * 4 + (((q >> 3) & 1) ^ zl) * 2 + ((q >> 4) ^ c)
    k = jnp.arange(4, dtype=jnp.int32)
    blocks = ((k & 1) ^ xh) * 2 + ((k >> 1) ^ zl)
    pos = jnp.concatenate([words, zh.reshape(1), blocks])

    f_cols = jnp.stack([force_w[:, k * units : (k + 1) * units] for k in range(parts)])
    f = lax.all_to_all(f_cols, "zh", 0, 0, tiled=True)
    f = f.reshape(parts * ROWS, units).T[None]
    f_xh = swap(f, "xh")
    f = jnp.concatenate([f, f_xh], axis=0)
    f_zl = swap(f, "zl")
    f = (f, f_zl, swap(f, "c"), swap(f_zl, "c"))

    packed = to_all(spins_packed, "zh", parts)
    w = lax.dynamic_slice_in_dim(weight, zh * units, units, 1)
    spins, hidden = hidden_pass(pos, packed, w, hb, units)
    partial = first_pass(pos, spins, hidden, f, fb)
    rows = partial.shape[0]
    values, st, norm = first_sum(over_groups(to_all(partial, "zh", parts), rows))
    n = values.size
    st0 = over_sets(st, n)

    keep, send = image_pass(samples, pos, spins, hidden, values, st0)
    g = keep + swap(send, "c")
    g, mine = image_sum(lax.all_to_all(g, QUAD, 0, 0, tiled=True), units)
    g = lax.all_to_all(g, QUAD, 0, 0, tiled=True)

    partial = second_pass(samples, pos, spins, hidden, f, fb, g, swap(g, "c"), mine, st0, norm)
    got = lax.all_to_all(partial, "zh", 0, 0, tiled=True)
    st, norms = second_sum(over_groups(got, rows), values, norm)
    st1 = over_sets(st, n)
    out_w, out_b = update_pass(samples, force_w, fb, got, st0, norm, st1, norms)
    return out_w, out_b.reshape(-1)


def solution(mesh):
    torus = Mesh(mesh.devices.reshape(2, 4, 2, 4, 2, 2), ("xl", "y", "xh", "zh", "zl", "c"))
    in_specs = (P(None, SMP), P(None, GRP), P(GRP), P(SMP, GRP), P(GRP))
    out_specs = (P(SMP, GRP), P(GRP))
    return jax.shard_map(body, mesh=torus, in_specs=in_specs, out_specs=out_specs, check_vma=False)
```

```python
import functools

import jax
import jax.numpy as jnp
from jax import lax
from jax.experimental import pallas as pl
from jax.experimental.pallas import tpu as pltpu
from jax.sharding import Mesh
from jax.sharding import PartitionSpec as P


GRP = ("xl", "y")
SMP = ("xh", "zh", "zl", "c")
QUAD = ("xh", "zl")
SETS = ("xh", "zl", "c")
SWAP = [(0, 1), (1, 0)]
LAM = 0.01
ROWS = 32
NB = 8
TILE = 1024
LIMIT = 14
SUB = TILE // 128
EXTRA = 8
F32, BF16 = jnp.float32, jnp.bfloat16
VMEM = pl.BlockSpec(memory_space=pltpu.VMEM)
SMEM = pl.BlockSpec(memory_space=pltpu.SMEM)


def swap(x, axis):
    return lax.ppermute(x, axis, SWAP)


def to_all(x, axes, size):
    return lax.all_to_all(jnp.broadcast_to(x[None], (size, *x.shape)), axes, 0, 0, tiled=True)


def split_terms(x):
    hi = x.astype(BF16)
    return hi, (x - hi.astype(F32)).astype(BF16)


def resident(x):
    return pltpu.with_memory_space_constraint(x, pltpu.VMEM)


def call(kernel, ins, outs, scratch=(), flops=0):
    return pl.pallas_call(
        kernel,
        in_specs=ins,
        out_specs=[VMEM] * len(outs),
        out_shape=outs,
        scratch_shapes=scratch,
        compiler_params=pltpu.CompilerParams(vmem_limit_bytes=LIMIT << 20),
        cost_estimate=pl.CostEstimate(flops=flops, bytes_accessed=1 << 20, transcendentals=0),
    )


def cols(t):
    return pl.ds(pl.multiple_of(t * TILE, TILE), TILE)


def rows_to_column(rows):
    return jnp.concatenate(
        [jnp.broadcast_to(rows[k : k + 1, :], (128, 128)).T[:, :1] for k in range(rows.shape[0])], axis=0
    )


def total(x):
    return jnp.full((1, 128), jnp.sum(x), F32)


def to_rows(line):
    return jnp.concatenate([line[:, k * 128 : (k + 1) * 128] for k in range(line.shape[1] // 128)], axis=0)


def to_line(rows):
    return jnp.concatenate([rows[k : k + 1, :] for k in range(rows.shape[0])], axis=1)


def sub(t):
    return pl.ds(pl.multiple_of(t * SUB, SUB), SUB)


def hidden_kernel(pos_ref, packed_ref, w_ref, hb_ref, s_ref, h_ref, wt):
    units = wt.shape[0]
    for b in range(NB):
        rows = [w_ref[pl.ds(pl.multiple_of(pos_ref[4 * b + k] * ROWS, ROWS), ROWS), :] for k in range(4)]
        block = jnp.concatenate(rows, axis=0).astype(F32)
        wt[:, b * 128 : (b + 1) * 128] = block.T.astype(BF16)
    shifts = 31 - lax.broadcasted_iota(jnp.int32, (ROWS, TILE), 0)
    hb = rows_to_column(my_rows(pos_ref, hb_ref, units))

    def step(t, carry):
        for q in range(32):
            word = packed_ref[t, pl.ds(pos_ref[q], 1), :]
            up = jnp.left_shift(jnp.broadcast_to(word, (ROWS, TILE)), shifts) < 0
            s_ref[q * ROWS : (q + 1) * ROWS, cols(t)] = jnp.where(up, 1.0, -1.0).astype(BF16)
        pre = jnp.dot(wt[...], s_ref[:, cols(t)], preferred_element_type=F32)
        h_ref[:, cols(t)] = jnp.tanh(pre + hb)
        return carry

    lax.fori_loop(0, packed_ref.shape[0], step, 0)


def hidden_pass(pos, packed, w, hb, units):
    n = packed.shape[0] * TILE
    return call(
        hidden_kernel,
        [SMEM, VMEM, VMEM, VMEM],
        [pltpu.VMEM((NB * 128, n), BF16), pltpu.VMEM((units, n), F32)],
        [pltpu.VMEM((units, NB * 128), BF16)],
        flops=4 * 10**9,
    )(pos, packed, w, hb)


def project(s_ref, h_ref, lhs, bias, p_ref):
    units = h_ref.shape[0]

    def step(t, carry):
        out = jnp.dot(lhs[...], s_ref[:, cols(t)], preferred_element_type=F32)
        proj = out[:units] + out[units:] + bias
        p_ref[sub(t), :] = to_rows(jnp.sum(h_ref[:, cols(t)] * proj, axis=0, keepdims=True))
        return carry

    lax.fori_loop(0, s_ref.shape[1] // TILE, step, 0)


def set_block(lhs, b, x):
    units = x.shape[0]
    hi, lo = split_terms(x)
    lhs[:units, b * 128 : (b + 1) * 128] = hi
    lhs[units:, b * 128 : (b + 1) * 128] = lo


def my_rows(pos_ref, ref, units):
    return ref[pl.ds(pos_ref[32] * (units // 128), units // 128), :]


def first_kernel(pos_ref, s_ref, h_ref, f0, f1, f2, f3, fb_ref, p_ref, lhs):
    units = h_ref.shape[0]
    norm = jnp.zeros((units, 128), F32)
    for b in range(NB):
        x = (f0, f1, f2, f3)[b // 2][b % 2]
        set_block(lhs, b, x)
        norm = norm + x * x
    fb = my_rows(pos_ref, fb_ref, units)
    n = p_ref.shape[0] - EXTRA
    p_ref[n:, :] = jnp.zeros((EXTRA, 128), F32)
    p_ref[n : n + 1, :] = total(norm) + total(fb * fb)
    project(s_ref, h_ref, lhs, rows_to_column(fb), p_ref)


def first_pass(pos, spins, hidden, f, fb):
    units, n = hidden.shape
    return call(
        first_kernel,
        [SMEM] + [VMEM] * 7,
        [jax.ShapeDtypeStruct((n // 128 + EXTRA, 128), F32)],
        [pltpu.VMEM((2 * units, NB * 128), BF16)],
        flops=4 * 10**9,
    )(pos, resident(spins), resident(hidden), *f, fb)[0]


def step_of(norm, spread, samples, length):
    return norm / (spread / samples + LAM * length)


def second_kernel(samples, pos_ref, s_ref, h_ref, f0, f1, f2, f3, fb_ref, g0, g1, mine_ref, st_ref, norm_ref, out_ref, lhs):
    units = h_ref.shape[0]
    norm0 = norm_ref[0:1, :]
    a = step_of(norm0, joined(st_ref, h_ref.shape[1])[1], samples, norm0)
    rr = jnp.zeros((units, 128), F32)
    rf = jnp.zeros((units, 128), F32)
    for b in range(NB):
        f = (f0, f1, f2, f3)[b // 2][b % 2]
        g = (g0, g1)[b // 4][pos_ref[33 + b % 4], :units, :]
        r = f - a * (g + LAM * f)
        set_block(lhs, b, r)
        rr = rr + r * r
        rf = rf + r * f
    fb = my_rows(pos_ref, fb_ref, units)
    rb = fb - a * (g0[0, units : units + units // 128, :] + LAM * fb)
    n = h_ref.shape[1] // 128
    p_ref = out_ref.at[0]
    p_ref[n : n + EXTRA, :] = jnp.zeros((EXTRA, 128), F32)
    p_ref[n : n + 1, :] = total(rr) + total(rb * rb)
    p_ref[n + 1 : n + 2, :] = total(rf) + total(rb * fb)
    p_ref[n + 2 : n + 2 + units // 128, :] = g0[0, units : units + units // 128, :]
    project(s_ref, h_ref, lhs, rows_to_column(rb), p_ref)
    for k in range(1, out_ref.shape[0]):
        out_ref[k, : n + EXTRA, :] = out_ref[0, : n + EXTRA, :]
    for k in range(out_ref.shape[0]):
        for h in range(units // 128):
            at = n + EXTRA + h * ROWS
            out_ref[k, at : at + ROWS, :] = mine_ref[k * ROWS : (k + 1) * ROWS, h * 128 : (h + 1) * 128]


def second_pass(samples, pos, spins, hidden, f, fb, g0, g1, mine, st, norm):
    units, n = hidden.shape
    parts = mine.shape[0] // ROWS
    return call(
        functools.partial(second_kernel, samples),
        [SMEM] + [VMEM] * 12,
        [jax.ShapeDtypeStruct((parts, n // 128 + EXTRA + units // 128 * ROWS, 128), F32)],
        [pltpu.VMEM((2 * units, NB * 128), BF16)],
        flops=4 * 10**9,
    )(pos, resident(spins), resident(hidden), *f, fb, g0, g1, mine, st, norm)[0]


def put_stats(v, st_ref):
    mean = jnp.sum(v) / v.size
    st_ref[0:1, :] = jnp.full((1, 128), mean, F32)
    st_ref[1:2, :] = total((v - mean) ** 2)
    st_ref[2:, :] = jnp.zeros((st_ref.shape[0] - 2, 128), F32)


def over_chain_kernel(got_ref, all_ref):
    rows = all_ref.shape[1]
    x = got_ref[0, :rows, :]
    for k in range(1, got_ref.shape[0]):
        x = x + got_ref[k, :rows, :]
    for k in range(all_ref.shape[0]):
        all_ref[k] = x


def over_groups(got, rows):
    (x,) = call(over_chain_kernel, [VMEM], [jax.ShapeDtypeStruct((lax.axis_size(GRP), rows, 128), F32)])(got)
    return lax.all_to_all(x, GRP, 0, 0, tiled=True)


def summed(got_ref):
    x = got_ref[0]
    for k in range(1, got_ref.shape[0]):
        x = x + got_ref[k]
    n = x.shape[0] - EXTRA
    return x[:n], x[n:]


def first_sum_kernel(got_ref, v_ref, st_ref, norm_ref):
    v, extra = summed(got_ref)
    v_ref[...] = v
    norm_ref[...] = extra
    put_stats(v, st_ref)


def first_sum(got):
    shape = lambda *s: jax.ShapeDtypeStruct(s, F32)
    return call(first_sum_kernel, [VMEM], [shape(got.shape[1] - EXTRA, 128), shape(8, 128), shape(EXTRA, 128)])(got)


def second_sum_kernel(got_ref, v_ref, norm_ref, st_ref, next_ref):
    u, extra = summed(got_ref)
    next_ref[...] = extra
    beta = extra[0:1, 0:1] / norm_ref[0:1, 0:1]
    put_stats(u + beta * v_ref[...], st_ref)


def second_sum(got, values, norm):
    shape = lambda *s: jax.ShapeDtypeStruct(s, F32)
    return call(second_sum_kernel, [VMEM] * 3, [shape(8, 128), shape(EXTRA, 128)])(
        got, values, norm
    )


def of_sets(st):
    return to_all(st, SETS, lax.axis_size(SETS))


def joined(st_ref, count):
    sets = st_ref.shape[0]
    mean = st_ref[0, 0:1, :]
    for k in range(1, sets):
        mean = mean + st_ref[k, 0:1, :]
    mean = mean * (1.0 / sets)
    spread = jnp.zeros_like(mean)
    for k in range(sets):
        off = st_ref[k, 0:1, :] - mean
        spread = spread + (st_ref[k, 1:2, :] + count * (off * off))
    return mean, spread


def image_kernel(samples, pos_ref, s_ref, h_ref, v_ref, st_ref, keep_ref, send_ref, acc, lanes):
    units = h_ref.shape[0]
    mean = joined(st_ref, h_ref.shape[1])[0][:, 0:1]
    acc[...] = jnp.zeros(acc.shape, F32)
    lanes[...] = jnp.zeros(lanes.shape, F32)

    def step(t, carry):
        r = h_ref[:, cols(t)] * to_line((v_ref[sub(t), :] - mean) * (1.0 / samples))
        both = jnp.concatenate(split_terms(r), axis=0)
        out = lax.dot_general(both, s_ref[:, cols(t)], (((1,), (1,)), ((), ())), preferred_element_type=F32)
        acc[...] += out[:units] + out[units:]
        part = r[:, :128]
        for k in range(1, TILE // 128):
            part = part + r[:, k * 128 : (k + 1) * 128]
        lanes[...] += part
        return carry

    lax.fori_loop(0, s_ref.shape[1] // TILE, step, 0)
    bias = [
        jnp.sum(lanes[k * 128 : (k + 1) * 128, :].T, axis=0, keepdims=True) for k in range(units // 128)
    ] + [jnp.zeros((8 - units // 128, 128), F32)]
    bias = jnp.concatenate(bias, axis=0)
    for b in range(NB):
        ref = (keep_ref, send_ref)[b // 4]
        at = pos_ref[33 + b % 4]
        ref[at, :units, :] = acc[:, b * 128 : (b + 1) * 128]
        ref[at, units:, :] = bias


def image_pass(samples, pos, spins, hidden, values, st):
    units = hidden.shape[0]
    return call(
        functools.partial(image_kernel, samples),
        [SMEM] + [VMEM] * 4,
        [jax.ShapeDtypeStruct((4, units + 8, 128), F32)] * 2,
        [pltpu.VMEM((units, NB * 128), F32), pltpu.VMEM((units, 128), F32)],
        flops=4 * 10**9,
    )(pos, resident(spins), resident(hidden), values, st)


def image_sum_kernel(got_ref, all_ref, mine_ref):
    units = mine_ref.shape[1]
    x = got_ref[0] + got_ref[1] + (got_ref[2] + got_ref[3])
    for k in range(4):
        all_ref[k] = x
    mine_ref[...] = x[:units].T


def image_sum(got, units):
    shape = lambda *s: jax.ShapeDtypeStruct(s, F32)
    return call(image_sum_kernel, [VMEM], [shape(*got.shape), shape(128, units)])(got)


def update_kernel(samples, f_ref, fb_ref, got_ref, st0_ref, norm_ref, st1_ref, next_ref, w_ref, b_ref):
    count = samples // st0_ref.shape[0]
    norm0, norm1 = norm_ref[0:1, 0:1], next_ref[0:1, 0:1]
    cross = next_ref[1:2, 0:1]
    beta = norm1 / norm0
    step0 = step_of(norm0, joined(st0_ref, count)[1][:, 0:1], samples, norm0)
    step1 = step_of(norm1, joined(st1_ref, count)[1][:, 0:1], samples, norm1 + 2.0 * beta * cross + beta * beta * norm0)

    def update(f, g):
        r = f - step0 * (g + LAM * f)
        return step0 * f + step1 * (r + beta * f)

    parts = got_ref.shape[0]
    per = f_ref.shape[1] // 128 // parts
    n = got_ref.shape[1] - EXTRA - per * ROWS
    for k in range(parts):
        for h in range(per):
            b = k * per + h
            at = n + EXTRA + h * ROWS
            w_ref[:, b * 128 : (b + 1) * 128] = update(f_ref[:, b * 128 : (b + 1) * 128], got_ref[k, at : at + ROWS, :])
            b_ref[b : b + 1, :] = update(fb_ref[b : b + 1, :], got_ref[k, n + 2 + h : n + 3 + h, :])


def update_pass(samples, f, fb, got, st0, norm, st1, norms):
    shape = lambda s: jax.ShapeDtypeStruct(s, F32)
    return call(
        functools.partial(update_kernel, samples), [VMEM] * 7, [shape(f.shape), shape(fb.shape)]
    )(f, fb, got, st0, norm, st1, norms)


def body(spins_packed, weight, hidden_bias, force_w, force_b):
    xh, zh, zl, c = (lax.axis_index(a) for a in SMP)
    parts = lax.axis_size("zh")
    units = weight.shape[1] // parts
    samples = spins_packed.shape[1] * lax.axis_size(SMP)
    hb = hidden_bias.reshape(-1, 128)
    fb = force_b.reshape(-1, 128)

    q = jnp.arange(32, dtype=jnp.int32)
    words = (((q >> 2) & 1) ^ xh) * 16 + (q & 3) * 4 + (((q >> 3) & 1) ^ zl) * 2 + ((q >> 4) ^ c)
    k = jnp.arange(4, dtype=jnp.int32)
    blocks = ((k & 1) ^ xh) * 2 + ((k >> 1) ^ zl)
    pos = jnp.concatenate([words, zh.reshape(1), blocks])

    f_cols = jnp.stack([force_w[:, k * units : (k + 1) * units] for k in range(parts)])
    f = lax.all_to_all(f_cols, "zh", 0, 0, tiled=True)
    f = f.reshape(parts * ROWS, units).T[None]
    f_xh = swap(f, "xh")
    f = jnp.concatenate([f, f_xh], axis=0)
    f_zl = swap(f, "zl")
    f = (f, f_zl, swap(f, "c"), swap(f_zl, "c"))

    packed = to_all(spins_packed, "zh", parts)
    w = lax.dynamic_slice_in_dim(weight, zh * units, units, 1)
    spins, hidden = hidden_pass(pos, packed, w, hb, units)
    partial = first_pass(pos, spins, hidden, f, fb)
    rows = partial.shape[0]
    values, st, norm = first_sum(over_groups(to_all(partial, "zh", parts), rows))
    st0 = of_sets(st)

    keep, send = image_pass(samples, pos, spins, hidden, values, st0)
    g = keep + swap(send, "c")
    g, mine = image_sum(lax.all_to_all(g, QUAD, 0, 0, tiled=True), units)
    g = lax.all_to_all(g, QUAD, 0, 0, tiled=True)

    partial = second_pass(samples, pos, spins, hidden, f, fb, g, swap(g, "c"), mine, st0, norm)
    got = lax.all_to_all(partial, "zh", 0, 0, tiled=True)
    st, norms = second_sum(over_groups(got, rows), values, norm)
    st1 = of_sets(st)
    out_w, out_b = update_pass(samples, force_w, fb, got, st0, norm, st1, norms)
    return out_w, out_b.reshape(-1)


def solution(mesh):
    torus = Mesh(mesh.devices.reshape(2, 4, 2, 4, 2, 2), ("xl", "y", "xh", "zh", "zl", "c"))
    in_specs = (P(None, SMP), P(None, GRP), P(GRP), P(SMP, GRP), P(GRP))
    out_specs = (P(SMP, GRP), P(GRP))
    return jax.shard_map(body, mesh=torus, in_specs=in_specs, out_specs=out_specs, check_vma=False)
```

```python
import functools

import jax
import jax.numpy as jnp
from jax import lax
from jax.experimental import pallas as pl
from jax.experimental.pallas import tpu as pltpu
from jax.sharding import Mesh
from jax.sharding import PartitionSpec as P


GRP = ("xl", "y")
SMP = ("xh", "zh", "zl", "c")
QUAD = ("xh", "zl")
SETS = ("xh", "zl", "c")
SWAP = [(0, 1), (1, 0)]
LAM = 0.01
ROWS = 32
NB = 8
TILE = 1024
LIMIT = 14
SUB = TILE // 128
EXTRA = 8
F32, BF16 = jnp.float32, jnp.bfloat16
VMEM = pl.BlockSpec(memory_space=pltpu.VMEM)
SMEM = pl.BlockSpec(memory_space=pltpu.SMEM)


def swap(x, axis):
    return lax.ppermute(x, axis, SWAP)


def to_all(x, axes, size):
    return lax.all_to_all(jnp.broadcast_to(x[None], (size, *x.shape)), axes, 0, 0, tiled=True)


def split_terms(x):
    hi = x.astype(BF16)
    return hi, (x - hi.astype(F32)).astype(BF16)


def resident(x):
    return pltpu.with_memory_space_constraint(x, pltpu.VMEM)


def call(kernel, ins, outs, scratch=(), flops=0):
    return pl.pallas_call(
        kernel,
        in_specs=ins,
        out_specs=[VMEM] * len(outs),
        out_shape=outs,
        scratch_shapes=scratch,
        compiler_params=pltpu.CompilerParams(vmem_limit_bytes=LIMIT << 20),
        cost_estimate=pl.CostEstimate(flops=flops, bytes_accessed=1 << 20, transcendentals=0),
    )


def cols(t):
    return pl.ds(pl.multiple_of(t * TILE, TILE), TILE)


def rows_to_column(rows):
    return jnp.concatenate(
        [jnp.broadcast_to(rows[k : k + 1, :], (128, 128)).T[:, :1] for k in range(rows.shape[0])], axis=0
    )


def total(x):
    return jnp.full((1, 128), jnp.sum(x), F32)


def to_rows(line):
    return jnp.concatenate([line[:, k * 128 : (k + 1) * 128] for k in range(line.shape[1] // 128)], axis=0)


def to_line(rows):
    return jnp.concatenate([rows[k : k + 1, :] for k in range(rows.shape[0])], axis=1)


def sub(t):
    return pl.ds(pl.multiple_of(t * SUB, SUB), SUB)


def hidden_kernel(pos_ref, packed_ref, w_ref, hb_ref, s_ref, h_ref, wt):
    units = wt.shape[0]
    for b in range(NB):
        rows = [w_ref[pl.ds(pl.multiple_of(pos_ref[4 * b + k] * ROWS, ROWS), ROWS), :] for k in range(4)]
        block = jnp.concatenate(rows, axis=0).astype(F32)
        wt[:, b * 128 : (b + 1) * 128] = block.T.astype(BF16)
    shifts = 31 - lax.broadcasted_iota(jnp.int32, (ROWS, TILE), 0)
    hb = rows_to_column(my_rows(pos_ref, hb_ref, units))

    def step(t, carry):
        for q in range(32):
            word = packed_ref[t, pl.ds(pos_ref[q], 1), :]
            up = jnp.left_shift(jnp.broadcast_to(word, (ROWS, TILE)), shifts) < 0
            s_ref[q * ROWS : (q + 1) * ROWS, cols(t)] = jnp.where(up, 1.0, -1.0).astype(BF16)
        pre = jnp.dot(wt[...], s_ref[:, cols(t)], preferred_element_type=F32)
        h_ref[:, cols(t)] = jnp.tanh(pre + hb)
        return carry

    lax.fori_loop(0, packed_ref.shape[0], step, 0)


def hidden_pass(pos, packed, w, hb, units):
    n = packed.shape[0] * TILE
    return call(
        hidden_kernel,
        [SMEM, VMEM, VMEM, VMEM],
        [pltpu.VMEM((NB * 128, n), BF16), pltpu.VMEM((units, n), F32)],
        [pltpu.VMEM((units, NB * 128), BF16)],
        flops=4 * 10**9,
    )(pos, packed, w, hb)


def project(s_ref, h_ref, lhs, bias, p_ref):
    units = h_ref.shape[0]

    def step(t, carry):
        out = jnp.dot(lhs[...], s_ref[:, cols(t)], preferred_element_type=F32)
        proj = out[:units] + out[units:] + bias
        p_ref[sub(t), :] = to_rows(jnp.sum(h_ref[:, cols(t)] * proj, axis=0, keepdims=True))
        return carry

    lax.fori_loop(0, s_ref.shape[1] // TILE, step, 0)


def set_block(lhs, b, x):
    units = x.shape[0]
    hi, lo = split_terms(x)
    lhs[:units, b * 128 : (b + 1) * 128] = hi
    lhs[units:, b * 128 : (b + 1) * 128] = lo


def my_rows(pos_ref, ref, units):
    return ref[pl.ds(pos_ref[32] * (units // 128), units // 128), :]


def first_kernel(pos_ref, s_ref, h_ref, f0, f1, f2, f3, fb_ref, p_ref, lhs):
    units = h_ref.shape[0]
    norm = jnp.zeros((units, 128), F32)
    for b in range(NB):
        x = (f0, f1, f2, f3)[b // 2][b % 2]
        set_block(lhs, b, x)
        norm = norm + x * x
    fb = my_rows(pos_ref, fb_ref, units)
    n = p_ref.shape[0] - EXTRA
    p_ref[n:, :] = jnp.zeros((EXTRA, 128), F32)
    p_ref[n : n + 1, :] = total(norm) + total(fb * fb)
    project(s_ref, h_ref, lhs, rows_to_column(fb), p_ref)
    p_ref[n + 1 : n + 2, :] = total(p_ref[:n, :])


def first_pass(pos, spins, hidden, f, fb):
    units, n = hidden.shape
    return call(
        first_kernel,
        [SMEM] + [VMEM] * 7,
        [jax.ShapeDtypeStruct((n // 128 + EXTRA, 128), F32)],
        [pltpu.VMEM((2 * units, NB * 128), BF16)],
        flops=4 * 10**9,
    )(pos, resident(spins), resident(hidden), *f, fb)[0]


def step_of(norm, spread, samples, length):
    return norm / (spread / samples + LAM * length)


def second_kernel(samples, pos_ref, s_ref, h_ref, f0, f1, f2, f3, fb_ref, g0, g1, mine_ref, norm_ref, out_ref, lhs):
    units = h_ref.shape[0]
    norm0 = norm_ref[0:1, :]
    spread = g0[0, units + units // 128 : units + units // 128 + 1, :]
    a = step_of(norm0, spread, samples, norm0)
    rr = jnp.zeros((units, 128), F32)
    rf = jnp.zeros((units, 128), F32)
    for b in range(NB):
        f = (f0, f1, f2, f3)[b // 2][b % 2]
        g = (g0, g1)[b // 4][pos_ref[33 + b % 4], :units, :]
        r = f - a * (g + LAM * f)
        set_block(lhs, b, r)
        rr = rr + r * r
        rf = rf + r * f
    fb = my_rows(pos_ref, fb_ref, units)
    rb = fb - a * (g0[0, units : units + units // 128, :] + LAM * fb)
    n = h_ref.shape[1] // 128
    p_ref = out_ref.at[0]
    p_ref[n : n + EXTRA, :] = jnp.zeros((EXTRA, 128), F32)
    p_ref[n : n + 1, :] = total(rr) + total(rb * rb)
    p_ref[n + 1 : n + 2, :] = total(rf) + total(rb * fb)
    p_ref[n + 2 : n + 2 + units // 128, :] = g0[0, units : units + units // 128, :]
    p_ref[n + 2 + units // 128 : n + 3 + units // 128, :] = spread
    project(s_ref, h_ref, lhs, rows_to_column(rb), p_ref)
    for k in range(1, out_ref.shape[0]):
        out_ref[k, : n + EXTRA, :] = out_ref[0, : n + EXTRA, :]
    for k in range(out_ref.shape[0]):
        for h in range(units // 128):
            at = n + EXTRA + h * ROWS
            out_ref[k, at : at + ROWS, :] = mine_ref[k * ROWS : (k + 1) * ROWS, h * 128 : (h + 1) * 128]


def second_pass(samples, pos, spins, hidden, f, fb, g0, g1, mine, norm):
    units, n = hidden.shape
    parts = mine.shape[0] // ROWS
    return call(
        functools.partial(second_kernel, samples),
        [SMEM] + [VMEM] * 11,
        [jax.ShapeDtypeStruct((parts, n // 128 + EXTRA + units // 128 * ROWS, 128), F32)],
        [pltpu.VMEM((2 * units, NB * 128), BF16)],
        flops=4 * 10**9,
    )(pos, resident(spins), resident(hidden), *f, fb, g0, g1, mine, norm)[0]


def put_stats(v, st_ref):
    mean = jnp.sum(v) / v.size
    st_ref[0:1, :] = jnp.full((1, 128), mean, F32)
    st_ref[1:2, :] = total((v - mean) ** 2)
    st_ref[2:, :] = jnp.zeros((st_ref.shape[0] - 2, 128), F32)


def over_chain_kernel(got_ref, all_ref):
    rows = all_ref.shape[1]
    x = got_ref[0, :rows, :]
    for k in range(1, got_ref.shape[0]):
        x = x + got_ref[k, :rows, :]
    for k in range(all_ref.shape[0]):
        all_ref[k] = x


def over_groups(got, rows):
    (x,) = call(over_chain_kernel, [VMEM], [jax.ShapeDtypeStruct((lax.axis_size(GRP), rows, 128), F32)])(got)
    return lax.all_to_all(x, GRP, 0, 0, tiled=True)


def summed(got_ref):
    x = got_ref[0]
    for k in range(1, got_ref.shape[0]):
        x = x + got_ref[k]
    n = x.shape[0] - EXTRA
    return x[:n], x[n:]


def sum_of_set(got_ref, mine, stride, count):
    x = got_ref[mine]
    for k in range(1, count):
        x = x + got_ref[mine + k * stride]
    n = x.shape[0] - EXTRA
    everyone = got_ref[0, n + 1 : n + 2, :]
    for k in range(1, got_ref.shape[0]):
        everyone = everyone + got_ref[k, n + 1 : n + 2, :]
    return x, everyone, n


def first_chain_kernel(pos_ref, got_ref, all_ref):
    x, everyone, n = sum_of_set(got_ref, pos_ref[37], 2, got_ref.shape[0] // 2)
    for k in range(all_ref.shape[0]):
        all_ref[k] = x
        all_ref[k, n + 1 : n + 2, :] = everyone


def first_sum_kernel(pos_ref, got_ref, v_ref, extra_ref):
    peers = got_ref.shape[0] // 2
    x, everyone, n = sum_of_set(got_ref, pos_ref[38] * peers, 1, peers)
    v_ref[...] = x[:n]
    extra_ref[...] = x[n:]
    extra_ref[1:2, :] = everyone


def first_sum(pos, partial):
    shape = lambda *s: jax.ShapeDtypeStruct(s, F32)
    rows = partial.shape[0]
    chain, plane = ("zh", "zl"), ("xh", *GRP)
    got = to_all(partial, chain, lax.axis_size(chain))
    (x,) = call(first_chain_kernel, [SMEM, VMEM], [shape(lax.axis_size(plane), rows, 128)])(pos, got)
    got = lax.all_to_all(x, plane, 0, 0, tiled=True)
    return call(first_sum_kernel, [SMEM, VMEM], [shape(rows - EXTRA, 128), shape(EXTRA, 128)])(pos, got)


def second_sum_kernel(got_ref, v_ref, norm_ref, st_ref, next_ref):
    u, extra = summed(got_ref)
    next_ref[...] = extra
    beta = extra[0:1, 0:1] / norm_ref[0:1, 0:1]
    put_stats(u + beta * v_ref[...], st_ref)


def second_sum(got, values, norm):
    shape = lambda *s: jax.ShapeDtypeStruct(s, F32)
    return call(second_sum_kernel, [VMEM] * 3, [shape(8, 128), shape(EXTRA, 128)])(
        got, values, norm
    )


def of_sets(st):
    return to_all(st, SETS, lax.axis_size(SETS))


def joined(st_ref, count):
    sets = st_ref.shape[0]
    mean = st_ref[0, 0:1, :]
    for k in range(1, sets):
        mean = mean + st_ref[k, 0:1, :]
    mean = mean * (1.0 / sets)
    spread = jnp.zeros_like(mean)
    for k in range(sets):
        off = st_ref[k, 0:1, :] - mean
        spread = spread + (st_ref[k, 1:2, :] + count * (off * off))
    return mean, spread


def image_kernel(samples, pos_ref, s_ref, h_ref, v_ref, near_ref, far_ref, keep_ref, send_ref, acc, lanes):
    units = h_ref.shape[0]
    mean = (near_ref[1:2, 0:1] + far_ref[1:2, 0:1]) * (1.0 / samples)
    spread = total((v_ref[...] - mean) ** 2)
    acc[...] = jnp.zeros(acc.shape, F32)
    lanes[...] = jnp.zeros(lanes.shape, F32)

    def step(t, carry):
        r = h_ref[:, cols(t)] * to_line((v_ref[sub(t), :] - mean) * (1.0 / samples))
        both = jnp.concatenate(split_terms(r), axis=0)
        out = lax.dot_general(both, s_ref[:, cols(t)], (((1,), (1,)), ((), ())), preferred_element_type=F32)
        acc[...] += out[:units] + out[units:]
        part = r[:, :128]
        for k in range(1, TILE // 128):
            part = part + r[:, k * 128 : (k + 1) * 128]
        lanes[...] += part
        return carry

    lax.fori_loop(0, s_ref.shape[1] // TILE, step, 0)
    bias = [
        jnp.sum(lanes[k * 128 : (k + 1) * 128, :].T, axis=0, keepdims=True) for k in range(units // 128)
    ] + [spread, jnp.zeros((7 - units // 128, 128), F32)]
    bias = jnp.concatenate(bias, axis=0)
    for b in range(NB):
        ref = (keep_ref, send_ref)[b // 4]
        at = pos_ref[33 + b % 4]
        ref[at, :units, :] = acc[:, b * 128 : (b + 1) * 128]
        ref[at, units:, :] = bias


def image_pass(samples, pos, spins, hidden, values, near, far):
    units = hidden.shape[0]
    return call(
        functools.partial(image_kernel, samples),
        [SMEM] + [VMEM] * 5,
        [jax.ShapeDtypeStruct((4, units + 8, 128), F32)] * 2,
        [pltpu.VMEM((units, NB * 128), F32), pltpu.VMEM((units, 128), F32)],
        flops=4 * 10**9,
    )(pos, resident(spins), resident(hidden), values, near, far)


def image_sum_kernel(got_ref, all_ref, mine_ref):
    units = mine_ref.shape[1]
    x = got_ref[0] + got_ref[1] + (got_ref[2] + got_ref[3])
    for k in range(4):
        all_ref[k] = x
    mine_ref[...] = x[:units].T


def image_sum(got, units):
    shape = lambda *s: jax.ShapeDtypeStruct(s, F32)
    return call(image_sum_kernel, [VMEM], [shape(*got.shape), shape(128, units)])(got)


def update_kernel(samples, f_ref, fb_ref, got_ref, norm_ref, st1_ref, next_ref, w_ref, b_ref):
    parts = got_ref.shape[0]
    per = f_ref.shape[1] // 128 // parts
    n = got_ref.shape[1] - EXTRA - per * ROWS
    count = samples // st1_ref.shape[0]
    norm0, norm1 = norm_ref[0:1, 0:1], next_ref[0:1, 0:1]
    cross = next_ref[1:2, 0:1]
    beta = norm1 / norm0
    step0 = step_of(norm0, got_ref[0, n + 2 + per : n + 3 + per, 0:1], samples, norm0)
    step1 = step_of(norm1, joined(st1_ref, count)[1][:, 0:1], samples, norm1 + 2.0 * beta * cross + beta * beta * norm0)

    def update(f, g):
        r = f - step0 * (g + LAM * f)
        return step0 * f + step1 * (r + beta * f)

    for k in range(parts):
        for h in range(per):
            b = k * per + h
            at = n + EXTRA + h * ROWS
            w_ref[:, b * 128 : (b + 1) * 128] = update(f_ref[:, b * 128 : (b + 1) * 128], got_ref[k, at : at + ROWS, :])
            b_ref[b : b + 1, :] = update(fb_ref[b : b + 1, :], got_ref[k, n + 2 + h : n + 3 + h, :])


def update_pass(samples, f, fb, got, norm, st1, norms):
    shape = lambda s: jax.ShapeDtypeStruct(s, F32)
    return call(
        functools.partial(update_kernel, samples), [VMEM] * 6, [shape(f.shape), shape(fb.shape)]
    )(f, fb, got, norm, st1, norms)


def body(spins_packed, weight, hidden_bias, force_w, force_b):
    xh, zh, zl, c = (lax.axis_index(a) for a in SMP)
    parts = lax.axis_size("zh")
    units = weight.shape[1] // parts
    samples = spins_packed.shape[1] * lax.axis_size(SMP)
    hb = hidden_bias.reshape(-1, 128)
    fb = force_b.reshape(-1, 128)

    q = jnp.arange(32, dtype=jnp.int32)
    words = (((q >> 2) & 1) ^ xh) * 16 + (q & 3) * 4 + (((q >> 3) & 1) ^ zl) * 2 + ((q >> 4) ^ c)
    k = jnp.arange(4, dtype=jnp.int32)
    blocks = ((k & 1) ^ xh) * 2 + ((k >> 1) ^ zl)
    pos = jnp.concatenate([words, zh.reshape(1), blocks, zl.reshape(1), xh.reshape(1)])

    f_cols = jnp.stack([force_w[:, k * units : (k + 1) * units] for k in range(parts)])
    f = lax.all_to_all(f_cols, "zh", 0, 0, tiled=True)
    f = f.reshape(parts * ROWS, units).T[None]
    f_xh = swap(f, "xh")
    f = jnp.concatenate([f, f_xh], axis=0)
    f_zl = swap(f, "zl")
    f = (f, f_zl, swap(f, "c"), swap(f_zl, "c"))

    packed = to_all(spins_packed, "zh", parts)
    w = lax.dynamic_slice_in_dim(weight, zh * units, units, 1)
    spins, hidden = hidden_pass(pos, packed, w, hb, units)
    partial = first_pass(pos, spins, hidden, f, fb)
    rows = partial.shape[0]
    values, norm = first_sum(pos, partial)
    norm_far = swap(norm, "c")

    keep, send = image_pass(samples, pos, spins, hidden, values, norm, norm_far)
    g = keep + swap(send, "c")
    g, mine = image_sum(lax.all_to_all(g, QUAD, 0, 0, tiled=True), units)
    g = lax.all_to_all(g, QUAD, 0, 0, tiled=True)

    partial = second_pass(samples, pos, spins, hidden, f, fb, g, swap(g, "c"), mine, norm)
    got = lax.all_to_all(partial, "zh", 0, 0, tiled=True)
    st, norms = second_sum(over_groups(got, rows), values, norm)
    st1 = of_sets(st)
    out_w, out_b = update_pass(samples, force_w, fb, got, norm, st1, norms)
    return out_w, out_b.reshape(-1)


def solution(mesh):
    torus = Mesh(mesh.devices.reshape(2, 4, 2, 4, 2, 2), ("xl", "y", "xh", "zh", "zl", "c"))
    in_specs = (P(None, SMP), P(None, GRP), P(GRP), P(SMP, GRP), P(GRP))
    out_specs = (P(SMP, GRP), P(GRP))
    return jax.shard_map(body, mesh=torus, in_specs=in_specs, out_specs=out_specs, check_vma=False)
```

```python
import functools

import jax
import jax.numpy as jnp
from jax import lax
from jax.experimental import pallas as pl
from jax.experimental.pallas import tpu as pltpu
from jax.sharding import Mesh
from jax.sharding import PartitionSpec as P


GRP = ("xl", "y")
SMP = ("xh", "zh", "zl", "c")
QUAD = ("xh", "zl")
SETS = ("xh", "zl", "c")
SWAP = [(0, 1), (1, 0)]
LAM = 0.01
ROWS = 32
NB = 8
TILE = 1024
LIMIT = 14
SUB = TILE // 128
EXTRA = 8
F32, BF16 = jnp.float32, jnp.bfloat16
VMEM = pl.BlockSpec(memory_space=pltpu.VMEM)
SMEM = pl.BlockSpec(memory_space=pltpu.SMEM)


def swap(x, axis):
    return lax.ppermute(x, axis, SWAP)


def to_all(x, axes, size):
    return lax.all_to_all(jnp.broadcast_to(x[None], (size, *x.shape)), axes, 0, 0, tiled=True)


def split_terms(x):
    hi = x.astype(BF16)
    return hi, (x - hi.astype(F32)).astype(BF16)


def resident(x):
    return pltpu.with_memory_space_constraint(x, pltpu.VMEM)


def call(kernel, ins, outs, scratch=(), flops=0):
    return pl.pallas_call(
        kernel,
        in_specs=ins,
        out_specs=[VMEM] * len(outs),
        out_shape=outs,
        scratch_shapes=scratch,
        compiler_params=pltpu.CompilerParams(vmem_limit_bytes=LIMIT << 20),
        cost_estimate=pl.CostEstimate(flops=flops, bytes_accessed=1 << 20, transcendentals=0),
    )


def cols(t):
    return pl.ds(pl.multiple_of(t * TILE, TILE), TILE)


def rows_to_column(rows):
    return jnp.concatenate(
        [jnp.broadcast_to(rows[k : k + 1, :], (128, 128)).T[:, :1] for k in range(rows.shape[0])], axis=0
    )


def total(x):
    return jnp.full((1, 128), jnp.sum(x), F32)


def to_rows(line):
    return jnp.concatenate([line[:, k * 128 : (k + 1) * 128] for k in range(line.shape[1] // 128)], axis=0)


def to_line(rows):
    return jnp.concatenate([rows[k : k + 1, :] for k in range(rows.shape[0])], axis=1)


def sub(t):
    return pl.ds(pl.multiple_of(t * SUB, SUB), SUB)


def hidden_kernel(pos_ref, x0, x1, x2, x3, w_ref, hb_ref, s_ref, h_ref, wt, packed_ref):
    units = wt.shape[0]
    for d, x in enumerate((x0, x1, x2, x3)):
        packed_ref[(pos_ref[32] + 4 - d) % 4] = x[...]
    for b in range(NB):
        rows = [w_ref[pl.ds(pl.multiple_of(pos_ref[4 * b + k] * ROWS, ROWS), ROWS), :] for k in range(4)]
        block = jnp.concatenate(rows, axis=0).astype(F32)
        wt[:, b * 128 : (b + 1) * 128] = block.T.astype(BF16)
    shifts = 31 - lax.broadcasted_iota(jnp.int32, (ROWS, TILE), 0)
    hb = rows_to_column(my_rows(pos_ref, hb_ref, units))

    def step(t, carry):
        for q in range(32):
            word = packed_ref[t, pl.ds(pos_ref[q], 1), :]
            up = jnp.left_shift(jnp.broadcast_to(word, (ROWS, TILE)), shifts) < 0
            s_ref[q * ROWS : (q + 1) * ROWS, cols(t)] = jnp.where(up, 1.0, -1.0).astype(BF16)
        pre = jnp.dot(wt[...], s_ref[:, cols(t)], preferred_element_type=F32)
        h_ref[:, cols(t)] = jnp.tanh(pre + hb)
        return carry

    lax.fori_loop(0, packed_ref.shape[0], step, 0)


def hidden_pass(pos, packed, w, hb, units):
    n = len(packed) * TILE
    return call(
        hidden_kernel,
        [SMEM] + [VMEM] * 6,
        [pltpu.VMEM((NB * 128, n), BF16), pltpu.VMEM((units, n), F32)],
        [pltpu.VMEM((units, NB * 128), BF16), pltpu.VMEM((len(packed), *packed[0].shape), jnp.int32)],
        flops=4 * 10**9,
    )(pos, *packed, w, hb)


def project(s_ref, h_ref, lhs, bias, p_ref):
    units = h_ref.shape[0]

    def step(t, carry):
        out = jnp.dot(lhs[...], s_ref[:, cols(t)], preferred_element_type=F32)
        proj = out[:units] + out[units:] + bias
        p_ref[sub(t), :] = to_rows(jnp.sum(h_ref[:, cols(t)] * proj, axis=0, keepdims=True))
        return carry

    lax.fori_loop(0, s_ref.shape[1] // TILE, step, 0)


def set_block(lhs, b, x):
    units = x.shape[0]
    hi, lo = split_terms(x)
    lhs[:units, b * 128 : (b + 1) * 128] = hi
    lhs[units:, b * 128 : (b + 1) * 128] = lo


def my_rows(pos_ref, ref, units):
    return ref[pl.ds(pos_ref[32] * (units // 128), units // 128), :]


def first_kernel(pos_ref, s_ref, h_ref, f0, f1, f2, f3, fb_ref, p_ref, lhs):
    units = h_ref.shape[0]
    norm = jnp.zeros((units, 128), F32)
    for b in range(NB):
        x = (f0, f1, f2, f3)[b // 2][b % 2]
        set_block(lhs, b, x)
        norm = norm + x * x
    fb = my_rows(pos_ref, fb_ref, units)
    n = p_ref.shape[0] - EXTRA
    p_ref[n:, :] = jnp.zeros((EXTRA, 128), F32)
    p_ref[n : n + 1, :] = total(norm) + total(fb * fb)
    project(s_ref, h_ref, lhs, rows_to_column(fb), p_ref)
    p_ref[n + 1 : n + 2, :] = total(p_ref[:n, :])


def first_pass(pos, spins, hidden, f, fb):
    units, n = hidden.shape
    return call(
        first_kernel,
        [SMEM] + [VMEM] * 7,
        [jax.ShapeDtypeStruct((n // 128 + EXTRA, 128), F32)],
        [pltpu.VMEM((2 * units, NB * 128), BF16)],
        flops=4 * 10**9,
    )(pos, resident(spins), resident(hidden), *f, fb)[0]


def step_of(norm, spread, samples, length):
    return norm / (spread / samples + LAM * length)


def second_kernel(samples, pos_ref, s_ref, h_ref, f0, f1, f2, f3, fb_ref, g0, g1, mine_ref, norm_ref, out_ref, lhs):
    units = h_ref.shape[0]
    norm0 = norm_ref[0:1, :]
    spread = g0[0, units + units // 128 : units + units // 128 + 1, :]
    a = step_of(norm0, spread, samples, norm0)
    rr = jnp.zeros((units, 128), F32)
    rf = jnp.zeros((units, 128), F32)
    for b in range(NB):
        f = (f0, f1, f2, f3)[b // 2][b % 2]
        g = (g0, g1)[b // 4][pos_ref[33 + b % 4], :units, :]
        r = f - a * (g + LAM * f)
        set_block(lhs, b, r)
        rr = rr + r * r
        rf = rf + r * f
    fb = my_rows(pos_ref, fb_ref, units)
    rb = fb - a * (g0[0, units : units + units // 128, :] + LAM * fb)
    n = h_ref.shape[1] // 128
    p_ref = out_ref.at[0]
    p_ref[n : n + EXTRA, :] = jnp.zeros((EXTRA, 128), F32)
    p_ref[n : n + 1, :] = total(rr) + total(rb * rb)
    p_ref[n + 1 : n + 2, :] = total(rf) + total(rb * fb)
    p_ref[n + 2 : n + 2 + units // 128, :] = g0[0, units : units + units // 128, :]
    p_ref[n + 2 + units // 128 : n + 3 + units // 128, :] = spread
    project(s_ref, h_ref, lhs, rows_to_column(rb), p_ref)
    for k in range(1, out_ref.shape[0]):
        out_ref[k, : n + EXTRA, :] = out_ref[0, : n + EXTRA, :]
    for k in range(out_ref.shape[0]):
        for h in range(units // 128):
            at = n + EXTRA + h * ROWS
            out_ref[k, at : at + ROWS, :] = mine_ref[k * ROWS : (k + 1) * ROWS, h * 128 : (h + 1) * 128]


def second_pass(samples, pos, spins, hidden, f, fb, g0, g1, mine, norm):
    units, n = hidden.shape
    parts = mine.shape[0] // ROWS
    return call(
        functools.partial(second_kernel, samples),
        [SMEM] + [VMEM] * 11,
        [jax.ShapeDtypeStruct((parts, n // 128 + EXTRA + units // 128 * ROWS, 128), F32)],
        [pltpu.VMEM((2 * units, NB * 128), BF16)],
        flops=4 * 10**9,
    )(pos, resident(spins), resident(hidden), *f, fb, g0, g1, mine, norm)[0]


def put_stats(v, st_ref):
    mean = jnp.sum(v) / v.size
    st_ref[0:1, :] = jnp.full((1, 128), mean, F32)
    st_ref[1:2, :] = total((v - mean) ** 2)
    st_ref[2:, :] = jnp.zeros((st_ref.shape[0] - 2, 128), F32)


def over_chain_kernel(got_ref, all_ref):
    rows = all_ref.shape[1]
    x = got_ref[0, :rows, :]
    for k in range(1, got_ref.shape[0]):
        x = x + got_ref[k, :rows, :]
    for k in range(all_ref.shape[0]):
        all_ref[k] = x


def over_groups(got, rows):
    (x,) = call(over_chain_kernel, [VMEM], [jax.ShapeDtypeStruct((lax.axis_size(GRP), rows, 128), F32)])(got)
    return lax.all_to_all(x, GRP, 0, 0, tiled=True)


def summed(got_ref):
    x = got_ref[0]
    for k in range(1, got_ref.shape[0]):
        x = x + got_ref[k]
    n = x.shape[0] - EXTRA
    return x[:n], x[n:]


def sum_of_set(got_ref, mine, stride, count):
    x = got_ref[mine]
    for k in range(1, count):
        x = x + got_ref[mine + k * stride]
    n = x.shape[0] - EXTRA
    everyone = got_ref[0, n + 1 : n + 2, :]
    for k in range(1, got_ref.shape[0]):
        everyone = everyone + got_ref[k, n + 1 : n + 2, :]
    return x, everyone, n


def first_chain_kernel(pos_ref, got_ref, all_ref):
    x, everyone, n = sum_of_set(got_ref, pos_ref[37], 2, got_ref.shape[0] // 2)
    for k in range(all_ref.shape[0]):
        all_ref[k] = x
        all_ref[k, n + 1 : n + 2, :] = everyone


def first_sum_kernel(pos_ref, got_ref, v_ref, extra_ref):
    peers = got_ref.shape[0] // 2
    x, everyone, n = sum_of_set(got_ref, pos_ref[38] * peers, 1, peers)
    v_ref[...] = x[:n]
    extra_ref[...] = x[n:]
    extra_ref[1:2, :] = everyone


def first_sum(pos, partial):
    shape = lambda *s: jax.ShapeDtypeStruct(s, F32)
    rows = partial.shape[0]
    chain, plane = ("zh", "zl"), ("xh", *GRP)
    got = to_all(partial, chain, lax.axis_size(chain))
    (x,) = call(first_chain_kernel, [SMEM, VMEM], [shape(lax.axis_size(plane), rows, 128)])(pos, got)
    got = lax.all_to_all(x, plane, 0, 0, tiled=True)
    return call(first_sum_kernel, [SMEM, VMEM], [shape(rows - EXTRA, 128), shape(EXTRA, 128)])(pos, got)


def second_sum_kernel(got_ref, v_ref, norm_ref, st_ref, next_ref):
    u, extra = summed(got_ref)
    next_ref[...] = extra
    beta = extra[0:1, 0:1] / norm_ref[0:1, 0:1]
    put_stats(u + beta * v_ref[...], st_ref)


def second_sum(got, values, norm):
    shape = lambda *s: jax.ShapeDtypeStruct(s, F32)
    return call(second_sum_kernel, [VMEM] * 3, [shape(8, 128), shape(EXTRA, 128)])(
        got, values, norm
    )


def of_sets(st):
    return to_all(st, SETS, lax.axis_size(SETS))


def joined(st_ref, count):
    sets = st_ref.shape[0]
    mean = st_ref[0, 0:1, :]
    for k in range(1, sets):
        mean = mean + st_ref[k, 0:1, :]
    mean = mean * (1.0 / sets)
    spread = jnp.zeros_like(mean)
    for k in range(sets):
        off = st_ref[k, 0:1, :] - mean
        spread = spread + (st_ref[k, 1:2, :] + count * (off * off))
    return mean, spread


def image_kernel(samples, pos_ref, s_ref, h_ref, v_ref, near_ref, far_ref, keep_ref, send_ref, acc, lanes):
    units = h_ref.shape[0]
    mean = (near_ref[1:2, 0:1] + far_ref[1:2, 0:1]) * (1.0 / samples)
    spread = total((v_ref[...] - mean) ** 2)
    acc[...] = jnp.zeros(acc.shape, F32)
    lanes[...] = jnp.zeros(lanes.shape, F32)

    def step(t, carry):
        r = h_ref[:, cols(t)] * to_line((v_ref[sub(t), :] - mean) * (1.0 / samples))
        both = jnp.concatenate(split_terms(r), axis=0)
        out = lax.dot_general(both, s_ref[:, cols(t)], (((1,), (1,)), ((), ())), preferred_element_type=F32)
        acc[...] += out[:units] + out[units:]
        part = r[:, :128]
        for k in range(1, TILE // 128):
            part = part + r[:, k * 128 : (k + 1) * 128]
        lanes[...] += part
        return carry

    lax.fori_loop(0, s_ref.shape[1] // TILE, step, 0)
    bias = [
        jnp.sum(lanes[k * 128 : (k + 1) * 128, :].T, axis=0, keepdims=True) for k in range(units // 128)
    ] + [spread, jnp.zeros((7 - units // 128, 128), F32)]
    bias = jnp.concatenate(bias, axis=0)
    for b in range(NB):
        ref = (keep_ref, send_ref)[b // 4]
        at = pos_ref[33 + b % 4]
        ref[at, :units, :] = acc[:, b * 128 : (b + 1) * 128]
        ref[at, units:, :] = bias


def image_pass(samples, pos, spins, hidden, values, near, far):
    units = hidden.shape[0]
    return call(
        functools.partial(image_kernel, samples),
        [SMEM] + [VMEM] * 5,
        [jax.ShapeDtypeStruct((4, units + 8, 128), F32)] * 2,
        [pltpu.VMEM((units, NB * 128), F32), pltpu.VMEM((units, 128), F32)],
        flops=4 * 10**9,
    )(pos, resident(spins), resident(hidden), values, near, far)


def image_sum_kernel(got_ref, all_ref, mine_ref):
    units = mine_ref.shape[1]
    x = got_ref[0] + got_ref[1] + (got_ref[2] + got_ref[3])
    for k in range(4):
        all_ref[k] = x
    mine_ref[...] = x[:units].T


def image_sum(got, units):
    shape = lambda *s: jax.ShapeDtypeStruct(s, F32)
    return call(image_sum_kernel, [VMEM], [shape(*got.shape), shape(128, units)])(got)


def update_kernel(samples, f_ref, fb_ref, got_ref, norm_ref, st1_ref, next_ref, w_ref, b_ref):
    parts = got_ref.shape[0]
    per = f_ref.shape[1] // 128 // parts
    n = got_ref.shape[1] - EXTRA - per * ROWS
    count = samples // st1_ref.shape[0]
    norm0, norm1 = norm_ref[0:1, 0:1], next_ref[0:1, 0:1]
    cross = next_ref[1:2, 0:1]
    beta = norm1 / norm0
    step0 = step_of(norm0, got_ref[0, n + 2 + per : n + 3 + per, 0:1], samples, norm0)
    step1 = step_of(norm1, joined(st1_ref, count)[1][:, 0:1], samples, norm1 + 2.0 * beta * cross + beta * beta * norm0)

    def update(f, g):
        r = f - step0 * (g + LAM * f)
        return step0 * f + step1 * (r + beta * f)

    for k in range(parts):
        for h in range(per):
            b = k * per + h
            at = n + EXTRA + h * ROWS
            w_ref[:, b * 128 : (b + 1) * 128] = update(f_ref[:, b * 128 : (b + 1) * 128], got_ref[k, at : at + ROWS, :])
            b_ref[b : b + 1, :] = update(fb_ref[b : b + 1, :], got_ref[k, n + 2 + h : n + 3 + h, :])


def update_pass(samples, f, fb, got, norm, st1, norms):
    shape = lambda s: jax.ShapeDtypeStruct(s, F32)
    return call(
        functools.partial(update_kernel, samples), [VMEM] * 6, [shape(f.shape), shape(fb.shape)]
    )(f, fb, got, norm, st1, norms)


def body(spins_packed, weight, hidden_bias, force_w, force_b):
    xh, zh, zl, c = (lax.axis_index(a) for a in SMP)
    parts = lax.axis_size("zh")
    units = weight.shape[1] // parts
    samples = spins_packed.shape[1] * lax.axis_size(SMP)
    hb = hidden_bias.reshape(-1, 128)
    fb = force_b.reshape(-1, 128)

    q = jnp.arange(32, dtype=jnp.int32)
    words = (((q >> 2) & 1) ^ xh) * 16 + (q & 3) * 4 + (((q >> 3) & 1) ^ zl) * 2 + ((q >> 4) ^ c)
    k = jnp.arange(4, dtype=jnp.int32)
    blocks = ((k & 1) ^ xh) * 2 + ((k >> 1) ^ zl)
    pos = jnp.concatenate([words, zh.reshape(1), blocks, zl.reshape(1), xh.reshape(1)])

    packed = [spins_packed]
    for d in (1, 2, 3):
        packed.append(lax.ppermute(spins_packed, "zh", [(i, (i + d) % 4) for i in range(4)]))

    f_cols = jnp.stack([force_w[:, k * units : (k + 1) * units] for k in range(parts)])
    f = lax.all_to_all(f_cols, "zh", 0, 0, tiled=True)
    f = f.reshape(parts * ROWS, units).T[None]
    f_xh = swap(f, "xh")
    f = jnp.concatenate([f, f_xh], axis=0)
    f_zl = swap(f, "zl")
    f = (f, f_zl, swap(f, "c"), swap(f_zl, "c"))

    w = lax.dynamic_slice_in_dim(weight, zh * units, units, 1)
    spins, hidden = hidden_pass(pos, packed, w, hb, units)
    partial = first_pass(pos, spins, hidden, f, fb)
    rows = partial.shape[0]
    values, norm = first_sum(pos, partial)
    norm_far = swap(norm, "c")

    keep, send = image_pass(samples, pos, spins, hidden, values, norm, norm_far)
    g = keep + swap(send, "c")
    g, mine = image_sum(lax.all_to_all(g, QUAD, 0, 0, tiled=True), units)
    g = lax.all_to_all(g, QUAD, 0, 0, tiled=True)

    partial = second_pass(samples, pos, spins, hidden, f, fb, g, swap(g, "c"), mine, norm)
    got = lax.all_to_all(partial, "zh", 0, 0, tiled=True)
    st, norms = second_sum(over_groups(got, rows), values, norm)
    st1 = of_sets(st)
    out_w, out_b = update_pass(samples, force_w, fb, got, norm, st1, norms)
    return out_w, out_b.reshape(-1)


def solution(mesh):
    torus = Mesh(mesh.devices.reshape(2, 4, 2, 4, 2, 2), ("xl", "y", "xh", "zh", "zl", "c"))
    in_specs = (P(None, SMP), P(None, GRP), P(GRP), P(SMP, GRP), P(GRP))
    out_specs = (P(SMP, GRP), P(GRP))
    return jax.shard_map(body, mesh=torus, in_specs=in_specs, out_specs=out_specs, check_vma=False)
```

```python
import functools

import jax
import jax.numpy as jnp
from jax import lax
from jax.experimental import pallas as pl
from jax.experimental.pallas import tpu as pltpu
from jax.sharding import Mesh
from jax.sharding import PartitionSpec as P


GRP = ("xl", "y")
SMP = ("xh", "zh", "zl", "c")
QUAD = ("xh", "zl")
SETS = ("xh", "zl", "c")
SWAP = [(0, 1), (1, 0)]
LAM = 0.01
ROWS = 32
NB = 8
TILE = 1024
LIMIT = 14
SUB = TILE // 128
EXTRA = 8
F32, BF16 = jnp.float32, jnp.bfloat16
VMEM = pl.BlockSpec(memory_space=pltpu.VMEM)
SMEM = pl.BlockSpec(memory_space=pltpu.SMEM)


def swap(x, axis):
    return lax.ppermute(x, axis, SWAP)


def to_all(x, axes, size):
    return lax.all_to_all(jnp.broadcast_to(x[None], (size, *x.shape)), axes, 0, 0, tiled=True)


def split_terms(x):
    hi = x.astype(BF16)
    return hi, (x - hi.astype(F32)).astype(BF16)


def resident(x):
    return pltpu.with_memory_space_constraint(x, pltpu.VMEM)


def call(kernel, ins, outs, scratch=(), flops=0):
    return pl.pallas_call(
        kernel,
        in_specs=ins,
        out_specs=[VMEM] * len(outs),
        out_shape=outs,
        scratch_shapes=scratch,
        compiler_params=pltpu.CompilerParams(vmem_limit_bytes=LIMIT << 20),
        cost_estimate=pl.CostEstimate(flops=flops, bytes_accessed=1 << 20, transcendentals=0),
    )


def cols(t):
    return pl.ds(pl.multiple_of(t * TILE, TILE), TILE)


def rows_to_column(rows):
    return jnp.concatenate(
        [jnp.broadcast_to(rows[k : k + 1, :], (128, 128)).T[:, :1] for k in range(rows.shape[0])], axis=0
    )


def total(x):
    return jnp.full((1, 128), jnp.sum(x), F32)


def to_rows(line):
    return jnp.concatenate([line[:, k * 128 : (k + 1) * 128] for k in range(line.shape[1] // 128)], axis=0)


def to_line(rows):
    return jnp.concatenate([rows[k : k + 1, :] for k in range(rows.shape[0])], axis=1)


def sub(t):
    return pl.ds(pl.multiple_of(t * SUB, SUB), SUB)


def hidden_kernel(pos_ref, x0, x1, x2, x3, w_ref, hb_ref, s_ref, h_ref, wt, packed_ref):
    units = wt.shape[0]
    for d, x in enumerate((x0, x1, x2, x3)):
        packed_ref[(pos_ref[32] + 4 - d) % 4] = x[...]
    for b in range(NB):
        rows = [w_ref[pl.ds(pl.multiple_of(pos_ref[4 * b + k] * ROWS, ROWS), ROWS), :] for k in range(4)]
        block = jnp.concatenate(rows, axis=0).astype(F32)
        wt[:, b * 128 : (b + 1) * 128] = block.T.astype(BF16)
    shifts = 31 - lax.broadcasted_iota(jnp.int32, (ROWS, TILE), 0)
    hb = rows_to_column(my_rows(pos_ref, hb_ref, units))

    def step(t, carry):
        for q in range(32):
            word = packed_ref[t, pl.ds(pos_ref[q], 1), :]
            up = jnp.left_shift(jnp.broadcast_to(word, (ROWS, TILE)), shifts) < 0
            s_ref[q * ROWS : (q + 1) * ROWS, cols(t)] = jnp.where(up, 1.0, -1.0).astype(BF16)
        pre = jnp.dot(wt[...], s_ref[:, cols(t)], preferred_element_type=F32)
        h_ref[:, cols(t)] = jnp.tanh(pre + hb)
        return carry

    lax.fori_loop(0, packed_ref.shape[0], step, 0)


def hidden_pass(pos, packed, w, hb, units):
    n = len(packed) * TILE
    return call(
        hidden_kernel,
        [SMEM] + [VMEM] * 6,
        [pltpu.VMEM((NB * 128, n), BF16), pltpu.VMEM((units, n), F32)],
        [pltpu.VMEM((units, NB * 128), BF16), pltpu.VMEM((len(packed), *packed[0].shape), jnp.int32)],
        flops=4 * 10**9,
    )(pos, *packed, w, hb)


def project(s_ref, h_ref, lhs, bias, p_ref):
    units = h_ref.shape[0]

    def step(t, carry):
        out = jnp.dot(lhs[...], s_ref[:, cols(t)], preferred_element_type=F32)
        proj = out[:units] + out[units:] + bias
        p_ref[sub(t), :] = to_rows(jnp.sum(h_ref[:, cols(t)] * proj, axis=0, keepdims=True))
        return carry

    lax.fori_loop(0, s_ref.shape[1] // TILE, step, 0)


def set_block(lhs, b, x):
    units = x.shape[0]
    hi, lo = split_terms(x)
    lhs[:units, b * 128 : (b + 1) * 128] = hi
    lhs[units:, b * 128 : (b + 1) * 128] = lo


def my_rows(pos_ref, ref, units):
    return ref[pl.ds(pos_ref[32] * (units // 128), units // 128), :]


def first_kernel(pos_ref, s_ref, h_ref, f0, f1, f2, f3, fb_ref, p_ref, lhs):
    units = h_ref.shape[0]
    norm = jnp.zeros((units, 128), F32)
    for b in range(NB):
        x = (f0, f1, f2, f3)[b // 2][b % 2]
        set_block(lhs, b, x)
        norm = norm + x * x
    fb = my_rows(pos_ref, fb_ref, units)
    n = p_ref.shape[0] - EXTRA
    p_ref[n:, :] = jnp.zeros((EXTRA, 128), F32)
    p_ref[n : n + 1, :] = total(norm) + total(fb * fb)
    project(s_ref, h_ref, lhs, rows_to_column(fb), p_ref)
    p_ref[n + 1 : n + 2, :] = total(p_ref[:n, :])


def first_pass(pos, spins, hidden, f, fb):
    units, n = hidden.shape
    return call(
        first_kernel,
        [SMEM] + [VMEM] * 7,
        [jax.ShapeDtypeStruct((n // 128 + EXTRA, 128), F32)],
        [pltpu.VMEM((2 * units, NB * 128), BF16)],
        flops=4 * 10**9,
    )(pos, resident(spins), resident(hidden), *f, fb)[0]


def step_of(norm, spread, samples, length):
    return norm / (spread / samples + LAM * length)


def second_kernel(samples, pos_ref, s_ref, h_ref, f0, f1, f2, f3, fb_ref, g0, g1, mine_ref, norm_ref, out_ref, lhs):
    units = h_ref.shape[0]
    norm0 = norm_ref[0:1, :]
    spread = g0[0, units + units // 128 : units + units // 128 + 1, :]
    a = step_of(norm0, spread, samples, norm0)
    rr = jnp.zeros((units, 128), F32)
    rf = jnp.zeros((units, 128), F32)
    for b in range(NB):
        f = (f0, f1, f2, f3)[b // 2][b % 2]
        g = (g0, g1)[b // 4][pos_ref[33 + b % 4], :units, :]
        r = f - a * (g + LAM * f)
        set_block(lhs, b, r)
        rr = rr + r * r
        rf = rf + r * f
    fb = my_rows(pos_ref, fb_ref, units)
    rb = fb - a * (g0[0, units : units + units // 128, :] + LAM * fb)
    n = h_ref.shape[1] // 128
    p_ref = out_ref.at[0]
    p_ref[n : n + EXTRA, :] = jnp.zeros((EXTRA, 128), F32)
    p_ref[n : n + 1, :] = total(rr) + total(rb * rb)
    p_ref[n + 1 : n + 2, :] = total(rf) + total(rb * fb)
    p_ref[n + 2 : n + 2 + units // 128, :] = g0[0, units : units + units // 128, :]
    p_ref[n + 2 + units // 128 : n + 3 + units // 128, :] = spread
    project(s_ref, h_ref, lhs, rows_to_column(rb), p_ref)
    for k in range(1, out_ref.shape[0]):
        out_ref[k, : n + EXTRA, :] = out_ref[0, : n + EXTRA, :]
    for k in range(out_ref.shape[0]):
        to = (pos_ref[32] + 4 - k) % 4
        for h in range(units // 128):
            at = n + EXTRA + h * ROWS
            out_ref[to, at : at + ROWS, :] = mine_ref[k * ROWS : (k + 1) * ROWS, h * 128 : (h + 1) * 128]


def second_pass(samples, pos, spins, hidden, f, fb, g0, g1, mine, norm):
    units, n = hidden.shape
    parts = mine.shape[0] // ROWS
    return call(
        functools.partial(second_kernel, samples),
        [SMEM] + [VMEM] * 11,
        [jax.ShapeDtypeStruct((parts, n // 128 + EXTRA + units // 128 * ROWS, 128), F32)],
        [pltpu.VMEM((2 * units, NB * 128), BF16)],
        flops=4 * 10**9,
    )(pos, resident(spins), resident(hidden), *f, fb, g0, g1, mine, norm)[0]


def put_stats(v, st_ref):
    mean = jnp.sum(v) / v.size
    st_ref[0:1, :] = jnp.full((1, 128), mean, F32)
    st_ref[1:2, :] = total((v - mean) ** 2)
    st_ref[2:, :] = jnp.zeros((st_ref.shape[0] - 2, 128), F32)


def over_chain_kernel(got_ref, all_ref):
    rows = all_ref.shape[1]
    x = got_ref[0, :rows, :]
    for k in range(1, got_ref.shape[0]):
        x = x + got_ref[k, :rows, :]
    for k in range(all_ref.shape[0]):
        all_ref[k] = x


def over_groups(got, rows):
    (x,) = call(over_chain_kernel, [VMEM], [jax.ShapeDtypeStruct((lax.axis_size(GRP), rows, 128), F32)])(got)
    return lax.all_to_all(x, GRP, 0, 0, tiled=True)


def summed(got_ref):
    x = got_ref[0]
    for k in range(1, got_ref.shape[0]):
        x = x + got_ref[k]
    n = x.shape[0] - EXTRA
    return x[:n], x[n:]


def sum_of_set(got_ref, mine, stride, count):
    x = got_ref[mine]
    for k in range(1, count):
        x = x + got_ref[mine + k * stride]
    n = x.shape[0] - EXTRA
    everyone = got_ref[0, n + 1 : n + 2, :]
    for k in range(1, got_ref.shape[0]):
        everyone = everyone + got_ref[k, n + 1 : n + 2, :]
    return x, everyone, n


def first_chain_kernel(pos_ref, got_ref, all_ref):
    x, everyone, n = sum_of_set(got_ref, pos_ref[37], 2, got_ref.shape[0] // 2)
    for k in range(all_ref.shape[0]):
        all_ref[k] = x
        all_ref[k, n + 1 : n + 2, :] = everyone


def first_sum_kernel(pos_ref, got_ref, v_ref, extra_ref):
    peers = got_ref.shape[0] // 2
    x, everyone, n = sum_of_set(got_ref, pos_ref[38] * peers, 1, peers)
    v_ref[...] = x[:n]
    extra_ref[...] = x[n:]
    extra_ref[1:2, :] = everyone


def first_sum(pos, partial):
    shape = lambda *s: jax.ShapeDtypeStruct(s, F32)
    rows = partial.shape[0]
    chain, plane = ("zh", "zl"), ("xh", *GRP)
    got = to_all(partial, chain, lax.axis_size(chain))
    (x,) = call(first_chain_kernel, [SMEM, VMEM], [shape(lax.axis_size(plane), rows, 128)])(pos, got)
    got = lax.all_to_all(x, plane, 0, 0, tiled=True)
    return call(first_sum_kernel, [SMEM, VMEM], [shape(rows - EXTRA, 128), shape(EXTRA, 128)])(pos, got)


def second_sum_kernel(got_ref, v_ref, norm_ref, st_ref, next_ref):
    u, extra = summed(got_ref)
    next_ref[...] = extra
    beta = extra[0:1, 0:1] / norm_ref[0:1, 0:1]
    put_stats(u + beta * v_ref[...], st_ref)


def second_sum(got, values, norm):
    shape = lambda *s: jax.ShapeDtypeStruct(s, F32)
    return call(second_sum_kernel, [VMEM] * 3, [shape(8, 128), shape(EXTRA, 128)])(
        got, values, norm
    )


def of_sets(st):
    return to_all(st, SETS, lax.axis_size(SETS))


def joined(st_ref, count):
    sets = st_ref.shape[0]
    mean = st_ref[0, 0:1, :]
    for k in range(1, sets):
        mean = mean + st_ref[k, 0:1, :]
    mean = mean * (1.0 / sets)
    spread = jnp.zeros_like(mean)
    for k in range(sets):
        off = st_ref[k, 0:1, :] - mean
        spread = spread + (st_ref[k, 1:2, :] + count * (off * off))
    return mean, spread


def columns_kernel(pos_ref, f_ref, o0, o1, o2, o3):
    units = o0.shape[1]
    for d, out in enumerate((o0, o1, o2, o3)):
        to = (pos_ref[32] + d) % 4
        out[...] = f_ref[:, pl.ds(pl.multiple_of(to * units, units), units)]


def columns_of(pos, f, units):
    out = jax.ShapeDtypeStruct((f.shape[0], units), F32)
    return call(columns_kernel, [SMEM, VMEM], [out] * 4)(pos, f)


def turned_kernel(f0, f1, f2, f3, out_ref):
    out_ref[0] = jnp.concatenate([f0[...], f1[...], f2[...], f3[...]], axis=0).T


def turned(f):
    rows, units = f[0].shape
    out = jax.ShapeDtypeStruct((1, units, rows * 4), F32)
    return call(turned_kernel, [VMEM] * 4, [out])(*f)[0]


def image_kernel(samples, pos_ref, s_ref, h_ref, v_ref, near_ref, far_ref, keep_ref, send_ref, acc, lanes):
    units = h_ref.shape[0]
    mean = (near_ref[1:2, 0:1] + far_ref[1:2, 0:1]) * (1.0 / samples)
    spread = total((v_ref[...] - mean) ** 2)
    acc[...] = jnp.zeros(acc.shape, F32)
    lanes[...] = jnp.zeros(lanes.shape, F32)

    def step(t, carry):
        r = h_ref[:, cols(t)] * to_line((v_ref[sub(t), :] - mean) * (1.0 / samples))
        both = jnp.concatenate(split_terms(r), axis=0)
        out = lax.dot_general(both, s_ref[:, cols(t)], (((1,), (1,)), ((), ())), preferred_element_type=F32)
        acc[...] += out[:units] + out[units:]
        part = r[:, :128]
        for k in range(1, TILE // 128):
            part = part + r[:, k * 128 : (k + 1) * 128]
        lanes[...] += part
        return carry

    lax.fori_loop(0, s_ref.shape[1] // TILE, step, 0)
    bias = [
        jnp.sum(lanes[k * 128 : (k + 1) * 128, :].T, axis=0, keepdims=True) for k in range(units // 128)
    ] + [spread, jnp.zeros((7 - units // 128, 128), F32)]
    bias = jnp.concatenate(bias, axis=0)
    for b in range(NB):
        ref = (keep_ref, send_ref)[b // 4]
        at = pos_ref[33 + b % 4]
        ref[at, :units, :] = acc[:, b * 128 : (b + 1) * 128]
        ref[at, units:, :] = bias


def image_pass(samples, pos, spins, hidden, values, near, far):
    units = hidden.shape[0]
    return call(
        functools.partial(image_kernel, samples),
        [SMEM] + [VMEM] * 5,
        [jax.ShapeDtypeStruct((4, units + 8, 128), F32)] * 2,
        [pltpu.VMEM((units, NB * 128), F32), pltpu.VMEM((units, 128), F32)],
        flops=4 * 10**9,
    )(pos, resident(spins), resident(hidden), values, near, far)


def image_sum_kernel(got_ref, all_ref, mine_ref):
    units = mine_ref.shape[1]
    x = got_ref[0] + got_ref[1] + (got_ref[2] + got_ref[3])
    for k in range(4):
        all_ref[k] = x
    mine_ref[...] = x[:units].T


def image_sum(got, units):
    shape = lambda *s: jax.ShapeDtypeStruct(s, F32)
    return call(image_sum_kernel, [VMEM], [shape(*got.shape), shape(128, units)])(got)


def update_kernel(samples, f_ref, fb_ref, got_ref, norm_ref, st1_ref, next_ref, w_ref, b_ref):
    parts = got_ref.shape[0]
    per = f_ref.shape[1] // 128 // parts
    n = got_ref.shape[1] - EXTRA - per * ROWS
    count = samples // st1_ref.shape[0]
    norm0, norm1 = norm_ref[0:1, 0:1], next_ref[0:1, 0:1]
    cross = next_ref[1:2, 0:1]
    beta = norm1 / norm0
    step0 = step_of(norm0, got_ref[0, n + 2 + per : n + 3 + per, 0:1], samples, norm0)
    step1 = step_of(norm1, joined(st1_ref, count)[1][:, 0:1], samples, norm1 + 2.0 * beta * cross + beta * beta * norm0)

    def update(f, g):
        r = f - step0 * (g + LAM * f)
        return step0 * f + step1 * (r + beta * f)

    for k in range(parts):
        for h in range(per):
            b = k * per + h
            at = n + EXTRA + h * ROWS
            w_ref[:, b * 128 : (b + 1) * 128] = update(f_ref[:, b * 128 : (b + 1) * 128], got_ref[k, at : at + ROWS, :])
            b_ref[b : b + 1, :] = update(fb_ref[b : b + 1, :], got_ref[k, n + 2 + h : n + 3 + h, :])


def update_pass(samples, f, fb, got, norm, st1, norms):
    shape = lambda s: jax.ShapeDtypeStruct(s, F32)
    return call(
        functools.partial(update_kernel, samples), [VMEM] * 6, [shape(f.shape), shape(fb.shape)]
    )(f, fb, got, norm, st1, norms)


def body(spins_packed, weight, hidden_bias, force_w, force_b):
    xh, zh, zl, c = (lax.axis_index(a) for a in SMP)
    parts = lax.axis_size("zh")
    units = weight.shape[1] // parts
    samples = spins_packed.shape[1] * lax.axis_size(SMP)
    hb = hidden_bias.reshape(-1, 128)
    fb = force_b.reshape(-1, 128)

    q = jnp.arange(32, dtype=jnp.int32)
    words = (((q >> 2) & 1) ^ xh) * 16 + ((zh - q) & 3) * 4 + (((q >> 3) & 1) ^ zl) * 2 + ((q >> 4) ^ c)
    k = jnp.arange(4, dtype=jnp.int32)
    blocks = ((k & 1) ^ xh) * 2 + ((k >> 1) ^ zl)
    pos = jnp.concatenate([words, zh.reshape(1), blocks, zl.reshape(1), xh.reshape(1)])

    turn = lambda x, d: lax.ppermute(x, "zh", [(i, (i + d) % parts) for i in range(parts)])
    f = list(columns_of(pos, force_w, units))
    for d in (1, 2, 3):
        f[d] = turn(f[d], d)

    packed = [spins_packed]
    for d in (1, 2, 3):
        packed.append(turn(spins_packed, d))

    f = turned(f)
    f_xh = swap(f, "xh")
    f = jnp.concatenate([f, f_xh], axis=0)
    f_zl = swap(f, "zl")
    f = (f, f_zl, swap(f, "c"), swap(f_zl, "c"))

    w = lax.dynamic_slice_in_dim(weight, zh * units, units, 1)
    spins, hidden = hidden_pass(pos, packed, w, hb, units)
    partial = first_pass(pos, spins, hidden, f, fb)
    rows = partial.shape[0]
    values, norm = first_sum(pos, partial)
    norm_far = swap(norm, "c")

    keep, send = image_pass(samples, pos, spins, hidden, values, norm, norm_far)
    g = keep + swap(send, "c")
    g, mine = image_sum(lax.all_to_all(g, QUAD, 0, 0, tiled=True), units)
    g = lax.all_to_all(g, QUAD, 0, 0, tiled=True)

    partial = second_pass(samples, pos, spins, hidden, f, fb, g, swap(g, "c"), mine, norm)
    got = lax.all_to_all(partial, "zh", 0, 0, tiled=True)
    st, norms = second_sum(over_groups(got, rows), values, norm)
    st1 = of_sets(st)
    out_w, out_b = update_pass(samples, force_w, fb, got, norm, st1, norms)
    return out_w, out_b.reshape(-1)


def solution(mesh):
    torus = Mesh(mesh.devices.reshape(2, 4, 2, 4, 2, 2), ("xl", "y", "xh", "zh", "zl", "c"))
    in_specs = (P(None, SMP), P(None, GRP), P(GRP), P(SMP, GRP), P(GRP))
    out_specs = (P(SMP, GRP), P(GRP))
    return jax.shard_map(body, mesh=torus, in_specs=in_specs, out_specs=out_specs, check_vma=False)
```

```python
import functools

import jax
import jax.numpy as jnp
from jax import lax
from jax.experimental import pallas as pl
from jax.experimental.pallas import tpu as pltpu
from jax.sharding import Mesh
from jax.sharding import PartitionSpec as P


GRP = ("xl", "y")
SMP = ("xh", "zh", "zl", "c")
QUAD = ("xh", "zl")
SETS = ("xh", "zl", "c")
SWAP = [(0, 1), (1, 0)]
LAM = 0.01
ROWS = 32
NB = 8
TILE = 1024
LIMIT = 14
SUB = TILE // 128
EXTRA = 8
F32, BF16 = jnp.float32, jnp.bfloat16
VMEM = pl.BlockSpec(memory_space=pltpu.VMEM)
SMEM = pl.BlockSpec(memory_space=pltpu.SMEM)


def swap(x, axis):
    return lax.ppermute(x, axis, SWAP)


def to_all(x, axes, size):
    return lax.all_to_all(jnp.broadcast_to(x[None], (size, *x.shape)), axes, 0, 0, tiled=True)


def split_terms(x):
    hi = x.astype(BF16)
    return hi, (x - hi.astype(F32)).astype(BF16)


def resident(x):
    return pltpu.with_memory_space_constraint(x, pltpu.VMEM)


def call(kernel, ins, outs, scratch=(), flops=0):
    return pl.pallas_call(
        kernel,
        in_specs=ins,
        out_specs=[VMEM] * len(outs),
        out_shape=outs,
        scratch_shapes=scratch,
        compiler_params=pltpu.CompilerParams(vmem_limit_bytes=LIMIT << 20),
        cost_estimate=pl.CostEstimate(flops=flops, bytes_accessed=1 << 20, transcendentals=0),
    )


def cols(t):
    return pl.ds(pl.multiple_of(t * TILE, TILE), TILE)


def rows_to_column(rows):
    return jnp.concatenate(
        [jnp.broadcast_to(rows[k : k + 1, :], (128, 128)).T[:, :1] for k in range(rows.shape[0])], axis=0
    )


def total(x):
    return jnp.full((1, 128), jnp.sum(x), F32)


def to_rows(line):
    return jnp.concatenate([line[:, k * 128 : (k + 1) * 128] for k in range(line.shape[1] // 128)], axis=0)


def to_line(rows):
    return jnp.concatenate([rows[k : k + 1, :] for k in range(rows.shape[0])], axis=1)


def sub(t):
    return pl.ds(pl.multiple_of(t * SUB, SUB), SUB)


def hidden_kernel(pos_ref, x0, x1, x2, x3, w_ref, hb_ref, s_ref, h_ref, wt, packed_ref):
    units = wt.shape[0]
    for d, x in enumerate((x0, x1, x2, x3)):
        packed_ref[(pos_ref[32] + 4 - d) % 4] = x[...]
    for b in range(NB):
        rows = [w_ref[pl.ds(pl.multiple_of(pos_ref[4 * b + k] * ROWS, ROWS), ROWS), :] for k in range(4)]
        block = jnp.concatenate(rows, axis=0).astype(F32)
        wt[:, b * 128 : (b + 1) * 128] = block.T.astype(BF16)
    shifts = 31 - lax.broadcasted_iota(jnp.int32, (ROWS, TILE), 0)
    hb = rows_to_column(my_rows(pos_ref, hb_ref, units))

    def step(t, carry):
        for q in range(32):
            word = packed_ref[t, pl.ds(pos_ref[q], 1), :]
            up = jnp.left_shift(jnp.broadcast_to(word, (ROWS, TILE)), shifts) < 0
            s_ref[q * ROWS : (q + 1) * ROWS, cols(t)] = jnp.where(up, 1.0, -1.0).astype(BF16)
        pre = jnp.dot(wt[...], s_ref[:, cols(t)], preferred_element_type=F32)
        h_ref[:, cols(t)] = jnp.tanh(pre + hb)
        return carry

    lax.fori_loop(0, packed_ref.shape[0], step, 0)


def hidden_pass(pos, packed, w, hb, units):
    n = len(packed) * TILE
    return call(
        hidden_kernel,
        [SMEM] + [VMEM] * 6,
        [pltpu.VMEM((NB * 128, n), BF16), pltpu.VMEM((units, n), F32)],
        [pltpu.VMEM((units, NB * 128), BF16), pltpu.VMEM((len(packed), *packed[0].shape), jnp.int32)],
        flops=4 * 10**9,
    )(pos, *packed, w, hb)


def project(s_ref, h_ref, lhs, bias, p_ref):
    units = h_ref.shape[0]

    def step(t, carry):
        out = jnp.dot(lhs[...], s_ref[:, cols(t)], preferred_element_type=F32)
        proj = out[:units] + out[units:] + bias
        p_ref[sub(t), :] = to_rows(jnp.sum(h_ref[:, cols(t)] * proj, axis=0, keepdims=True))
        return carry

    lax.fori_loop(0, s_ref.shape[1] // TILE, step, 0)


def set_block(lhs, b, x):
    units = x.shape[0]
    hi, lo = split_terms(x)
    lhs[:units, b * 128 : (b + 1) * 128] = hi
    lhs[units:, b * 128 : (b + 1) * 128] = lo


def my_rows(pos_ref, ref, units):
    return ref[pl.ds(pos_ref[32] * (units // 128), units // 128), :]


def first_kernel(pos_ref, s_ref, h_ref, f0, f1, f2, f3, fb_ref, p_ref, lhs):
    units = h_ref.shape[0]
    norm = jnp.zeros((units, 128), F32)
    for b in range(NB):
        x = (f0, f1, f2, f3)[b // 2][b % 2]
        set_block(lhs, b, x)
        norm = norm + x * x
    fb = my_rows(pos_ref, fb_ref, units)
    n = p_ref.shape[0] - EXTRA
    p_ref[n:, :] = jnp.zeros((EXTRA, 128), F32)
    p_ref[n : n + 1, :] = total(norm) + total(fb * fb)
    project(s_ref, h_ref, lhs, rows_to_column(fb), p_ref)
    p_ref[n + 1 : n + 2, :] = total(p_ref[:n, :])


def first_pass(pos, spins, hidden, f, fb):
    units, n = hidden.shape
    return call(
        first_kernel,
        [SMEM] + [VMEM] * 7,
        [jax.ShapeDtypeStruct((n // 128 + EXTRA, 128), F32)],
        [pltpu.VMEM((2 * units, NB * 128), BF16)],
        flops=4 * 10**9,
    )(pos, resident(spins), resident(hidden), *f, fb)[0]


def step_of(norm, spread, samples, length):
    return norm / (spread / samples + LAM * length)


def second_kernel(samples, pos_ref, s_ref, h_ref, f0, f1, f2, f3, fb_ref, *refs):
    *g, mine_ref, norm_ref, out_ref, lhs = refs
    units = h_ref.shape[0]
    norm0 = norm_ref[0:1, :]
    spread = g[0][units + units // 128 : units + units // 128 + 1, :]
    a = step_of(norm0, spread, samples, norm0)
    rr = jnp.zeros((units, 128), F32)
    rf = jnp.zeros((units, 128), F32)
    for b in range(NB):
        f = (f0, f1, f2, f3)[b // 2][b % 2]
        r = f - a * (g[b][:units, :] + LAM * f)
        set_block(lhs, b, r)
        rr = rr + r * r
        rf = rf + r * f
    fb = my_rows(pos_ref, fb_ref, units)
    rb = fb - a * (g[0][units : units + units // 128, :] + LAM * fb)
    n = h_ref.shape[1] // 128
    p_ref = out_ref.at[0]
    p_ref[n : n + EXTRA, :] = jnp.zeros((EXTRA, 128), F32)
    p_ref[n : n + 1, :] = total(rr) + total(rb * rb)
    p_ref[n + 1 : n + 2, :] = total(rf) + total(rb * fb)
    p_ref[n + 2 : n + 2 + units // 128, :] = g[0][units : units + units // 128, :]
    p_ref[n + 2 + units // 128 : n + 3 + units // 128, :] = spread
    project(s_ref, h_ref, lhs, rows_to_column(rb), p_ref)
    for k in range(1, out_ref.shape[0]):
        out_ref[k, : n + EXTRA, :] = out_ref[0, : n + EXTRA, :]
    for k in range(out_ref.shape[0]):
        to = (pos_ref[32] + 4 - k) % 4
        for h in range(units // 128):
            at = n + EXTRA + h * ROWS
            out_ref[to, at : at + ROWS, :] = mine_ref[k * ROWS : (k + 1) * ROWS, h * 128 : (h + 1) * 128]


def second_pass(samples, pos, spins, hidden, f, fb, g, mine, norm):
    units, n = hidden.shape
    parts = mine.shape[0] // ROWS
    return call(
        functools.partial(second_kernel, samples),
        [SMEM] + [VMEM] * (9 + NB),
        [jax.ShapeDtypeStruct((parts, n // 128 + EXTRA + units // 128 * ROWS, 128), F32)],
        [pltpu.VMEM((2 * units, NB * 128), BF16)],
        flops=4 * 10**9,
    )(pos, resident(spins), resident(hidden), *f, fb, *g, mine, norm)[0]


def put_stats(v, st_ref):
    mean = jnp.sum(v) / v.size
    st_ref[0:1, :] = jnp.full((1, 128), mean, F32)
    st_ref[1:2, :] = total((v - mean) ** 2)
    st_ref[2:, :] = jnp.zeros((st_ref.shape[0] - 2, 128), F32)


def over_chain_kernel(got_ref, all_ref):
    rows = all_ref.shape[1]
    x = got_ref[0, :rows, :]
    for k in range(1, got_ref.shape[0]):
        x = x + got_ref[k, :rows, :]
    for k in range(all_ref.shape[0]):
        all_ref[k] = x


def over_groups(got, rows):
    (x,) = call(over_chain_kernel, [VMEM], [jax.ShapeDtypeStruct((lax.axis_size(GRP), rows, 128), F32)])(got)
    return lax.all_to_all(x, GRP, 0, 0, tiled=True)


def summed(got_ref):
    x = got_ref[0]
    for k in range(1, got_ref.shape[0]):
        x = x + got_ref[k]
    n = x.shape[0] - EXTRA
    return x[:n], x[n:]


def sum_of_set(got_ref, mine, stride, count):
    x = got_ref[mine]
    for k in range(1, count):
        x = x + got_ref[mine + k * stride]
    n = x.shape[0] - EXTRA
    everyone = got_ref[0, n + 1 : n + 2, :]
    for k in range(1, got_ref.shape[0]):
        everyone = everyone + got_ref[k, n + 1 : n + 2, :]
    return x, everyone, n


def first_chain_kernel(pos_ref, got_ref, all_ref):
    x, everyone, n = sum_of_set(got_ref, pos_ref[37], 2, got_ref.shape[0] // 2)
    for k in range(all_ref.shape[0]):
        all_ref[k] = x
        all_ref[k, n + 1 : n + 2, :] = everyone


def first_sum_kernel(pos_ref, got_ref, v_ref, extra_ref):
    peers = got_ref.shape[0] // 2
    x, everyone, n = sum_of_set(got_ref, pos_ref[38] * peers, 1, peers)
    v_ref[...] = x[:n]
    extra_ref[...] = x[n:]
    extra_ref[1:2, :] = everyone


def first_sum(pos, partial):
    shape = lambda *s: jax.ShapeDtypeStruct(s, F32)
    rows = partial.shape[0]
    chain, plane = ("zh", "zl"), ("xh", *GRP)
    got = to_all(partial, chain, lax.axis_size(chain))
    (x,) = call(first_chain_kernel, [SMEM, VMEM], [shape(lax.axis_size(plane), rows, 128)])(pos, got)
    got = lax.all_to_all(x, plane, 0, 0, tiled=True)
    return call(first_sum_kernel, [SMEM, VMEM], [shape(rows - EXTRA, 128), shape(EXTRA, 128)])(pos, got)


def second_sum_kernel(got_ref, v_ref, norm_ref, st_ref, next_ref):
    u, extra = summed(got_ref)
    next_ref[...] = extra
    beta = extra[0:1, 0:1] / norm_ref[0:1, 0:1]
    put_stats(u + beta * v_ref[...], st_ref)


def second_sum(got, values, norm):
    shape = lambda *s: jax.ShapeDtypeStruct(s, F32)
    return call(second_sum_kernel, [VMEM] * 3, [shape(8, 128), shape(EXTRA, 128)])(
        got, values, norm
    )


def of_sets(st):
    return to_all(st, SETS, lax.axis_size(SETS))


def joined(st_ref, count):
    sets = st_ref.shape[0]
    mean = st_ref[0, 0:1, :]
    for k in range(1, sets):
        mean = mean + st_ref[k, 0:1, :]
    mean = mean * (1.0 / sets)
    spread = jnp.zeros_like(mean)
    for k in range(sets):
        off = st_ref[k, 0:1, :] - mean
        spread = spread + (st_ref[k, 1:2, :] + count * (off * off))
    return mean, spread


def columns_kernel(pos_ref, f_ref, o0, o1, o2, o3):
    units = o0.shape[1]
    for d, out in enumerate((o0, o1, o2, o3)):
        to = (pos_ref[32] + d) % 4
        out[...] = f_ref[:, pl.ds(pl.multiple_of(to * units, units), units)]


def columns_of(pos, f, units):
    out = jax.ShapeDtypeStruct((f.shape[0], units), F32)
    return call(columns_kernel, [SMEM, VMEM], [out] * 4)(pos, f)


def turned_kernel(f0, f1, f2, f3, out_ref):
    out_ref[0] = jnp.concatenate([f0[...], f1[...], f2[...], f3[...]], axis=0).T


def turned(f):
    rows, units = f[0].shape
    out = jax.ShapeDtypeStruct((1, units, rows * 4), F32)
    return call(turned_kernel, [VMEM] * 4, [out])(*f)[0]


def image_kernel(samples, pos_ref, s_ref, h_ref, v_ref, near_ref, far_ref, keep_ref, send_ref, acc, lanes):
    units = h_ref.shape[0]
    mean = (near_ref[1:2, 0:1] + far_ref[1:2, 0:1]) * (1.0 / samples)
    spread = total((v_ref[...] - mean) ** 2)
    acc[...] = jnp.zeros(acc.shape, F32)
    lanes[...] = jnp.zeros(lanes.shape, F32)

    def step(t, carry):
        r = h_ref[:, cols(t)] * to_line((v_ref[sub(t), :] - mean) * (1.0 / samples))
        both = jnp.concatenate(split_terms(r), axis=0)
        out = lax.dot_general(both, s_ref[:, cols(t)], (((1,), (1,)), ((), ())), preferred_element_type=F32)
        acc[...] += out[:units] + out[units:]
        part = r[:, :128]
        for k in range(1, TILE // 128):
            part = part + r[:, k * 128 : (k + 1) * 128]
        lanes[...] += part
        return carry

    lax.fori_loop(0, s_ref.shape[1] // TILE, step, 0)
    bias = [
        jnp.sum(lanes[k * 128 : (k + 1) * 128, :].T, axis=0, keepdims=True) for k in range(units // 128)
    ] + [spread, jnp.zeros((7 - units // 128, 128), F32)]
    bias = jnp.concatenate(bias, axis=0)
    for b in range(NB):
        ref = (keep_ref, send_ref)[b // 4]
        at = b % 4
        ref[at, :units, :] = acc[:, b * 128 : (b + 1) * 128]
        ref[at, units:, :] = bias


def image_pass(samples, pos, spins, hidden, values, near, far):
    units = hidden.shape[0]
    return call(
        functools.partial(image_kernel, samples),
        [SMEM] + [VMEM] * 5,
        [jax.ShapeDtypeStruct((4, units + 8, 128), F32)] * 2,
        [pltpu.VMEM((units, NB * 128), F32), pltpu.VMEM((units, 128), F32)],
        flops=4 * 10**9,
    )(pos, resident(spins), resident(hidden), values, near, far)


def halves_kernel(keep_ref, got_ref, o0, o1, o2, o3):
    for k, out in enumerate((o0, o1, o2, o3)):
        out[...] = keep_ref[k] + got_ref[k]


def halves(keep, got):
    return call(halves_kernel, [VMEM] * 2, [jax.ShapeDtypeStruct(keep.shape[1:], F32)] * 4)(keep, got)


def image_sum_kernel(g0, g1, g2, g3, all_ref, mine_ref):
    units = mine_ref.shape[1]
    x = g0[...] + g1[...] + (g2[...] + g3[...])
    all_ref[...] = x
    mine_ref[...] = x[:units].T


def image_sum(g, units):
    shape = lambda *s: jax.ShapeDtypeStruct(s, F32)
    return call(image_sum_kernel, [VMEM] * 4, [shape(*g[0].shape), shape(128, units)])(*g)


def to_quad(blocks):
    return [
        blocks[0],
        swap(blocks[1], "xh"),
        swap(blocks[2], "zl"),
        lax.ppermute(blocks[3], QUAD, [(i, i ^ 3) for i in range(4)]),
    ]


def update_kernel(samples, f_ref, fb_ref, got_ref, norm_ref, st1_ref, next_ref, w_ref, b_ref):
    parts = got_ref.shape[0]
    per = f_ref.shape[1] // 128 // parts
    n = got_ref.shape[1] - EXTRA - per * ROWS
    count = samples // st1_ref.shape[0]
    norm0, norm1 = norm_ref[0:1, 0:1], next_ref[0:1, 0:1]
    cross = next_ref[1:2, 0:1]
    beta = norm1 / norm0
    step0 = step_of(norm0, got_ref[0, n + 2 + per : n + 3 + per, 0:1], samples, norm0)
    step1 = step_of(norm1, joined(st1_ref, count)[1][:, 0:1], samples, norm1 + 2.0 * beta * cross + beta * beta * norm0)

    def update(f, g):
        r = f - step0 * (g + LAM * f)
        return step0 * f + step1 * (r + beta * f)

    for k in range(parts):
        for h in range(per):
            b = k * per + h
            at = n + EXTRA + h * ROWS
            w_ref[:, b * 128 : (b + 1) * 128] = update(f_ref[:, b * 128 : (b + 1) * 128], got_ref[k, at : at + ROWS, :])
            b_ref[b : b + 1, :] = update(fb_ref[b : b + 1, :], got_ref[k, n + 2 + h : n + 3 + h, :])


def update_pass(samples, f, fb, got, norm, st1, norms):
    shape = lambda s: jax.ShapeDtypeStruct(s, F32)
    return call(
        functools.partial(update_kernel, samples), [VMEM] * 6, [shape(f.shape), shape(fb.shape)]
    )(f, fb, got, norm, st1, norms)


def body(spins_packed, weight, hidden_bias, force_w, force_b):
    xh, zh, zl, c = (lax.axis_index(a) for a in SMP)
    parts = lax.axis_size("zh")
    units = weight.shape[1] // parts
    samples = spins_packed.shape[1] * lax.axis_size(SMP)
    hb = hidden_bias.reshape(-1, 128)
    fb = force_b.reshape(-1, 128)

    q = jnp.arange(32, dtype=jnp.int32)
    words = (((q >> 2) & 1) ^ xh) * 16 + ((zh - q) & 3) * 4 + (((q >> 3) & 1) ^ zl) * 2 + ((q >> 4) ^ c)
    k = jnp.arange(4, dtype=jnp.int32)
    blocks = ((k & 1) ^ xh) * 2 + ((k >> 1) ^ zl)
    pos = jnp.concatenate([words, zh.reshape(1), blocks, zl.reshape(1), xh.reshape(1)])

    turn = lambda x, d: lax.ppermute(x, "zh", [(i, (i + d) % parts) for i in range(parts)])
    f = list(columns_of(pos, force_w, units))
    for d in (1, 2, 3):
        f[d] = turn(f[d], d)

    packed = [spins_packed]
    for d in (1, 2, 3):
        packed.append(turn(spins_packed, d))

    f = turned(f)
    f_xh = swap(f, "xh")
    f = jnp.concatenate([f, f_xh], axis=0)
    f_zl = swap(f, "zl")
    f = (f, f_zl, swap(f, "c"), swap(f_zl, "c"))

    w = lax.dynamic_slice_in_dim(weight, zh * units, units, 1)
    spins, hidden = hidden_pass(pos, packed, w, hb, units)
    partial = first_pass(pos, spins, hidden, f, fb)
    rows = partial.shape[0]
    values, norm = first_sum(pos, partial)
    norm_far = swap(norm, "c")

    keep, send = image_pass(samples, pos, spins, hidden, values, norm, norm_far)
    g, mine = image_sum(to_quad(halves(keep, swap(send, "c"))), units)
    g = to_quad([g] * 4)
    g += [swap(x, "c") for x in g]

    partial = second_pass(samples, pos, spins, hidden, f, fb, g, mine, norm)
    got = lax.all_to_all(partial, "zh", 0, 0, tiled=True)
    st, norms = second_sum(over_groups(got, rows), values, norm)
    st1 = of_sets(st)
    out_w, out_b = update_pass(samples, force_w, fb, got, norm, st1, norms)
    return out_w, out_b.reshape(-1)


def solution(mesh):
    torus = Mesh(mesh.devices.reshape(2, 4, 2, 4, 2, 2), ("xl", "y", "xh", "zh", "zl", "c"))
    in_specs = (P(None, SMP), P(None, GRP), P(GRP), P(SMP, GRP), P(GRP))
    out_specs = (P(SMP, GRP), P(GRP))
    return jax.shard_map(body, mesh=torus, in_specs=in_specs, out_specs=out_specs, check_vma=False)
```

```python
import functools

import jax
import jax.numpy as jnp
from jax import lax
from jax.experimental import pallas as pl
from jax.experimental.pallas import tpu as pltpu
from jax.sharding import Mesh
from jax.sharding import PartitionSpec as P


GRP = ("xl", "y")
SMP = ("xh", "zh", "zl", "c")
QUAD = ("xh", "zl")
SWAP = [(0, 1), (1, 0)]
LAM = 0.01
ROWS = 32
NB = 8
TILE = 1024
LIMIT = 14
SUB = TILE // 128
EXTRA = 8
F32, BF16 = jnp.float32, jnp.bfloat16
VMEM = pl.BlockSpec(memory_space=pltpu.VMEM)
SMEM = pl.BlockSpec(memory_space=pltpu.SMEM)


def swap(x, axis):
    return lax.ppermute(x, axis, SWAP)


def to_all(x, axes, size):
    return lax.all_to_all(jnp.broadcast_to(x[None], (size, *x.shape)), axes, 0, 0, tiled=True)


def split_terms(x):
    hi = x.astype(BF16)
    return hi, (x - hi.astype(F32)).astype(BF16)


def resident(x):
    return pltpu.with_memory_space_constraint(x, pltpu.VMEM)


def call(kernel, ins, outs, scratch=(), flops=0):
    return pl.pallas_call(
        kernel,
        in_specs=ins,
        out_specs=[VMEM] * len(outs),
        out_shape=outs,
        scratch_shapes=scratch,
        compiler_params=pltpu.CompilerParams(vmem_limit_bytes=LIMIT << 20),
        cost_estimate=pl.CostEstimate(flops=flops, bytes_accessed=1 << 20, transcendentals=0),
    )


def cols(t):
    return pl.ds(pl.multiple_of(t * TILE, TILE), TILE)


def rows_to_column(rows):
    return jnp.concatenate(
        [jnp.broadcast_to(rows[k : k + 1, :], (128, 128)).T[:, :1] for k in range(rows.shape[0])], axis=0
    )


def total(x):
    return jnp.full((1, 128), jnp.sum(x), F32)


def to_rows(line):
    return jnp.concatenate([line[:, k * 128 : (k + 1) * 128] for k in range(line.shape[1] // 128)], axis=0)


def to_line(rows):
    return jnp.concatenate([rows[k : k + 1, :] for k in range(rows.shape[0])], axis=1)


def sub(t):
    return pl.ds(pl.multiple_of(t * SUB, SUB), SUB)


def hidden_kernel(pos_ref, x0, x1, x2, x3, w_ref, hb_ref, s_ref, h_ref, wt, packed_ref):
    units = wt.shape[0]
    for d, x in enumerate((x0, x1, x2, x3)):
        packed_ref[(pos_ref[32] + 4 - d) % 4] = x[...]
    for b in range(NB):
        rows = [w_ref[pl.ds(pl.multiple_of(pos_ref[4 * b + k] * ROWS, ROWS), ROWS), :] for k in range(4)]
        block = jnp.concatenate(rows, axis=0).astype(F32)
        wt[:, b * 128 : (b + 1) * 128] = block.T.astype(BF16)
    shifts = 31 - lax.broadcasted_iota(jnp.int32, (ROWS, TILE), 0)
    hb = rows_to_column(my_rows(pos_ref, hb_ref, units))

    def step(t, carry):
        for q in range(32):
            word = packed_ref[t, pl.ds(pos_ref[q], 1), :]
            up = jnp.left_shift(jnp.broadcast_to(word, (ROWS, TILE)), shifts) < 0
            s_ref[q * ROWS : (q + 1) * ROWS, cols(t)] = jnp.where(up, 1.0, -1.0).astype(BF16)
        pre = jnp.dot(wt[...], s_ref[:, cols(t)], preferred_element_type=F32)
        h_ref[:, cols(t)] = jnp.tanh(pre + hb)
        return carry

    lax.fori_loop(0, packed_ref.shape[0], step, 0)


def hidden_pass(pos, packed, w, hb, units):
    n = len(packed) * TILE
    return call(
        hidden_kernel,
        [SMEM] + [VMEM] * 6,
        [pltpu.VMEM((NB * 128, n), BF16), pltpu.VMEM((units, n), F32)],
        [pltpu.VMEM((units, NB * 128), BF16), pltpu.VMEM((len(packed), *packed[0].shape), jnp.int32)],
        flops=4 * 10**9,
    )(pos, *packed, w, hb)


def project(s_ref, h_ref, lhs, bias, p_ref):
    units = h_ref.shape[0]

    def step(t, carry):
        out = jnp.dot(lhs[...], s_ref[:, cols(t)], preferred_element_type=F32)
        proj = out[:units] + out[units:] + bias
        p_ref[sub(t), :] = to_rows(jnp.sum(h_ref[:, cols(t)] * proj, axis=0, keepdims=True))
        return carry

    lax.fori_loop(0, s_ref.shape[1] // TILE, step, 0)


def set_block(lhs, b, x):
    units = x.shape[0]
    hi, lo = split_terms(x)
    lhs[:units, b * 128 : (b + 1) * 128] = hi
    lhs[units:, b * 128 : (b + 1) * 128] = lo


def my_rows(pos_ref, ref, units):
    return ref[pl.ds(pos_ref[32] * (units // 128), units // 128), :]


def first_kernel(pos_ref, s_ref, h_ref, f0, f1, f2, f3, fb_ref, p_ref, lhs):
    units = h_ref.shape[0]
    norm = jnp.zeros((units, 128), F32)
    for b in range(NB):
        x = (f0, f1, f2, f3)[b // 2][b % 2]
        set_block(lhs, b, x)
        norm = norm + x * x
    fb = my_rows(pos_ref, fb_ref, units)
    n = p_ref.shape[0] - EXTRA
    p_ref[n:, :] = jnp.zeros((EXTRA, 128), F32)
    p_ref[n : n + 1, :] = total(norm) + total(fb * fb)
    project(s_ref, h_ref, lhs, rows_to_column(fb), p_ref)
    p_ref[n + 1 : n + 2, :] = total(p_ref[:n, :])


def first_pass(pos, spins, hidden, f, fb):
    units, n = hidden.shape
    return call(
        first_kernel,
        [SMEM] + [VMEM] * 7,
        [jax.ShapeDtypeStruct((n // 128 + EXTRA, 128), F32)],
        [pltpu.VMEM((2 * units, NB * 128), BF16)],
        flops=4 * 10**9,
    )(pos, resident(spins), resident(hidden), *f, fb)[0]


def step_of(norm, spread, samples, length):
    return norm / (spread / samples + LAM * length)


def second_kernel(samples, pos_ref, s_ref, h_ref, f0, f1, f2, f3, fb_ref, *refs):
    g, (mine_ref, norm_ref, *outs, lhs) = refs[:NB], refs[NB:]
    units = h_ref.shape[0]
    norm0 = norm_ref[0:1, :]
    spread = g[0][units + units // 128 : units + units // 128 + 1, :]
    a = step_of(norm0, spread, samples, norm0)
    rr = jnp.zeros((units, 128), F32)
    rf = jnp.zeros((units, 128), F32)
    for b in range(NB):
        f = (f0, f1, f2, f3)[b // 2][b % 2]
        r = f - a * (g[b][:units, :] + LAM * f)
        set_block(lhs, b, r)
        rr = rr + r * r
        rf = rf + r * f
    fb = my_rows(pos_ref, fb_ref, units)
    rb = fb - a * (g[0][units : units + units // 128, :] + LAM * fb)
    n = h_ref.shape[1] // 128
    p_ref = outs[0]
    p_ref[n : n + EXTRA, :] = jnp.zeros((EXTRA, 128), F32)
    p_ref[n : n + 1, :] = total(rr) + total(rb * rb)
    p_ref[n + 1 : n + 2, :] = total(rf) + total(rb * fb)
    p_ref[n + 2 : n + 2 + units // 128, :] = g[0][units : units + units // 128, :]
    p_ref[n + 2 + units // 128 : n + 3 + units // 128, :] = spread
    project(s_ref, h_ref, lhs, rows_to_column(rb), p_ref)
    for k, out in enumerate(outs):
        if k:
            out[: n + EXTRA, :] = p_ref[: n + EXTRA, :]
        place = -k % len(outs)
        for h in range(units // 128):
            at = n + EXTRA + h * ROWS
            out[at : at + ROWS, :] = mine_ref[place * ROWS : (place + 1) * ROWS, h * 128 : (h + 1) * 128]


def second_pass(samples, pos, spins, hidden, f, fb, g, mine, norm):
    units, n = hidden.shape
    parts = mine.shape[0] // ROWS
    return call(
        functools.partial(second_kernel, samples),
        [SMEM] + [VMEM] * (9 + NB),
        [jax.ShapeDtypeStruct((n // 128 + EXTRA + units // 128 * ROWS, 128), F32)] * parts,
        [pltpu.VMEM((2 * units, NB * 128), BF16)],
        flops=4 * 10**9,
    )(pos, resident(spins), resident(hidden), *f, fb, *g, mine, norm)


def put_stats(v, st_ref):
    mean = jnp.sum(v) / v.size
    st_ref[0:1, :] = jnp.full((1, 128), mean, F32)
    st_ref[1:2, :] = total((v - mean) ** 2)
    st_ref[2:, :] = jnp.zeros((st_ref.shape[0] - 2, 128), F32)


def over_chain_kernel(pos_ref, x0, x1, x2, x3, all_ref, got_ref):
    for d, x in enumerate((x0, x1, x2, x3)):
        got_ref[(pos_ref[32] + 4 - d) % 4] = x[...]
    rows = all_ref.shape[1]
    x = got_ref[0, :rows, :]
    for k in range(1, got_ref.shape[0]):
        x = x + got_ref[k, :rows, :]
    for k in range(all_ref.shape[0]):
        all_ref[k] = x


def over_groups(pos, parts, rows):
    shape = lambda *s: jax.ShapeDtypeStruct(s, F32)
    x, got = call(
        over_chain_kernel,
        [SMEM] + [VMEM] * 4,
        [shape(lax.axis_size(GRP), rows, 128), shape(len(parts), *parts[0].shape)],
    )(pos, *parts)
    return lax.all_to_all(x, GRP, 0, 0, tiled=True), got


def summed(got_ref):
    x = got_ref[0]
    for k in range(1, got_ref.shape[0]):
        x = x + got_ref[k]
    n = x.shape[0] - EXTRA
    return x[:n], x[n:]


def sum_of_set(got_ref, mine, stride, count):
    x = got_ref[mine]
    for k in range(1, count):
        x = x + got_ref[mine + k * stride]
    n = x.shape[0] - EXTRA
    everyone = got_ref[0, n + 1 : n + 2, :]
    for k in range(1, got_ref.shape[0]):
        everyone = everyone + got_ref[k, n + 1 : n + 2, :]
    return x, everyone, n


def first_chain_kernel(pos_ref, got_ref, all_ref):
    x, everyone, n = sum_of_set(got_ref, pos_ref[37], 2, got_ref.shape[0] // 2)
    for k in range(all_ref.shape[0]):
        all_ref[k] = x
        all_ref[k, n + 1 : n + 2, :] = everyone


def first_sum_kernel(pos_ref, got_ref, v_ref, extra_ref):
    peers = got_ref.shape[0] // 2
    x, everyone, n = sum_of_set(got_ref, pos_ref[38] * peers, 1, peers)
    v_ref[...] = x[:n]
    extra_ref[...] = x[n:]
    extra_ref[1:2, :] = everyone


def first_sum(pos, partial):
    shape = lambda *s: jax.ShapeDtypeStruct(s, F32)
    rows = partial.shape[0]
    chain, plane = ("zh", "zl"), ("xh", *GRP)
    got = to_all(partial, chain, lax.axis_size(chain))
    (x,) = call(first_chain_kernel, [SMEM, VMEM], [shape(lax.axis_size(plane), rows, 128)])(pos, got)
    got = lax.all_to_all(x, plane, 0, 0, tiled=True)
    return call(first_sum_kernel, [SMEM, VMEM], [shape(rows - EXTRA, 128), shape(EXTRA, 128)])(pos, got)


def second_sum_kernel(got_ref, v_ref, norm_ref, st_ref, next_ref):
    u, extra = summed(got_ref)
    next_ref[...] = extra
    beta = extra[0:1, 0:1] / norm_ref[0:1, 0:1]
    put_stats(u + beta * v_ref[...], st_ref)


def second_sum(got, values, norm):
    shape = lambda *s: jax.ShapeDtypeStruct(s, F32)
    return call(second_sum_kernel, [VMEM] * 3, [shape(8, 128), shape(EXTRA, 128)])(
        got, values, norm
    )


def pair_kernel(count, st_ref, got_ref, out_ref):
    delta = got_ref[0:1, :] - st_ref[0:1, :]
    out_ref[...] = st_ref[...] + got_ref[...]
    out_ref[0:1, :] = 0.5 * (st_ref[0:1, :] + got_ref[0:1, :])
    out_ref[1:2, :] = st_ref[1:2, :] + got_ref[1:2, :] + (0.5 * count) * delta * delta


def of_chips(st, count):
    (st,) = call(
        functools.partial(pair_kernel, count), [VMEM] * 2, [jax.ShapeDtypeStruct(st.shape, F32)]
    )(st, swap(st, "c"))
    return to_quad([st] * 4)


def joined_spread(refs, count):
    a, b, c, d = (ref[0:1, :] for ref in refs)
    mean = 0.25 * ((a + b) + (c + d))
    a, b, c, d = (ref[1:2, :] + count * (ref[0:1, :] - mean) ** 2 for ref in refs)
    return (a + b) + (c + d)


def columns_kernel(pos_ref, f_ref, o0, o1, o2, o3):
    units = o0.shape[1]
    for d, out in enumerate((o0, o1, o2, o3)):
        to = (pos_ref[32] + d) % 4
        out[...] = f_ref[:, pl.ds(pl.multiple_of(to * units, units), units)]


def columns_of(pos, f, units):
    out = jax.ShapeDtypeStruct((f.shape[0], units), F32)
    return call(columns_kernel, [SMEM, VMEM], [out] * 4)(pos, f)


def turned_kernel(f0, f1, f2, f3, out_ref):
    out_ref[0] = jnp.concatenate([f0[...], f1[...], f2[...], f3[...]], axis=0).T


def turned(f):
    rows, units = f[0].shape
    out = jax.ShapeDtypeStruct((1, units, rows * 4), F32)
    return call(turned_kernel, [VMEM] * 4, [out])(*f)[0]


def image_kernel(samples, pos_ref, s_ref, h_ref, v_ref, near_ref, far_ref, keep_ref, send_ref, acc, lanes):
    units = h_ref.shape[0]
    mean = (near_ref[1:2, 0:1] + far_ref[1:2, 0:1]) * (1.0 / samples)
    spread = total((v_ref[...] - mean) ** 2)
    acc[...] = jnp.zeros(acc.shape, F32)
    lanes[...] = jnp.zeros(lanes.shape, F32)

    def step(t, carry):
        r = h_ref[:, cols(t)] * to_line((v_ref[sub(t), :] - mean) * (1.0 / samples))
        both = jnp.concatenate(split_terms(r), axis=0)
        out = lax.dot_general(both, s_ref[:, cols(t)], (((1,), (1,)), ((), ())), preferred_element_type=F32)
        acc[...] += out[:units] + out[units:]
        part = r[:, :128]
        for k in range(1, TILE // 128):
            part = part + r[:, k * 128 : (k + 1) * 128]
        lanes[...] += part
        return carry

    lax.fori_loop(0, s_ref.shape[1] // TILE, step, 0)
    bias = [
        jnp.sum(lanes[k * 128 : (k + 1) * 128, :].T, axis=0, keepdims=True) for k in range(units // 128)
    ] + [spread, jnp.zeros((7 - units // 128, 128), F32)]
    bias = jnp.concatenate(bias, axis=0)
    for b in range(NB):
        ref = (keep_ref, send_ref)[b // 4]
        at = b % 4
        ref[at, :units, :] = acc[:, b * 128 : (b + 1) * 128]
        ref[at, units:, :] = bias


def image_pass(samples, pos, spins, hidden, values, near, far):
    units = hidden.shape[0]
    return call(
        functools.partial(image_kernel, samples),
        [SMEM] + [VMEM] * 5,
        [jax.ShapeDtypeStruct((4, units + 8, 128), F32)] * 2,
        [pltpu.VMEM((units, NB * 128), F32), pltpu.VMEM((units, 128), F32)],
        flops=4 * 10**9,
    )(pos, resident(spins), resident(hidden), values, near, far)


def halves_kernel(keep_ref, got_ref, o0, o1, o2, o3):
    for k, out in enumerate((o0, o1, o2, o3)):
        out[...] = keep_ref[k] + got_ref[k]


def halves(keep, got):
    return call(halves_kernel, [VMEM] * 2, [jax.ShapeDtypeStruct(keep.shape[1:], F32)] * 4)(keep, got)


def image_sum_kernel(g0, g1, g2, g3, all_ref, mine_ref):
    units = mine_ref.shape[1]
    x = g0[...] + g1[...] + (g2[...] + g3[...])
    all_ref[...] = x
    mine_ref[...] = x[:units].T


def image_sum(g, units):
    shape = lambda *s: jax.ShapeDtypeStruct(s, F32)
    return call(image_sum_kernel, [VMEM] * 4, [shape(*g[0].shape), shape(128, units)])(*g)


def to_quad(blocks):
    return [
        blocks[0],
        swap(blocks[1], "xh"),
        swap(blocks[2], "zl"),
        lax.ppermute(blocks[3], QUAD, [(i, i ^ 3) for i in range(4)]),
    ]


def update_kernel(samples, f_ref, fb_ref, got_ref, norm_ref, next_ref, *refs):
    *st_refs, w_ref, b_ref = refs
    parts = got_ref.shape[0]
    per = f_ref.shape[1] // 128 // parts
    n = got_ref.shape[1] - EXTRA - per * ROWS
    norm0, norm1 = norm_ref[0:1, 0:1], next_ref[0:1, 0:1]
    cross = next_ref[1:2, 0:1]
    beta = norm1 / norm0
    step0 = step_of(norm0, got_ref[0, n + 2 + per : n + 3 + per, 0:1], samples, norm0)
    step1 = step_of(norm1, joined_spread(st_refs, samples // 4)[:, 0:1], samples, norm1 + 2.0 * beta * cross + beta * beta * norm0)

    def update(f, g):
        r = f - step0 * (g + LAM * f)
        return step0 * f + step1 * (r + beta * f)

    for k in range(parts):
        for h in range(per):
            b = k * per + h
            at = n + EXTRA + h * ROWS
            w_ref[:, b * 128 : (b + 1) * 128] = update(f_ref[:, b * 128 : (b + 1) * 128], got_ref[k, at : at + ROWS, :])
            b_ref[b : b + 1, :] = update(fb_ref[b : b + 1, :], got_ref[k, n + 2 + h : n + 3 + h, :])


def update_pass(samples, f, fb, got, norm, st1, norms):
    shape = lambda s: jax.ShapeDtypeStruct(s, F32)
    return call(
        functools.partial(update_kernel, samples), [VMEM] * 9, [shape(f.shape), shape(fb.shape)]
    )(f, fb, got, norm, norms, *st1)


def body(spins_packed, weight, hidden_bias, force_w, force_b):
    xh, zh, zl, c = (lax.axis_index(a) for a in SMP)
    parts = lax.axis_size("zh")
    units = weight.shape[1] // parts
    samples = spins_packed.shape[1] * lax.axis_size(SMP)
    hb = hidden_bias.reshape(-1, 128)
    fb = force_b.reshape(-1, 128)

    q = jnp.arange(32, dtype=jnp.int32)
    words = (((q >> 2) & 1) ^ xh) * 16 + ((zh - q) & 3) * 4 + (((q >> 3) & 1) ^ zl) * 2 + ((q >> 4) ^ c)
    k = jnp.arange(4, dtype=jnp.int32)
    blocks = ((k & 1) ^ xh) * 2 + ((k >> 1) ^ zl)
    pos = jnp.concatenate([words, zh.reshape(1), blocks, zl.reshape(1), xh.reshape(1)])

    turn = lambda x, d: lax.ppermute(x, "zh", [(i, (i + d) % parts) for i in range(parts)])
    f = list(columns_of(pos, force_w, units))
    for d in (1, 2, 3):
        f[d] = turn(f[d], d)

    packed = [spins_packed]
    for d in (1, 2, 3):
        packed.append(turn(spins_packed, d))

    f = turned(f)
    f_xh = swap(f, "xh")
    f = jnp.concatenate([f, f_xh], axis=0)
    f_zl = swap(f, "zl")
    f = (f, f_zl, swap(f, "c"), swap(f_zl, "c"))

    w = lax.dynamic_slice_in_dim(weight, zh * units, units, 1)
    spins, hidden = hidden_pass(pos, packed, w, hb, units)
    partial = first_pass(pos, spins, hidden, f, fb)
    rows = partial.shape[0]
    values, norm = first_sum(pos, partial)
    norm_far = swap(norm, "c")

    keep, send = image_pass(samples, pos, spins, hidden, values, norm, norm_far)
    g, mine = image_sum(to_quad(halves(keep, swap(send, "c"))), units)
    g = to_quad([g] * 4)
    g += [swap(x, "c") for x in g]

    partials = second_pass(samples, pos, spins, hidden, f, fb, g, mine, norm)
    sums, got = over_groups(pos, [turn(x, d) if d else x for d, x in enumerate(partials)], rows)
    st, norms = second_sum(sums, values, norm)
    st1 = of_chips(st, values.size)
    out_w, out_b = update_pass(samples, force_w, fb, got, norm, st1, norms)
    return out_w, out_b.reshape(-1)


def solution(mesh):
    torus = Mesh(mesh.devices.reshape(2, 4, 2, 4, 2, 2), ("xl", "y", "xh", "zh", "zl", "c"))
    in_specs = (P(None, SMP), P(None, GRP), P(GRP), P(SMP, GRP), P(GRP))
    out_specs = (P(SMP, GRP), P(GRP))
    return jax.shard_map(body, mesh=torus, in_specs=in_specs, out_specs=out_specs, check_vma=False)
```

```python
import functools

import jax
import jax.numpy as jnp
from jax import lax
from jax.experimental import pallas as pl
from jax.experimental.pallas import tpu as pltpu
from jax.sharding import Mesh
from jax.sharding import PartitionSpec as P


GRP = ("xl", "y")
SMP = ("xh", "zh", "zl", "c")
QUAD = ("xh", "zl")
SWAP = [(0, 1), (1, 0)]
LAM = 0.01
ROWS = 32
NB = 8
TILE = 1024
LIMIT = 36
WIDE = 4096
EXTRA = 8
F32, BF16 = jnp.float32, jnp.bfloat16
VMEM = pl.BlockSpec(memory_space=pltpu.VMEM)
SMEM = pl.BlockSpec(memory_space=pltpu.SMEM)


def swap(x, axis):
    return lax.ppermute(x, axis, SWAP)


def to_all(x, axes, size):
    return lax.all_to_all(jnp.broadcast_to(x[None], (size, *x.shape)), axes, 0, 0, tiled=True)


def split_terms(x):
    hi = x.astype(BF16)
    return hi, (x - hi.astype(F32)).astype(BF16)


def resident(x):
    return pltpu.with_memory_space_constraint(x, pltpu.VMEM)


def call(kernel, ins, outs, scratch=(), flops=0):
    return pl.pallas_call(
        kernel,
        in_specs=ins,
        out_specs=[VMEM] * len(outs),
        out_shape=outs,
        scratch_shapes=scratch,
        compiler_params=pltpu.CompilerParams(vmem_limit_bytes=LIMIT << 20),
        cost_estimate=pl.CostEstimate(flops=flops, bytes_accessed=1 << 20, transcendentals=0),
    )


def cols(t, width=TILE):
    return pl.ds(pl.multiple_of(t * width, width), width)


def rows_to_column(rows):
    return jnp.concatenate(
        [jnp.broadcast_to(rows[k : k + 1, :], (128, 128)).T[:, :1] for k in range(rows.shape[0])], axis=0
    )


def total(x):
    return jnp.full((1, 128), jnp.sum(x), F32)


def to_rows(line):
    return jnp.concatenate([line[:, k * 128 : (k + 1) * 128] for k in range(line.shape[1] // 128)], axis=0)


def to_line(rows):
    return jnp.concatenate([rows[k : k + 1, :] for k in range(rows.shape[0])], axis=1)


def sub(t):
    return cols(t, WIDE // 128)


def hidden_kernel(pos_ref, x0, x1, x2, x3, w_ref, hb_ref, s_ref, h_ref, wt, packed_ref):
    units = wt.shape[0]
    for d, x in enumerate((x0, x1, x2, x3)):
        packed_ref[(pos_ref[32] + 4 - d) % 4] = x[...]
    for b in range(NB):
        rows = [w_ref[pl.ds(pl.multiple_of(pos_ref[4 * b + k] * ROWS, ROWS), ROWS), :] for k in range(4)]
        block = jnp.concatenate(rows, axis=0).astype(F32)
        wt[:, b * 128 : (b + 1) * 128] = block.T.astype(BF16)
    shifts = 31 - lax.broadcasted_iota(jnp.int32, (ROWS, TILE), 0)
    hb = rows_to_column(my_rows(pos_ref, hb_ref, units))

    def step(t, carry):
        for q in range(32):
            word = packed_ref[t, pl.ds(pos_ref[q], 1), :]
            up = jnp.left_shift(jnp.broadcast_to(word, (ROWS, TILE)), shifts) < 0
            s_ref[q * ROWS : (q + 1) * ROWS, cols(t)] = jnp.where(up, 1.0, -1.0).astype(BF16)
        pre = jnp.dot(wt[...], s_ref[:, cols(t)], preferred_element_type=F32)
        h_ref[:, cols(t)] = jnp.tanh(pre + hb)
        return carry

    lax.fori_loop(0, packed_ref.shape[0], step, 0)


def hidden_pass(pos, packed, w, hb, units):
    n = len(packed) * TILE
    return call(
        hidden_kernel,
        [SMEM] + [VMEM] * 6,
        [pltpu.VMEM((NB * 128, n), BF16), pltpu.VMEM((units, n), F32)],
        [pltpu.VMEM((units, NB * 128), BF16), pltpu.VMEM((len(packed), *packed[0].shape), jnp.int32)],
        flops=4 * 10**9,
    )(pos, *packed, w, hb)


def project(s_ref, h_ref, lhs, bias, p_ref):
    units = h_ref.shape[0]

    def step(t, carry):
        out = jnp.dot(lhs[...], s_ref[:, cols(t, WIDE)], preferred_element_type=F32)
        proj = out[:units] + out[units:] + bias
        p_ref[sub(t), :] = to_rows(jnp.sum(h_ref[:, cols(t, WIDE)] * proj, axis=0, keepdims=True))
        return carry

    lax.fori_loop(0, s_ref.shape[1] // WIDE, step, 0)


def set_block(lhs, b, x):
    units = x.shape[0]
    hi, lo = split_terms(x)
    lhs[:units, b * 128 : (b + 1) * 128] = hi
    lhs[units:, b * 128 : (b + 1) * 128] = lo


def my_rows(pos_ref, ref, units):
    return ref[pl.ds(pos_ref[32] * (units // 128), units // 128), :]


def first_kernel(pos_ref, s_ref, h_ref, f0, f1, f2, f3, fb_ref, p_ref, lhs):
    units = h_ref.shape[0]
    norm = jnp.zeros((units, 128), F32)
    for b in range(NB):
        x = (f0, f1, f2, f3)[b // 2][b % 2]
        set_block(lhs, b, x)
        norm = norm + x * x
    fb = my_rows(pos_ref, fb_ref, units)
    n = p_ref.shape[0] - EXTRA
    p_ref[n:, :] = jnp.zeros((EXTRA, 128), F32)
    p_ref[n : n + 1, :] = total(norm) + total(fb * fb)
    project(s_ref, h_ref, lhs, rows_to_column(fb), p_ref)
    p_ref[n + 1 : n + 2, :] = total(p_ref[:n, :])


def first_pass(pos, spins, hidden, f, fb):
    units, n = hidden.shape
    return call(
        first_kernel,
        [SMEM] + [VMEM] * 7,
        [jax.ShapeDtypeStruct((n // 128 + EXTRA, 128), F32)],
        [pltpu.VMEM((2 * units, NB * 128), BF16)],
        flops=4 * 10**9,
    )(pos, resident(spins), resident(hidden), *f, fb)[0]


def step_of(norm, spread, samples, length):
    return norm / (spread / samples + LAM * length)


def second_kernel(samples, pos_ref, s_ref, h_ref, f0, f1, f2, f3, fb_ref, *refs):
    g, (mine_ref, norm_ref, *outs, lhs) = refs[:NB], refs[NB:]
    units = h_ref.shape[0]
    norm0 = norm_ref[0:1, :]
    spread = g[0][units + units // 128 : units + units // 128 + 1, :]
    a = step_of(norm0, spread, samples, norm0)
    rr = jnp.zeros((units, 128), F32)
    rf = jnp.zeros((units, 128), F32)
    for b in range(NB):
        f = (f0, f1, f2, f3)[b // 2][b % 2]
        r = f - a * (g[b][:units, :] + LAM * f)
        set_block(lhs, b, r)
        rr = rr + r * r
        rf = rf + r * f
    fb = my_rows(pos_ref, fb_ref, units)
    rb = fb - a * (g[0][units : units + units // 128, :] + LAM * fb)
    n = h_ref.shape[1] // 128
    p_ref = outs[0]
    p_ref[n : n + EXTRA, :] = jnp.zeros((EXTRA, 128), F32)
    p_ref[n : n + 1, :] = total(rr) + total(rb * rb)
    p_ref[n + 1 : n + 2, :] = total(rf) + total(rb * fb)
    p_ref[n + 2 : n + 2 + units // 128, :] = g[0][units : units + units // 128, :]
    p_ref[n + 2 + units // 128 : n + 3 + units // 128, :] = spread
    project(s_ref, h_ref, lhs, rows_to_column(rb), p_ref)
    for k, out in enumerate(outs):
        if k:
            out[: n + EXTRA, :] = p_ref[: n + EXTRA, :]
        place = -k % len(outs)
        for h in range(units // 128):
            at = n + EXTRA + h * ROWS
            out[at : at + ROWS, :] = mine_ref[place * ROWS : (place + 1) * ROWS, h * 128 : (h + 1) * 128]


def second_pass(samples, pos, spins, hidden, f, fb, g, mine, norm):
    units, n = hidden.shape
    parts = mine.shape[0] // ROWS
    return call(
        functools.partial(second_kernel, samples),
        [SMEM] + [VMEM] * (9 + NB),
        [jax.ShapeDtypeStruct((n // 128 + EXTRA + units // 128 * ROWS, 128), F32)] * parts,
        [pltpu.VMEM((2 * units, NB * 128), BF16)],
        flops=4 * 10**9,
    )(pos, resident(spins), resident(hidden), *f, fb, *g, mine, norm)


def put_stats(v, st_ref):
    mean = jnp.sum(v) / v.size
    st_ref[0:1, :] = jnp.full((1, 128), mean, F32)
    st_ref[1:2, :] = total((v - mean) ** 2)
    st_ref[2:, :] = jnp.zeros((st_ref.shape[0] - 2, 128), F32)


def over_chain_kernel(pos_ref, x0, x1, x2, x3, all_ref, got_ref):
    for d, x in enumerate((x0, x1, x2, x3)):
        got_ref[(pos_ref[32] + 4 - d) % 4] = x[...]
    rows = all_ref.shape[1]
    x = got_ref[0, :rows, :]
    for k in range(1, got_ref.shape[0]):
        x = x + got_ref[k, :rows, :]
    for k in range(all_ref.shape[0]):
        all_ref[k] = x


def over_groups(pos, parts, rows):
    shape = lambda *s: jax.ShapeDtypeStruct(s, F32)
    x, got = call(
        over_chain_kernel,
        [SMEM] + [VMEM] * 4,
        [shape(lax.axis_size(GRP), rows, 128), shape(len(parts), *parts[0].shape)],
    )(pos, *parts)
    return lax.all_to_all(x, GRP, 0, 0, tiled=True), got


def summed(got_ref):
    x = got_ref[0]
    for k in range(1, got_ref.shape[0]):
        x = x + got_ref[k]
    n = x.shape[0] - EXTRA
    return x[:n], x[n:]


def sum_of_set(got_ref, mine, stride, count):
    x = got_ref[mine]
    for k in range(1, count):
        x = x + got_ref[mine + k * stride]
    n = x.shape[0] - EXTRA
    everyone = got_ref[0, n + 1 : n + 2, :]
    for k in range(1, got_ref.shape[0]):
        everyone = everyone + got_ref[k, n + 1 : n + 2, :]
    return x, everyone, n


def first_chain_kernel(pos_ref, got_ref, all_ref):
    x, everyone, n = sum_of_set(got_ref, pos_ref[37], 2, got_ref.shape[0] // 2)
    for k in range(all_ref.shape[0]):
        all_ref[k] = x
        all_ref[k, n + 1 : n + 2, :] = everyone


def first_sum_kernel(pos_ref, got_ref, v_ref, extra_ref):
    peers = got_ref.shape[0] // 2
    x, everyone, n = sum_of_set(got_ref, pos_ref[38] * peers, 1, peers)
    v_ref[...] = x[:n]
    extra_ref[...] = x[n:]
    extra_ref[1:2, :] = everyone


def first_sum(pos, partial):
    shape = lambda *s: jax.ShapeDtypeStruct(s, F32)
    rows = partial.shape[0]
    chain, plane = ("zh", "zl"), ("xh", *GRP)
    got = to_all(partial, chain, lax.axis_size(chain))
    (x,) = call(first_chain_kernel, [SMEM, VMEM], [shape(lax.axis_size(plane), rows, 128)])(pos, got)
    got = lax.all_to_all(x, plane, 0, 0, tiled=True)
    return call(first_sum_kernel, [SMEM, VMEM], [shape(rows - EXTRA, 128), shape(EXTRA, 128)])(pos, got)


def second_sum_kernel(got_ref, v_ref, norm_ref, st_ref, next_ref):
    u, extra = summed(got_ref)
    next_ref[...] = extra
    beta = extra[0:1, 0:1] / norm_ref[0:1, 0:1]
    put_stats(u + beta * v_ref[...], st_ref)


def second_sum(got, values, norm):
    shape = lambda *s: jax.ShapeDtypeStruct(s, F32)
    return call(second_sum_kernel, [VMEM] * 3, [shape(8, 128), shape(EXTRA, 128)])(
        got, values, norm
    )


def pair_kernel(count, st_ref, got_ref, out_ref):
    delta = got_ref[0:1, :] - st_ref[0:1, :]
    out_ref[...] = st_ref[...] + got_ref[...]
    out_ref[0:1, :] = 0.5 * (st_ref[0:1, :] + got_ref[0:1, :])
    out_ref[1:2, :] = st_ref[1:2, :] + got_ref[1:2, :] + (0.5 * count) * delta * delta


def of_chips(st, count):
    (st,) = call(
        functools.partial(pair_kernel, count), [VMEM] * 2, [jax.ShapeDtypeStruct(st.shape, F32)]
    )(st, swap(st, "c"))
    return to_quad([st] * 4)


def joined_spread(refs, count):
    a, b, c, d = (ref[0:1, :] for ref in refs)
    mean = 0.25 * ((a + b) + (c + d))
    a, b, c, d = (ref[1:2, :] + count * (ref[0:1, :] - mean) ** 2 for ref in refs)
    return (a + b) + (c + d)


def columns_kernel(pos_ref, f_ref, o0, o1, o2, o3):
    units = o0.shape[1]
    for d, out in enumerate((o0, o1, o2, o3)):
        to = (pos_ref[32] + d) % 4
        out[...] = f_ref[:, pl.ds(pl.multiple_of(to * units, units), units)]


def columns_of(pos, f, units):
    out = jax.ShapeDtypeStruct((f.shape[0], units), F32)
    return call(columns_kernel, [SMEM, VMEM], [out] * 4)(pos, f)


def turned_kernel(f0, f1, f2, f3, out_ref):
    out_ref[0] = jnp.concatenate([f0[...], f1[...], f2[...], f3[...]], axis=0).T


def turned(f):
    rows, units = f[0].shape
    out = jax.ShapeDtypeStruct((1, units, rows * 4), F32)
    return call(turned_kernel, [VMEM] * 4, [out])(*f)[0]


def image_kernel(samples, pos_ref, s_ref, h_ref, v_ref, near_ref, far_ref, keep_ref, send_ref, acc, lanes):
    units = h_ref.shape[0]
    mean = (near_ref[1:2, 0:1] + far_ref[1:2, 0:1]) * (1.0 / samples)
    spread = total((v_ref[...] - mean) ** 2)
    acc[...] = jnp.zeros(acc.shape, F32)
    lanes[...] = jnp.zeros(lanes.shape, F32)

    def step(t, carry):
        r = h_ref[:, cols(t, WIDE)] * to_line((v_ref[sub(t), :] - mean) * (1.0 / samples))
        both = jnp.concatenate(split_terms(r), axis=0)
        out = lax.dot_general(both, s_ref[:, cols(t, WIDE)], (((1,), (1,)), ((), ())), preferred_element_type=F32)
        acc[...] += out[:units] + out[units:]
        part = r[:, :128]
        for k in range(1, WIDE // 128):
            part = part + r[:, k * 128 : (k + 1) * 128]
        lanes[...] += part
        return carry

    lax.fori_loop(0, s_ref.shape[1] // WIDE, step, 0)
    bias = [
        jnp.sum(lanes[k * 128 : (k + 1) * 128, :].T, axis=0, keepdims=True) for k in range(units // 128)
    ] + [spread, jnp.zeros((7 - units // 128, 128), F32)]
    bias = jnp.concatenate(bias, axis=0)
    for b in range(NB):
        ref = (keep_ref, send_ref)[b // 4]
        at = b % 4
        ref[at, :units, :] = acc[:, b * 128 : (b + 1) * 128]
        ref[at, units:, :] = bias


def image_pass(samples, pos, spins, hidden, values, near, far):
    units = hidden.shape[0]
    return call(
        functools.partial(image_kernel, samples),
        [SMEM] + [VMEM] * 5,
        [jax.ShapeDtypeStruct((4, units + 8, 128), F32)] * 2,
        [pltpu.VMEM((units, NB * 128), F32), pltpu.VMEM((units, 128), F32)],
        flops=4 * 10**9,
    )(pos, resident(spins), resident(hidden), values, near, far)


def halves_kernel(keep_ref, got_ref, o0, o1, o2, o3):
    for k, out in enumerate((o0, o1, o2, o3)):
        out[...] = keep_ref[k] + got_ref[k]


def halves(keep, got):
    return call(halves_kernel, [VMEM] * 2, [jax.ShapeDtypeStruct(keep.shape[1:], F32)] * 4)(keep, got)


def image_sum_kernel(g0, g1, g2, g3, all_ref, mine_ref):
    units = mine_ref.shape[1]
    x = g0[...] + g1[...] + (g2[...] + g3[...])
    all_ref[...] = x
    mine_ref[...] = x[:units].T


def image_sum(g, units):
    shape = lambda *s: jax.ShapeDtypeStruct(s, F32)
    return call(image_sum_kernel, [VMEM] * 4, [shape(*g[0].shape), shape(128, units)])(*g)


def to_quad(blocks):
    return [
        blocks[0],
        swap(blocks[1], "xh"),
        swap(blocks[2], "zl"),
        lax.ppermute(blocks[3], QUAD, [(i, i ^ 3) for i in range(4)]),
    ]


def update_kernel(samples, f_ref, fb_ref, got_ref, norm_ref, next_ref, *refs):
    *st_refs, w_ref, b_ref = refs
    parts = got_ref.shape[0]
    per = f_ref.shape[1] // 128 // parts
    n = got_ref.shape[1] - EXTRA - per * ROWS
    norm0, norm1 = norm_ref[0:1, 0:1], next_ref[0:1, 0:1]
    cross = next_ref[1:2, 0:1]
    beta = norm1 / norm0
    step0 = step_of(norm0, got_ref[0, n + 2 + per : n + 3 + per, 0:1], samples, norm0)
    step1 = step_of(norm1, joined_spread(st_refs, samples // 4)[:, 0:1], samples, norm1 + 2.0 * beta * cross + beta * beta * norm0)

    def update(f, g):
        r = f - step0 * (g + LAM * f)
        return step0 * f + step1 * (r + beta * f)

    for k in range(parts):
        for h in range(per):
            b = k * per + h
            at = n + EXTRA + h * ROWS
            w_ref[:, b * 128 : (b + 1) * 128] = update(f_ref[:, b * 128 : (b + 1) * 128], got_ref[k, at : at + ROWS, :])
            b_ref[b : b + 1, :] = update(fb_ref[b : b + 1, :], got_ref[k, n + 2 + h : n + 3 + h, :])


def update_pass(samples, f, fb, got, norm, st1, norms):
    shape = lambda s: jax.ShapeDtypeStruct(s, F32)
    return call(
        functools.partial(update_kernel, samples), [VMEM] * 9, [shape(f.shape), shape(fb.shape)]
    )(f, fb, got, norm, norms, *st1)


def body(spins_packed, weight, hidden_bias, force_w, force_b):
    xh, zh, zl, c = (lax.axis_index(a) for a in SMP)
    parts = lax.axis_size("zh")
    units = weight.shape[1] // parts
    samples = spins_packed.shape[1] * lax.axis_size(SMP)
    hb = hidden_bias.reshape(-1, 128)
    fb = force_b.reshape(-1, 128)

    q = jnp.arange(32, dtype=jnp.int32)
    words = (((q >> 2) & 1) ^ xh) * 16 + ((zh - q) & 3) * 4 + (((q >> 3) & 1) ^ zl) * 2 + ((q >> 4) ^ c)
    k = jnp.arange(4, dtype=jnp.int32)
    blocks = ((k & 1) ^ xh) * 2 + ((k >> 1) ^ zl)
    pos = jnp.concatenate([words, zh.reshape(1), blocks, zl.reshape(1), xh.reshape(1)])

    turn = lambda x, d: lax.ppermute(x, "zh", [(i, (i + d) % parts) for i in range(parts)])
    f = list(columns_of(pos, force_w, units))
    for d in (1, 2, 3):
        f[d] = turn(f[d], d)

    packed = [spins_packed]
    for d in (1, 2, 3):
        packed.append(turn(spins_packed, d))

    f = turned(f)
    f_xh = swap(f, "xh")
    f = jnp.concatenate([f, f_xh], axis=0)
    f_zl = swap(f, "zl")
    f = (f, f_zl, swap(f, "c"), swap(f_zl, "c"))

    w = lax.dynamic_slice_in_dim(weight, zh * units, units, 1)
    spins, hidden = hidden_pass(pos, packed, w, hb, units)
    partial = first_pass(pos, spins, hidden, f, fb)
    rows = partial.shape[0]
    values, norm = first_sum(pos, partial)
    norm_far = swap(norm, "c")

    keep, send = image_pass(samples, pos, spins, hidden, values, norm, norm_far)
    g, mine = image_sum(to_quad(halves(keep, swap(send, "c"))), units)
    g = to_quad([g] * 4)
    g += [swap(x, "c") for x in g]

    partials = second_pass(samples, pos, spins, hidden, f, fb, g, mine, norm)
    sums, got = over_groups(pos, [turn(x, d) if d else x for d, x in enumerate(partials)], rows)
    st, norms = second_sum(sums, values, norm)
    st1 = of_chips(st, values.size)
    out_w, out_b = update_pass(samples, force_w, fb, got, norm, st1, norms)
    return out_w, out_b.reshape(-1)


def solution(mesh):
    torus = Mesh(mesh.devices.reshape(2, 4, 2, 4, 2, 2), ("xl", "y", "xh", "zh", "zl", "c"))
    in_specs = (P(None, SMP), P(None, GRP), P(GRP), P(SMP, GRP), P(GRP))
    out_specs = (P(SMP, GRP), P(GRP))
    return jax.shard_map(body, mesh=torus, in_specs=in_specs, out_specs=out_specs, check_vma=False)
```
